64 devices in a mesh: data: 4 (over x, y), model: 16 (over z, core).
Axes of the slice: x: 2, y: 2, z: 8, core: 2. Of those that a mesh axis runs over, the one named last changes fastest.
The devices are a block of a 4x4x8 slice.
Arguments:
- x_tok: bfloat16 [8, 256, 5120], P('data', 'model'), parts along dimension 0
- dy_tok: bfloat16 [8, 256, 5120], P('data', 'model'), parts along dimension 0
- w_q: bfloat16 [5120, 32, 128], P(None, 'model')
- w_k: bfloat16 [5120, 8, 128], replicated
- w_v: bfloat16 [5120, 8, 128], replicated
- w_o: bfloat16 [32, 128, 5120], P('model')
Outputs:
- output 1: bfloat16 [8, 256, 5120], P('data', 'model'), parts along dimension 0
- output 2: float32 [20480, 32, 128], P('data', 'model'), parts along dimension 0
- output 3: float32 [163840, 128], P(('data', 'model')), parts along dimension 0
- output 4: float32 [163840, 128], P(('data', 'model')), parts along dimension 0
- output 5: float32 [128, 128, 5120], P(('data', 'model')), parts along dimension 0
There are 4 independent parts. The reference program is written for one: setup_inputs(seed, part) draws one part's arguments, and reference() takes and returns one part's arrays. A program takes and returns all parts, laid end to end along the dimension named above; an argument that names none is the same for every part.
All inputs are finite; a program needn't handle non-finite values.
Results may differ from the reference program's by a relative error of at most 0.00937.
Values are sent between devices in bfloat16 or wider.
A program may use at most 768 MiB of HBM per device.

```python
import jax
import jax.numpy as jnp
from jax import lax

D = 5120
HEADS = 32
KV_HEADS = 8
HEAD = 128
SEQ = 256
MICRO = 2

GROUP_HEADS = HEADS // KV_HEADS
SCORE_SCALE = HEAD ** -0.5


def setup_inputs(seed: int = 0, part: int = 0) -> dict:
    part_key = jax.random.fold_in(jax.random.key(seed), part)
    key_x, key_dy = jax.random.split(part_key, 2)
    key_q, key_k, key_v, key_o = jax.random.split(jax.random.key(seed + 1), 4)
    x_tok = jax.random.normal(key_x, (MICRO, SEQ, D), jnp.float32).astype(jnp.bfloat16)
    dy_tok = jax.random.normal(key_dy, (MICRO, SEQ, D), jnp.float32).astype(jnp.bfloat16)
    w_q = (jax.random.normal(key_q, (D, HEADS, HEAD), jnp.float32) * D ** -0.5).astype(jnp.bfloat16)
    w_k = (jax.random.normal(key_k, (D, KV_HEADS, HEAD), jnp.float32) * D ** -0.5).astype(jnp.bfloat16)
    w_v = (jax.random.normal(key_v, (D, KV_HEADS, HEAD), jnp.float32) * D ** -0.5).astype(jnp.bfloat16)
    w_o = (jax.random.normal(key_o, (HEADS, HEAD, D), jnp.float32) * (HEADS * HEAD) ** -0.5).astype(jnp.bfloat16)
    return {"x_tok": x_tok, "dy_tok": dy_tok, "w_q": w_q, "w_k": w_k, "w_v": w_v, "w_o": w_o}


def micro_grads(micro_in, w_q, w_k, w_v, w_o):
    x_micro, dy_micro = micro_in
    w_q_flat = w_q.reshape(D, HEADS * HEAD)
    w_k_flat = w_k.reshape(D, KV_HEADS * HEAD)
    w_v_flat = w_v.reshape(D, KV_HEADS * HEAD)
    w_o_flat = w_o.reshape(HEADS * HEAD, D)
    q_all = jnp.dot(x_micro, w_q_flat, preferred_element_type=jnp.float32).astype(jnp.bfloat16).reshape(SEQ, HEADS, HEAD)
    k_all = jnp.dot(x_micro, w_k_flat, preferred_element_type=jnp.float32).astype(jnp.bfloat16).reshape(SEQ, KV_HEADS, HEAD)
    v_all = jnp.dot(x_micro, w_v_flat, preferred_element_type=jnp.float32).astype(jnp.bfloat16).reshape(SEQ, KV_HEADS, HEAD)
    d_out = jnp.dot(dy_micro, w_o_flat.T, preferred_element_type=jnp.float32).astype(jnp.bfloat16).reshape(SEQ, HEADS, HEAD)
    k_rep = jnp.repeat(k_all, GROUP_HEADS, axis=1)
    v_rep = jnp.repeat(v_all, GROUP_HEADS, axis=1)
    q_pos = jnp.arange(SEQ)[:, None]
    k_pos = jnp.arange(SEQ)[None, :]

    def head_grads(head_in):
        q_head, k_head, v_head, do_head = head_in
        scores = jnp.dot(q_head, k_head.T, preferred_element_type=jnp.float32) * SCORE_SCALE
        scores = jnp.where(q_pos >= k_pos, scores, -jnp.inf)
        prob_f32 = jax.nn.softmax(scores, axis=-1)
        prob_b16 = prob_f32.astype(jnp.bfloat16)
        out_head = jnp.dot(prob_b16, v_head, preferred_element_type=jnp.float32).astype(jnp.bfloat16)
        d_prob = jnp.dot(do_head, v_head.T, preferred_element_type=jnp.float32)
        row_delta = jnp.sum(do_head.astype(jnp.float32) * out_head.astype(jnp.float32), axis=-1, keepdims=True)
        d_score = (prob_f32 * (d_prob - row_delta)).astype(jnp.bfloat16)
        dq_head = (jnp.dot(d_score, k_head, preferred_element_type=jnp.float32) * SCORE_SCALE).astype(jnp.bfloat16)
        dk_head = jnp.dot(d_score.T, q_head, preferred_element_type=jnp.float32) * SCORE_SCALE
        dv_head = jnp.dot(prob_b16.T, do_head, preferred_element_type=jnp.float32)
        dwo_head = jnp.dot(out_head.T, dy_micro, preferred_element_type=jnp.float32)
        return dq_head, dk_head, dv_head, dwo_head

    heads_major = (q_all.transpose(1, 0, 2), k_rep.transpose(1, 0, 2), v_rep.transpose(1, 0, 2), d_out.transpose(1, 0, 2))
    d_q, d_k, d_v, dw_o = lax.map(head_grads, heads_major)
    d_k_sum = d_k.reshape(KV_HEADS, GROUP_HEADS, SEQ, HEAD).sum(axis=1).astype(jnp.bfloat16)
    d_v_sum = d_v.reshape(KV_HEADS, GROUP_HEADS, SEQ, HEAD).sum(axis=1).astype(jnp.bfloat16)
    d_q_flat = d_q.transpose(1, 0, 2).reshape(SEQ, HEADS * HEAD)
    d_k_flat = d_k_sum.transpose(1, 0, 2).reshape(SEQ, KV_HEADS * HEAD)
    d_v_flat = d_v_sum.transpose(1, 0, 2).reshape(SEQ, KV_HEADS * HEAD)
    dw_q = jnp.dot(x_micro.T, d_q_flat, preferred_element_type=jnp.float32).reshape(D, HEADS, HEAD)
    dw_k = jnp.dot(x_micro.T, d_k_flat, preferred_element_type=jnp.float32).reshape(D, KV_HEADS, HEAD)
    dw_v = jnp.dot(x_micro.T, d_v_flat, preferred_element_type=jnp.float32).reshape(D, KV_HEADS, HEAD)
    dx_f32 = (jnp.dot(d_q_flat, w_q_flat.T, preferred_element_type=jnp.float32)
              + jnp.dot(d_k_flat, w_k_flat.T, preferred_element_type=jnp.float32)
              + jnp.dot(d_v_flat, w_v_flat.T, preferred_element_type=jnp.float32))
    return dx_f32.astype(jnp.bfloat16), dw_q, dw_k, dw_v, dw_o


def reference(x_tok, dy_tok, w_q, w_k, w_v, w_o):
    def one_micro(micro_in):
        return micro_grads(micro_in, w_q, w_k, w_v, w_o)

    dx_tok, dw_q, dw_k, dw_v, dw_o = lax.map(one_micro, (x_tok, dy_tok))
    dw_k_rows = dw_k.sum(axis=0).transpose(1, 0, 2).reshape(KV_HEADS * D, HEAD)
    dw_v_rows = dw_v.sum(axis=0).transpose(1, 0, 2).reshape(KV_HEADS * D, HEAD)
    return (dx_tok, dw_q.sum(axis=0), dw_k_rows, dw_v_rows, dw_o.sum(axis=0))
```

```python
import functools

import jax
import jax.numpy as jnp
from jax import lax
from jax.experimental import pallas as pl
from jax.experimental.pallas import tpu as pltpu
from jax.sharding import PartitionSpec as P

BF16 = jnp.bfloat16
F32 = jnp.float32
MESH = pl.DeviceIdType.MESH

NT = (((1,), (1,)), ((), ()))
NN = (((1,), (0,)), ((), ()))
TN = (((0,), (0,)), ((), ()))


def dot(a, b, dims=NN):
    return lax.dot_general(a, b, dims, preferred_element_type=F32)


def attn_kernel(n_dev, kv_heads, x_in, dy_in, wq_in, wk_in, wv_in, wo_in,
                dx_out, xf_out, dyf_out, dq_out, dkv_out, o_out,
                xb, dyb, wq, wo, wkv, stage_q, stage_kv, unpacked,
                acc_q, acc_kv, acc_do, qb, kvb, dob, ob, dqb, dkvp, prob_b, ds_b,
                dkv_f, dkv_peer, dkv_tot,
                dx_f, dx_tmp, psend, precv, sbuf, rbuf, dx_own,
                own_sem, w_sem, kvw_sem, out_sem,
                ag_send, ag_recv, d2d_send, d2d_recv, wx_sem,
                dkv_sem, ps_send, ps_recv, rs_send, rs_recv):
    n_chip = n_dev // 2
    half = n_chip // 2
    micro_n, tok, d_model = x_in.shape
    head_dim = wk_in.shape[1]
    heads = wq.shape[1] // head_dim
    n_rows = n_dev * tok
    par_rows = n_rows // 2
    me = lax.axis_index("model")
    z, c = me // 2, me % 2
    right = lax.rem(me + 2, n_dev)
    left = lax.rem(me + n_dev - 2, n_dev)
    peer = z * 2 + (1 - c)
    scale = head_dim ** -0.5

    def to(dev):
        return {"model": dev}

    bufs = ((x_in, xb), (dy_in, dyb))
    my_row = pl.multiple_of(c * par_rows + z * tok, tok)
    own = []
    for m in range(micro_n):
        for t, (src, buf) in enumerate(bufs):
            cp = pltpu.make_async_copy(src.at[m], buf.at[m, pl.ds(my_row, tok)], own_sem.at[m, t])
            cp.start()
            own.append(cp)
    wq_cp = pltpu.make_async_copy(wq_in, stage_q, w_sem.at[0])
    wq_cp.start()
    wo_cp = pltpu.make_async_copy(wo_in, wo, w_sem.at[1])
    wo_cp.start()
    kv_rows = stage_kv.shape[1]
    n_kv = wk_in.shape[0] // kv_rows

    def kv_load(i):
        @pl.when(c == 0)
        def _():
            pltpu.make_async_copy(wk_in.at[pl.ds(i * kv_rows, kv_rows)], stage_kv.at[i % 2], kvw_sem.at[i % 2]).start()

        @pl.when(c == 1)
        def _():
            pltpu.make_async_copy(wv_in.at[pl.ds(i * kv_rows, kv_rows)], stage_kv.at[i % 2], kvw_sem.at[i % 2]).start()

    kv_load(0)
    kv_load(1)

    barrier = pltpu.get_barrier_semaphore()
    for dev in (left, right, peer):
        pl.semaphore_signal(barrier, inc=1, device_id=to(dev), device_id_type=MESH)
    pl.semaphore_wait(barrier, 3)

    n_col = 2
    col_w = d_model // n_col
    sub_w = col_w // 2

    def blk(m, t, chip, col, width, core=None):
        row = pl.multiple_of((c if core is None else core) * par_rows + chip * tok, tok)
        return bufs[t][1].at[m, pl.ds(row, tok), pl.ds(col, width)]

    def send(ref, dev, ssem, rsem):
        pltpu.make_async_remote_copy(src_ref=ref, dst_ref=ref, send_sem=ssem, recv_sem=rsem,
                                     device_id=to(dev), device_id_type=MESH).start()

    def ag_start(m):
        for t in range(2):
            own[m * 2 + t].wait()
        for t in range(2):
            for j in range(n_col):
                ref = blk(m, t, z, j * col_w, col_w)
                send(ref, right, ag_send.at[m, t, j], ag_recv.at[m, t, j, 0, 0])
                send(ref, left, ag_send.at[m, t, j], ag_recv.at[m, t, j, 0, 1])
                send(ref, peer, d2d_send.at[m, t, j], d2d_recv.at[m, t, j])

    def ag_event(m, t, j, d):
        last = d == half
        for side in range(2):
            chip = lax.rem(z + (n_chip - d if side == 0 else d), n_chip)
            col, width = (j * col_w, col_w) if not last else (j * col_w + side * sub_w, sub_w)
            ref = blk(m, t, chip, col, width)
            pltpu.make_async_copy(ref, ref, ag_recv.at[m, t, j, d - 1, side]).wait()
            if d < half - 1:
                fwd = ref
            elif d == half - 1:
                fwd = blk(m, t, chip, j * col_w + side * sub_w, sub_w)
            else:
                fwd = None
            if fwd is not None:
                send(fwd, right if side == 0 else left, ag_send.at[m, t, j], ag_recv.at[m, t, j, d, side])
            send(ref, peer, d2d_send.at[m, t, j], d2d_recv.at[m, t, j])

    def peer_blocks(m, t, j, core):
        row = pl.multiple_of(core * par_rows, par_rows)
        return bufs[t][1].at[m, pl.ds(row, par_rows), pl.ds(j * col_w, col_w)]

    def d2d_wait(m, t, j):
        ref = peer_blocks(m, t, j, 1 - c)
        pltpu.make_async_copy(ref, ref, d2d_recv.at[m, t, j]).wait()

    un_rows = unpacked.shape[0]

    def prep_wq():
        wq_cp.wait()
        per = un_rows // heads

        def body(i, _):
            unpacked[...] = stage_q[pl.ds(pl.multiple_of(i * un_rows, un_rows), un_rows), :].astype(F32)
            for h in range(heads):
                wq[pl.ds(pl.multiple_of(i * per, per), per), h * head_dim:(h + 1) * head_dim] = (
                    unpacked[pl.ds(h, per, stride=heads), :].astype(BF16))
            return 0

        lax.fori_loop(0, stage_q.shape[0] // un_rows, body, 0)

    kv_col = pl.multiple_of(c * head_dim, head_dim)

    def prep_kv(i):
        pltpu.make_async_copy(wk_in.at[pl.ds(i * kv_rows, kv_rows)], stage_kv.at[i % 2], kvw_sem.at[i % 2]).wait()
        per = un_rows // kv_heads
        base = i * (kv_rows // kv_heads)

        def body(k, _):
            unpacked[...] = stage_kv[i % 2, pl.ds(pl.multiple_of(k * un_rows, un_rows), un_rows), :].astype(F32)
            wkv[pl.ds(pl.multiple_of(base + k * per, per), per), pl.ds(kv_col, head_dim)] = (
                unpacked[pl.ds(z, per, stride=kv_heads), :].astype(BF16))
            return 0

        lax.fori_loop(0, kv_rows // un_rows, body, 0)
        if i + 2 < n_kv:
            kv_load(i + 2)

    def kv_swap():
        ref = wkv.at[:, pl.ds(kv_col, head_dim)]
        pltpu.make_async_remote_copy(src_ref=ref, dst_ref=ref, send_sem=wx_sem.at[0], recv_sem=wx_sem.at[1],
                                     device_id=to(peer), device_id_type=MESH).start()

    def kv_swap_wait():
        ref = wkv.at[:, pl.ds(kv_col, head_dim)]
        pltpu.make_async_copy(ref, ref, wx_sem.at[0]).wait()
        ref = wkv.at[:, pl.ds(pl.multiple_of((1 - c) * head_dim, head_dim), head_dim)]
        pltpu.make_async_copy(ref, ref, wx_sem.at[1]).wait()

    def proj_x(m, j):
        for k in range(2):
            cols = slice(j * col_w + k * sub_w, j * col_w + (k + 1) * sub_w)
            a = dot(xb[m, :, cols], wq[cols, :])
            b = dot(xb[m, :, cols], wkv[cols, :])
            if j == 0 and k == 0:
                acc_q[...] = a
                acc_kv[...] = b
            else:
                acc_q[...] += a
                acc_kv[...] += b

    def proj_dy(m, j):
        for k in range(2):
            cols = slice(j * col_w + k * sub_w, j * col_w + (k + 1) * sub_w)
            a = dot(dyb[m, :, cols], wo[:, cols], NT)
            if j == 0 and k == 0:
                acc_do[...] = a
            else:
                acc_do[...] += a

    def round_x():
        qb[...] = acc_q[...].astype(BF16)
        kvb[...] = acc_kv[...].astype(BF16)

    def round_dy():
        dob[...] = acc_do[...].astype(BF16)

    def position(axis):
        r = lax.broadcasted_iota(jnp.int32, (n_rows, 1) if axis == 0 else (1, n_rows), axis)
        inner = r % par_rows
        return (inner // tok) * (2 * tok) + (r // par_rows) * tok + inner % tok

    def head(m, h):
        cols = slice(h * head_dim, (h + 1) * head_dim)
        q, k, v = qb[:, cols], kvb[:, :head_dim], kvb[:, head_dim:]
        do = dob[:, cols]
        s = dot(q, k, NT) * scale
        s = jnp.where(position(0) >= position(1), s, -jnp.inf)
        e = jnp.exp(s - jnp.max(s, axis=-1, keepdims=True))
        p = e / jnp.sum(e, axis=-1, keepdims=True)
        pb = p.astype(BF16)
        o = dot(pb, v).astype(BF16)
        ob[m, :, cols] = o
        dp = dot(do, v, NT)
        delta = jnp.sum(do.astype(F32) * o.astype(F32), axis=-1, keepdims=True)
        ds = (p * (dp - delta)).astype(BF16)
        prob_b[h] = pb
        ds_b[h] = ds
        dqb[m, :, cols] = (dot(ds, k) * scale).astype(BF16)

    def head_kv(m, h):
        cols = slice(h * head_dim, (h + 1) * head_dim)
        dk = dot(ds_b[h], qb[:, cols], TN) * scale
        dv = dot(prob_b[h], dob[:, cols], TN)
        if h == 0:
            dkv_f[m, :, :head_dim] = dk
            dkv_f[m, :, head_dim:] = dv
        else:
            dkv_f[m, :, :head_dim] += dk
            dkv_f[m, :, head_dim:] += dv

    def kv_round(m):
        dkvp[...] = dkv_f[m].astype(BF16)
        pltpu.make_async_remote_copy(src_ref=dkv_f.at[m], dst_ref=dkv_peer.at[m], send_sem=dkv_sem.at[m, 0],
                                     recv_sem=dkv_sem.at[m, 1], device_id=to(peer), device_id_type=MESH).start()

    def kv_total(m):
        pltpu.make_async_copy(dkv_f.at[m], dkv_f.at[m], dkv_sem.at[m, 0]).wait()
        pltpu.make_async_copy(dkv_peer.at[m], dkv_peer.at[m], dkv_sem.at[m, 1]).wait()
        dkv_tot[m] = (dkv_f[m] + dkv_peer[m]).astype(BF16)

    rs_n = 4
    rs_w = d_model // rs_n
    rs_h = rs_w // 2

    def dx_chunk(m, j):
        cols = slice(j * rs_w, (j + 1) * rs_w)
        dx_tmp[...] = dot(dqb[m], wq[cols, :], NT) + dot(dkvp[...], wkv[cols, :], NT)
        away = pl.ds(pl.multiple_of((1 - c) * par_rows, par_rows), par_rows)
        keep = pl.ds(pl.multiple_of(c * par_rows, par_rows), par_rows)
        psend[m, :, cols] = dx_tmp[away, :].astype(BF16)
        dx_f[m, :, cols] = dx_tmp[keep, :]
        pltpu.make_async_remote_copy(src_ref=psend.at[m, :, cols], dst_ref=precv.at[m, :, cols],
                                     send_sem=ps_send.at[m, j], recv_sem=ps_recv.at[m, j],
                                     device_id=to(peer), device_id_type=MESH).start()

    def own_part(m, chip, col, width):
        rows = pl.ds(pl.multiple_of(chip * tok, tok), tok)
        return dx_f[m, rows, col:col + width] + precv[m, rows, col:col + width].astype(F32)

    def rs_send_to(m, j, side, d, col, width):
        src = sbuf.at[m, side, d - 1, :, pl.ds(col, width)]
        dst = rbuf.at[m, side, d - 1, :, pl.ds(col, width)]
        pltpu.make_async_remote_copy(src_ref=src, dst_ref=dst, send_sem=rs_send.at[m, j],
                                     recv_sem=rs_recv.at[m, j, d - 1, side],
                                     device_id=to(right if side == 0 else left), device_id_type=MESH).start()

    def chip_at(side, d):
        return lax.rem(z + (d if side == 0 else n_chip - d), n_chip)

    def rs_start(m, j):
        ref = precv.at[m, :, pl.ds(j * rs_w, rs_w)]
        pltpu.make_async_copy(ref, ref, ps_recv.at[m, j]).wait()
        for side in range(2):
            col = j * rs_w + side * rs_h
            sbuf[m, side, half - 1, :, col:col + rs_h] = own_part(m, chip_at(side, half), col, rs_h).astype(BF16)
        for side in range(2):
            rs_send_to(m, j, side, half, j * rs_w + side * rs_h, rs_h)

    def rs_event(m, j, d):
        col = j * rs_w
        for side in range(2):
            rcol, rwidth = (col + side * rs_h, rs_h) if d == half else (col, rs_w)
            ref = rbuf.at[m, side, d - 1, :, pl.ds(rcol, rwidth)]
            pltpu.make_async_copy(ref, ref, rs_recv.at[m, j, d - 1, side]).wait()
        if d == 1:
            total = own_part(m, z, col, rs_w)
            for side in range(2):
                total = total + rbuf[m, side, 0, :, col:col + rs_w].astype(F32)
            dx_own[m, :, col:col + rs_w] = total.astype(BF16)
            return
        for side in range(2):
            chip = chip_at(side, d - 1)
            if d == half:
                a, b = col + side * rs_h, col + (1 - side) * rs_h
                sbuf[m, side, d - 2, :, a:a + rs_h] = (
                    own_part(m, chip, a, rs_h) + rbuf[m, side, d - 1, :, a:a + rs_h].astype(F32)).astype(BF16)
                sbuf[m, side, d - 2, :, b:b + rs_h] = own_part(m, chip, b, rs_h).astype(BF16)
            else:
                sbuf[m, side, d - 2, :, col:col + rs_w] = (
                    own_part(m, chip, col, rs_w)
                    + rbuf[m, side, d - 1, :, col:col + rs_w].astype(F32)).astype(BF16)
        for side in range(2):
            rs_send_to(m, j, side, d - 1, col, rs_w)

    outs = []

    def write_out(src, dst):
        cp = pltpu.make_async_copy(src, dst, out_sem.at[len(outs)])
        cp.start()
        outs.append(cp)

    tensor_cols = [(t, j) for t in range(2) for j in range(n_col)]

    ag_start(0)
    work = [prep_wq] + [functools.partial(prep_kv, i) for i in range(n_kv)] + [kv_swap]
    slots = [(d, t, j) for d in range(1, half) for t, j in tensor_cols]
    for s, (d, t, j) in enumerate(slots):
        ag_event(0, t, j, d)
        if work:
            work.pop(0)()
    for w in work:
        w()
    ag_start(1)
    wo_cp.wait()
    kv_swap_wait()

    def finish_gather(m, extra):
        for t, j in tensor_cols:
            ag_event(m, t, j, half)
            for f in extra.get((t, j), ()):
                f()
            if (t, j) == (0, 0):
                continue
            pt, pj = tensor_cols[tensor_cols.index((t, j)) - 1]
            finish_part(m, pt, pj)
        finish_part(m, *tensor_cols[-1])
        write_out(xb.at[m], xf_out.at[m])
        write_out(dyb.at[m], dyf_out.at[m])

    def finish_part(m, t, j):
        d2d_wait(m, t, j)
        (proj_x if t == 0 else proj_dy)(m, j)
        if j == n_col - 1:
            (round_x if t == 0 else round_dy)()

    def attn_steps(m):
        steps = []
        for h in range(heads):
            steps.append(functools.partial(head, m, h))
            steps.append(functools.partial(head_kv, m, h))
        steps.append(functools.partial(kv_round, m))
        return steps

    finish_gather(0, {})
    work = attn_steps(0) + [functools.partial(dx_chunk, 0, j) for j in range(rs_n)] + [functools.partial(kv_total, 0)]
    for s, (d, t, j) in enumerate(slots):
        ag_event(1, t, j, d)
        if work:
            work.pop(0)()
    for w in work:
        w()
    for j in range(rs_n):
        rs_start(0, j)
    finish_gather(1, {})
    work = attn_steps(1) + [functools.partial(dx_chunk, 1, j) for j in range(rs_n)]
    for d in range(half, 1, -1):
        for j in range(rs_n):
            rs_event(0, j, d)
            if work:
                work.pop(0)()
    for w in work:
        w()
    for j in range(rs_n):
        rs_event(0, j, 1)
        rs_start(1, j)
    write_out(dx_own.at[0], dx_out.at[0])
    kv_total(1)
    for m in range(micro_n):
        write_out(dqb.at[m], dq_out.at[m])
        write_out(dkv_tot.at[m], dkv_out.at[m])
        write_out(ob.at[m], o_out.at[m])
    for d in range(half, 0, -1):
        for j in range(rs_n):
            rs_event(1, j, d)
    write_out(dx_own.at[1], dx_out.at[1])

    for m in range(micro_n):
        for t, j in tensor_cols:
            rows = n_chip - 1
            ref = bufs[t][1].at[m, pl.ds(0, rows * tok), pl.ds(j * col_w, col_w)]
            pltpu.make_async_copy(ref, ref, ag_send.at[m, t, j]).wait()
            ref = peer_blocks(m, t, j, c)
            pltpu.make_async_copy(ref, ref, d2d_send.at[m, t, j]).wait()
        for j in range(rs_n):
            ref = psend.at[m, :, pl.ds(j * rs_w, rs_w)]
            pltpu.make_async_copy(ref, ref, ps_send.at[m, j]).wait()
            ref = psend.at[m, pl.ds(0, (n_chip - 1) * tok), pl.ds(j * rs_w, rs_w)]
            pltpu.make_async_copy(ref, ref, rs_send.at[m, j]).wait()
    for cp in outs:
        cp.wait()


def grad_kernel(heads, col_half, xf, xh, dyf, dq, dkv, o, dwq, dwk, dwv, dwo, tmp):
    micro_n = xf.shape[0]
    head_dim = dkv.shape[2] // 2
    tile = xf.shape[2]
    acc = sum(dot(xf[m], dq[m], TN) for m in range(micro_n))
    for h in range(heads):
        dwq[pl.ds(h, tile, stride=heads), :] = acc[:, h * head_dim:(h + 1) * head_dim]
    acc = sum(dot(xh[m], dkv[m], TN) for m in range(micro_n))
    dwk[...] = acc[:, :head_dim]
    dwv[...] = acc[:, head_dim:]
    dwo[...] = sum(dot(o[m], dyf[m], TN) for m in range(micro_n))


def solution(mesh):
    n_dev = mesh.shape["model"]

    def device_grads(x_loc, dy_loc, w_q, w_k, w_v, w_o):
        micro_n, tok, d_model = x_loc.shape
        heads, head_dim = w_q.shape[1], w_q.shape[2]
        kv_heads = w_k.shape[1]
        n_rows = tok * n_dev
        par_rows = n_rows // 2
        hd = heads * head_dim
        n_chip = n_dev // 2
        half = n_chip // 2
        any_spec = pl.BlockSpec(memory_space=pl.ANY)
        dma = pltpu.SemaphoreType.DMA
        scratch = [
            pltpu.VMEM((micro_n, n_rows, d_model), BF16),
            pltpu.VMEM((micro_n, n_rows, d_model), BF16),
            pltpu.VMEM((d_model, hd), BF16),
            pltpu.VMEM((hd, d_model), BF16),
            pltpu.VMEM((d_model, 2 * head_dim), BF16),
            pltpu.VMEM((d_model * heads, head_dim), BF16),
            pltpu.VMEM((2, d_model * kv_heads // 8, head_dim), BF16),
            pltpu.VMEM((512, head_dim), F32),
            pltpu.VMEM((n_rows, hd), F32),
            pltpu.VMEM((n_rows, 2 * head_dim), F32),
            pltpu.VMEM((n_rows, hd), F32),
            pltpu.VMEM((n_rows, hd), BF16),
            pltpu.VMEM((n_rows, 2 * head_dim), BF16),
            pltpu.VMEM((n_rows, hd), BF16),
            pltpu.VMEM((micro_n, n_rows, hd), BF16),
            pltpu.VMEM((micro_n, n_rows, hd), BF16),
            pltpu.VMEM((n_rows, 2 * head_dim), BF16),
            pltpu.VMEM((heads, n_rows, n_rows), BF16),
            pltpu.VMEM((heads, n_rows, n_rows), BF16),
            pltpu.VMEM((micro_n, n_rows, 2 * head_dim), F32),
            pltpu.VMEM((micro_n, n_rows, 2 * head_dim), F32),
            pltpu.VMEM((micro_n, n_rows, 2 * head_dim), BF16),
            pltpu.VMEM((micro_n, par_rows, d_model), F32),
            pltpu.VMEM((n_rows, d_model // 4), F32),
            pltpu.VMEM((micro_n, par_rows, d_model), BF16),
            pltpu.VMEM((micro_n, par_rows, d_model), BF16),
            pltpu.VMEM((micro_n, 2, half, tok, d_model), BF16),
            pltpu.VMEM((micro_n, 2, half, tok, d_model), BF16),
            pltpu.VMEM((micro_n, tok, d_model), BF16),
            dma((micro_n, 2)), dma((2,)), dma((2,)), dma((6 * micro_n,)),
            dma((micro_n, 2, 2)), dma((micro_n, 2, 2, half, 2)),
            dma((micro_n, 2, 2)), dma((micro_n, 2, 2)), dma((2,)),
            dma((micro_n, 2)), dma((micro_n, 4)), dma((micro_n, 4)),
            dma((micro_n, 4)), dma((micro_n, 4, half, 2)),
        ]
        dx, xf, dyf, dq, dkv, o = pl.pallas_call(
            functools.partial(attn_kernel, n_dev, kv_heads),
            out_shape=(
                jax.ShapeDtypeStruct((micro_n, tok, d_model), BF16),
                jax.ShapeDtypeStruct((micro_n, n_rows, d_model), BF16),
                jax.ShapeDtypeStruct((micro_n, n_rows, d_model), BF16),
                jax.ShapeDtypeStruct((micro_n, n_rows, hd), BF16),
                jax.ShapeDtypeStruct((micro_n, n_rows, 2 * head_dim), BF16),
                jax.ShapeDtypeStruct((micro_n, n_rows, hd), BF16),
            ),
            in_specs=[any_spec] * 6,
            out_specs=(any_spec,) * 6,
            scratch_shapes=scratch,
            compiler_params=pltpu.CompilerParams(collective_id=0, has_side_effects=True,
                                                 vmem_limit_bytes=60 * 1024 * 1024),
        )(x_loc, dy_loc, w_q.reshape(d_model * heads, head_dim), w_k.reshape(d_model * kv_heads, head_dim),
          w_v.reshape(d_model * kv_heads, head_dim), w_o.reshape(hd, d_model))

        core = (lax.axis_index("model") % 2).astype(jnp.int32).reshape(1)
        steps = 10
        tile = d_model // steps
        half_tile = tile // 2
        full = lambda i, s: (0, 0, 0)
        dwq, dwk, dwv, dwo = pl.pallas_call(
            lambda s, *refs: grad_kernel(heads, half_tile, *refs, None),
            grid_spec=pltpu.PrefetchScalarGridSpec(
                num_scalar_prefetch=1,
                grid=(steps,),
                in_specs=[
                    pl.BlockSpec((micro_n, n_rows, tile), lambda i, s: (0, 0, i)),
                    pl.BlockSpec((micro_n, n_rows, half_tile), lambda i, s: (0, 0, s[0] * steps + i)),
                    pl.BlockSpec((micro_n, n_rows, tile), lambda i, s: (0, 0, i)),
                    pl.BlockSpec((micro_n, n_rows, hd), full),
                    pl.BlockSpec((micro_n, n_rows, 2 * head_dim), full),
                    pl.BlockSpec((micro_n, n_rows, hd), full),
                ],
                out_specs=[
                    pl.BlockSpec((tile * heads, head_dim), lambda i, s: (i, 0)),
                    pl.BlockSpec((half_tile, head_dim), lambda i, s: (i, 0)),
                    pl.BlockSpec((half_tile, head_dim), lambda i, s: (i, 0)),
                    pl.BlockSpec((hd, tile), lambda i, s: (0, i)),
                ],
            ),
            out_shape=(
                jax.ShapeDtypeStruct((d_model * heads, head_dim), F32),
                jax.ShapeDtypeStruct((d_model // 2, head_dim), F32),
                jax.ShapeDtypeStruct((d_model // 2, head_dim), F32),
                jax.ShapeDtypeStruct((hd, d_model), F32),
            ),
        )(core, xf, xf, dyf, dq, dkv, o)
        return dx, dwq.reshape(d_model, heads, head_dim), dwk, dwv, dwo.reshape(heads, head_dim, d_model)

    return jax.shard_map(
        device_grads, mesh=mesh,
        in_specs=(P("data", "model", None), P("data", "model", None), P(None, "model", None),
                  P(None, None, None), P(None, None, None), P("model", None, None)),
        out_specs=(P("data", "model", None), P("data", "model", None), P(("data", "model"), None),
                   P(("data", "model"), None), P(("data", "model"), None, None)),
        check_vma=False)
```

```python
import functools

import jax
import jax.numpy as jnp
from jax import lax
from jax.experimental import pallas as pl
from jax.experimental.pallas import tpu as pltpu
from jax.sharding import PartitionSpec as P

BF16 = jnp.bfloat16
F32 = jnp.float32
MESH = pl.DeviceIdType.MESH

NT = (((1,), (1,)), ((), ()))
NN = (((1,), (0,)), ((), ()))
TN = (((0,), (0,)), ((), ()))


def dot(a, b, dims=NN):
    return lax.dot_general(a, b, dims, preferred_element_type=F32)


def attn_kernel(n_dev, kv_heads, x_in, dy_in, wq_in, wk_in, wv_in, wo_in,
                dx_out, dwq, dwk, dwv, dwo,
                xb, dyb, wq, wo, wkv, stage_q, stage_kv, unpacked,
                acc_q, acc_kv, acc_do, qb, kvb, dob, ob, dqb, dkvp, prob_b, ds_b,
                dkv_f, dkv_peer, dkv_tot,
                dx_f, dx_tmp, psend, precv, sbuf, rbuf, dx_own,
                own_sem, w_sem, kvw_sem, out_sem,
                ag_send, ag_recv, d2d_send, d2d_recv, wx_sem,
                dkv_sem, ps_send, ps_recv, rs_send, rs_recv):
    n_chip = n_dev // 2
    half = n_chip // 2
    micro_n, tok, d_model = x_in.shape
    head_dim = wk_in.shape[1]
    heads = wq.shape[1] // head_dim
    n_rows = n_dev * tok
    par_rows = n_rows // 2
    me = lax.axis_index("model")
    z, c = me // 2, me % 2
    right = lax.rem(me + 2, n_dev)
    left = lax.rem(me + n_dev - 2, n_dev)
    peer = z * 2 + (1 - c)
    scale = head_dim ** -0.5

    def to(dev):
        return {"model": dev}

    bufs = ((x_in, xb), (dy_in, dyb))
    my_row = pl.multiple_of(c * par_rows + z * tok, tok)
    own = []
    for m in range(micro_n):
        for t, (src, buf) in enumerate(bufs):
            cp = pltpu.make_async_copy(src.at[m], buf.at[m, pl.ds(my_row, tok)], own_sem.at[m, t])
            cp.start()
            own.append(cp)
    wq_cp = pltpu.make_async_copy(wq_in, stage_q, w_sem.at[0])
    wq_cp.start()
    wo_cp = pltpu.make_async_copy(wo_in, wo, w_sem.at[1])
    wo_cp.start()
    kv_rows = stage_kv.shape[1]
    n_kv = wk_in.shape[0] // kv_rows

    def kv_load(i):
        @pl.when(c == 0)
        def _():
            pltpu.make_async_copy(wk_in.at[pl.ds(i * kv_rows, kv_rows)], stage_kv.at[i % 2], kvw_sem.at[i % 2]).start()

        @pl.when(c == 1)
        def _():
            pltpu.make_async_copy(wv_in.at[pl.ds(i * kv_rows, kv_rows)], stage_kv.at[i % 2], kvw_sem.at[i % 2]).start()

    kv_load(0)
    kv_load(1)

    barrier = pltpu.get_barrier_semaphore()
    for dev in (left, right, peer):
        pl.semaphore_signal(barrier, inc=1, device_id=to(dev), device_id_type=MESH)
    pl.semaphore_wait(barrier, 3)

    n_col = 2
    col_w = d_model // n_col
    sub_w = col_w // 2

    def blk(m, t, chip, col, width, core=None):
        row = pl.multiple_of((c if core is None else core) * par_rows + chip * tok, tok)
        return bufs[t][1].at[m, pl.ds(row, tok), pl.ds(col, width)]

    def send(ref, dev, ssem, rsem):
        pltpu.make_async_remote_copy(src_ref=ref, dst_ref=ref, send_sem=ssem, recv_sem=rsem,
                                     device_id=to(dev), device_id_type=MESH).start()

    def ag_start(m):
        for t in range(2):
            own[m * 2 + t].wait()
        for t in range(2):
            for j in range(n_col):
                ref = blk(m, t, z, j * col_w, col_w)
                send(ref, right, ag_send.at[m, t, j], ag_recv.at[m, t, j, 0, 0])
                send(ref, left, ag_send.at[m, t, j], ag_recv.at[m, t, j, 0, 1])
                send(ref, peer, d2d_send.at[m, t, j], d2d_recv.at[m, t, j])

    def ag_event(m, t, j, d):
        last = d == half
        for side in range(2):
            chip = lax.rem(z + (n_chip - d if side == 0 else d), n_chip)
            col, width = (j * col_w, col_w) if not last else (j * col_w + side * sub_w, sub_w)
            ref = blk(m, t, chip, col, width)
            pltpu.make_async_copy(ref, ref, ag_recv.at[m, t, j, d - 1, side]).wait()
            if d < half - 1:
                fwd = ref
            elif d == half - 1:
                fwd = blk(m, t, chip, j * col_w + side * sub_w, sub_w)
            else:
                fwd = None
            if fwd is not None:
                send(fwd, right if side == 0 else left, ag_send.at[m, t, j], ag_recv.at[m, t, j, d, side])
            send(ref, peer, d2d_send.at[m, t, j], d2d_recv.at[m, t, j])

    def peer_blocks(m, t, j, core):
        row = pl.multiple_of(core * par_rows, par_rows)
        return bufs[t][1].at[m, pl.ds(row, par_rows), pl.ds(j * col_w, col_w)]

    def d2d_wait(m, t, j):
        ref = peer_blocks(m, t, j, 1 - c)
        pltpu.make_async_copy(ref, ref, d2d_recv.at[m, t, j]).wait()

    un_rows = unpacked.shape[0]

    def prep_wq():
        wq_cp.wait()
        per = un_rows // heads

        def body(i, _):
            unpacked[...] = stage_q[pl.ds(pl.multiple_of(i * un_rows, un_rows), un_rows), :].astype(F32)
            for h in range(heads):
                wq[pl.ds(pl.multiple_of(i * per, per), per), h * head_dim:(h + 1) * head_dim] = (
                    unpacked[pl.ds(h, per, stride=heads), :].astype(BF16))
            return 0

        lax.fori_loop(0, stage_q.shape[0] // un_rows, body, 0)

    kv_col = pl.multiple_of(c * head_dim, head_dim)

    def prep_kv(i):
        pltpu.make_async_copy(wk_in.at[pl.ds(i * kv_rows, kv_rows)], stage_kv.at[i % 2], kvw_sem.at[i % 2]).wait()
        per = un_rows // kv_heads
        base = i * (kv_rows // kv_heads)

        def body(k, _):
            unpacked[...] = stage_kv[i % 2, pl.ds(pl.multiple_of(k * un_rows, un_rows), un_rows), :].astype(F32)
            wkv[pl.ds(pl.multiple_of(base + k * per, per), per), pl.ds(kv_col, head_dim)] = (
                unpacked[pl.ds(z, per, stride=kv_heads), :].astype(BF16))
            return 0

        lax.fori_loop(0, kv_rows // un_rows, body, 0)
        if i + 2 < n_kv:
            kv_load(i + 2)

    def kv_swap():
        ref = wkv.at[:, pl.ds(kv_col, head_dim)]
        pltpu.make_async_remote_copy(src_ref=ref, dst_ref=ref, send_sem=wx_sem.at[0], recv_sem=wx_sem.at[1],
                                     device_id=to(peer), device_id_type=MESH).start()

    def kv_swap_wait():
        ref = wkv.at[:, pl.ds(kv_col, head_dim)]
        pltpu.make_async_copy(ref, ref, wx_sem.at[0]).wait()
        ref = wkv.at[:, pl.ds(pl.multiple_of((1 - c) * head_dim, head_dim), head_dim)]
        pltpu.make_async_copy(ref, ref, wx_sem.at[1]).wait()

    def proj_x(m, j):
        for k in range(2):
            cols = slice(j * col_w + k * sub_w, j * col_w + (k + 1) * sub_w)
            a = dot(xb[m, :, cols], wq[cols, :])
            b = dot(xb[m, :, cols], wkv[cols, :])
            if j == 0 and k == 0:
                acc_q[...] = a
                acc_kv[...] = b
            else:
                acc_q[...] += a
                acc_kv[...] += b

    def proj_dy(m, j):
        for k in range(2):
            cols = slice(j * col_w + k * sub_w, j * col_w + (k + 1) * sub_w)
            a = dot(dyb[m, :, cols], wo[:, cols], NT)
            if j == 0 and k == 0:
                acc_do[...] = a
            else:
                acc_do[...] += a

    def round_x():
        qb[...] = acc_q[...].astype(BF16)
        kvb[...] = acc_kv[...].astype(BF16)

    def round_dy():
        dob[...] = acc_do[...].astype(BF16)

    def position(axis):
        r = lax.broadcasted_iota(jnp.int32, (n_rows, 1) if axis == 0 else (1, n_rows), axis)
        inner = r % par_rows
        return (inner // tok) * (2 * tok) + (r // par_rows) * tok + inner % tok

    def head(m, h):
        cols = slice(h * head_dim, (h + 1) * head_dim)
        q, k, v = qb[:, cols], kvb[:, :head_dim], kvb[:, head_dim:]
        do = dob[:, cols]
        s = dot(q, k, NT) * scale
        s = jnp.where(position(0) >= position(1), s, -jnp.inf)
        e = jnp.exp(s - jnp.max(s, axis=-1, keepdims=True))
        p = e / jnp.sum(e, axis=-1, keepdims=True)
        pb = p.astype(BF16)
        o = dot(pb, v).astype(BF16)
        ob[m, :, cols] = o
        dp = dot(do, v, NT)
        delta = jnp.sum(do.astype(F32) * o.astype(F32), axis=-1, keepdims=True)
        ds = (p * (dp - delta)).astype(BF16)
        prob_b[h] = pb
        ds_b[h] = ds
        dqb[m, :, cols] = (dot(ds, k) * scale).astype(BF16)

    def head_kv(m, h):
        cols = slice(h * head_dim, (h + 1) * head_dim)
        dk = dot(ds_b[h], qb[:, cols], TN) * scale
        dv = dot(prob_b[h], dob[:, cols], TN)
        if h == 0:
            dkv_f[m, :, :head_dim] = dk
            dkv_f[m, :, head_dim:] = dv
        else:
            dkv_f[m, :, :head_dim] += dk
            dkv_f[m, :, head_dim:] += dv

    def kv_round(m):
        dkvp[...] = dkv_f[m].astype(BF16)
        pltpu.make_async_remote_copy(src_ref=dkv_f.at[m], dst_ref=dkv_peer.at[m], send_sem=dkv_sem.at[m, 0],
                                     recv_sem=dkv_sem.at[m, 1], device_id=to(peer), device_id_type=MESH).start()

    def kv_total(m):
        pltpu.make_async_copy(dkv_f.at[m], dkv_f.at[m], dkv_sem.at[m, 0]).wait()
        pltpu.make_async_copy(dkv_peer.at[m], dkv_peer.at[m], dkv_sem.at[m, 1]).wait()
        dkv_tot[m] = (dkv_f[m] + dkv_peer[m]).astype(BF16)

    dw_n = 4
    dw_w = d_model // dw_n

    def put(ref, idx, val, m):
        if m == 0:
            ref[idx] = val
        else:
            ref[idx] += val

    def dw_x(m, i):
        ck = lax.rem(c * (dw_n // 2) + i, dw_n)
        start = pl.multiple_of(ck * dw_w, dw_w)
        xt = xb[m, :, pl.ds(start, dw_w)].T
        g = dot(xt, dqb[m])
        for h in range(heads):
            put(dwq, (pl.ds(start * heads + h, dw_w, stride=heads), slice(None)),
                g[:, h * head_dim:(h + 1) * head_dim], m)
        if i < dw_n // 2:
            g = dot(xt, dkv_tot[m])
            rows = slice(i * dw_w, (i + 1) * dw_w)
            put(dwk, (rows, slice(None)), g[:, :head_dim], m)
            put(dwv, (rows, slice(None)), g[:, head_dim:], m)

    def dw_o(m, i):
        cols = slice(i * dw_w, (i + 1) * dw_w)
        put(dwo, (slice(None), cols), dot(ob[m], dyb[m, :, cols], TN), m)

    def dw_steps(m):
        return ([functools.partial(dw_o, m, i) for i in range(dw_n)]
                + [functools.partial(dw_x, m, i) for i in range(dw_n)])

    rs_n = 4
    rs_w = d_model // rs_n
    rs_h = rs_w // 2

    def dx_chunk(m, j):
        cols = slice(j * rs_w, (j + 1) * rs_w)
        dx_tmp[...] = dot(dqb[m], wq[cols, :], NT) + dot(dkvp[...], wkv[cols, :], NT)
        away = pl.ds(pl.multiple_of((1 - c) * par_rows, par_rows), par_rows)
        keep = pl.ds(pl.multiple_of(c * par_rows, par_rows), par_rows)
        psend[m, :, cols] = dx_tmp[away, :].astype(BF16)
        dx_f[m, :, cols] = dx_tmp[keep, :]
        pltpu.make_async_remote_copy(src_ref=psend.at[m, :, cols], dst_ref=precv.at[m, :, cols],
                                     send_sem=ps_send.at[m, j], recv_sem=ps_recv.at[m, j],
                                     device_id=to(peer), device_id_type=MESH).start()

    def own_part(m, chip, col, width):
        rows = pl.ds(pl.multiple_of(chip * tok, tok), tok)
        return dx_f[m, rows, col:col + width] + precv[m, rows, col:col + width].astype(F32)

    def rs_send_to(m, j, side, d, col, width):
        src = sbuf.at[m, side, d - 1, :, pl.ds(col, width)]
        dst = rbuf.at[m, side, d - 1, :, pl.ds(col, width)]
        pltpu.make_async_remote_copy(src_ref=src, dst_ref=dst, send_sem=rs_send.at[m, j],
                                     recv_sem=rs_recv.at[m, j, d - 1, side],
                                     device_id=to(right if side == 0 else left), device_id_type=MESH).start()

    def chip_at(side, d):
        return lax.rem(z + (d if side == 0 else n_chip - d), n_chip)

    def rs_start(m, j):
        ref = precv.at[m, :, pl.ds(j * rs_w, rs_w)]
        pltpu.make_async_copy(ref, ref, ps_recv.at[m, j]).wait()
        for side in range(2):
            col = j * rs_w + side * rs_h
            sbuf[m, side, half - 1, :, col:col + rs_h] = own_part(m, chip_at(side, half), col, rs_h).astype(BF16)
        for side in range(2):
            rs_send_to(m, j, side, half, j * rs_w + side * rs_h, rs_h)

    def rs_event(m, j, d):
        col = j * rs_w
        for side in range(2):
            rcol, rwidth = (col + side * rs_h, rs_h) if d == half else (col, rs_w)
            ref = rbuf.at[m, side, d - 1, :, pl.ds(rcol, rwidth)]
            pltpu.make_async_copy(ref, ref, rs_recv.at[m, j, d - 1, side]).wait()
        if d == 1:
            total = own_part(m, z, col, rs_w)
            for side in range(2):
                total = total + rbuf[m, side, 0, :, col:col + rs_w].astype(F32)
            dx_own[m, :, col:col + rs_w] = total.astype(BF16)
            return
        for side in range(2):
            chip = chip_at(side, d - 1)
            if d == half:
                a, b = col + side * rs_h, col + (1 - side) * rs_h
                sbuf[m, side, d - 2, :, a:a + rs_h] = (
                    own_part(m, chip, a, rs_h) + rbuf[m, side, d - 1, :, a:a + rs_h].astype(F32)).astype(BF16)
                sbuf[m, side, d - 2, :, b:b + rs_h] = own_part(m, chip, b, rs_h).astype(BF16)
            else:
                sbuf[m, side, d - 2, :, col:col + rs_w] = (
                    own_part(m, chip, col, rs_w)
                    + rbuf[m, side, d - 1, :, col:col + rs_w].astype(F32)).astype(BF16)
        for side in range(2):
            rs_send_to(m, j, side, d - 1, col, rs_w)

    outs = []

    def write_out(src, dst):
        cp = pltpu.make_async_copy(src, dst, out_sem.at[len(outs)])
        cp.start()
        outs.append(cp)

    tensor_cols = [(t, j) for t in range(2) for j in range(n_col)]

    ag_start(0)
    work = [prep_wq] + [functools.partial(prep_kv, i) for i in range(n_kv)] + [kv_swap]
    slots = [(d, t, j) for d in range(1, half) for t, j in tensor_cols]
    for s, (d, t, j) in enumerate(slots):
        ag_event(0, t, j, d)
        if work:
            work.pop(0)()
    for w in work:
        w()
    ag_start(1)
    wo_cp.wait()
    kv_swap_wait()

    def finish_gather(m, extra):
        for t, j in tensor_cols:
            ag_event(m, t, j, half)
            for f in extra.get((t, j), ()):
                f()
            if (t, j) == (0, 0):
                continue
            pt, pj = tensor_cols[tensor_cols.index((t, j)) - 1]
            finish_part(m, pt, pj)
        finish_part(m, *tensor_cols[-1])

    def finish_part(m, t, j):
        d2d_wait(m, t, j)
        (proj_x if t == 0 else proj_dy)(m, j)
        if j == n_col - 1:
            (round_x if t == 0 else round_dy)()

    def attn_steps(m):
        steps = []
        for h in range(heads):
            steps.append(functools.partial(head, m, h))
            steps.append(functools.partial(head_kv, m, h))
        steps.append(functools.partial(kv_round, m))
        return steps

    finish_gather(0, {})
    work = attn_steps(0) + [functools.partial(dx_chunk, 0, j) for j in range(rs_n)]
    later = [functools.partial(kv_total, 0)] + dw_steps(0)
    for d, t, j in slots:
        ag_event(1, t, j, d)
        (work or later).pop(0)()
    for j in range(rs_n):
        rs_start(0, j)
    finish_gather(1, {})
    work = attn_steps(1) + [functools.partial(dx_chunk, 1, j) for j in range(rs_n)]
    for d in range(half, 1, -1):
        for j in range(rs_n):
            rs_event(0, j, d)
            (work or later).pop(0)()
    for j in range(rs_n):
        rs_start(1, j)
    later += [functools.partial(kv_total, 1)] + dw_steps(1)
    for j in range(rs_n):
        rs_event(0, j, 1)
        later.pop(0)()
    write_out(dx_own.at[0], dx_out.at[0])
    for d in range(half, 0, -1):
        for j in range(rs_n):
            rs_event(1, j, d)
            if later:
                later.pop(0)()
    write_out(dx_own.at[1], dx_out.at[1])

    for m in range(micro_n):
        for t, j in tensor_cols:
            rows = n_chip - 1
            ref = bufs[t][1].at[m, pl.ds(0, rows * tok), pl.ds(j * col_w, col_w)]
            pltpu.make_async_copy(ref, ref, ag_send.at[m, t, j]).wait()
            ref = peer_blocks(m, t, j, c)
            pltpu.make_async_copy(ref, ref, d2d_send.at[m, t, j]).wait()
        for j in range(rs_n):
            ref = psend.at[m, :, pl.ds(j * rs_w, rs_w)]
            pltpu.make_async_copy(ref, ref, ps_send.at[m, j]).wait()
            ref = psend.at[m, pl.ds(0, (n_chip - 1) * tok), pl.ds(j * rs_w, rs_w)]
            pltpu.make_async_copy(ref, ref, rs_send.at[m, j]).wait()
    for cp in outs:
        cp.wait()


def solution(mesh):
    n_dev = mesh.shape["model"]

    def device_grads(x_loc, dy_loc, w_q, w_k, w_v, w_o):
        micro_n, tok, d_model = x_loc.shape
        heads, head_dim = w_q.shape[1], w_q.shape[2]
        kv_heads = w_k.shape[1]
        n_rows = tok * n_dev
        par_rows = n_rows // 2
        hd = heads * head_dim
        n_chip = n_dev // 2
        half = n_chip // 2
        any_spec = pl.BlockSpec(memory_space=pl.ANY)
        dma = pltpu.SemaphoreType.DMA
        scratch = [
            pltpu.VMEM((micro_n, n_rows, d_model), BF16),
            pltpu.VMEM((micro_n, n_rows, d_model), BF16),
            pltpu.VMEM((d_model, hd), BF16),
            pltpu.VMEM((hd, d_model), BF16),
            pltpu.VMEM((d_model, 2 * head_dim), BF16),
            pltpu.VMEM((d_model * heads, head_dim), BF16),
            pltpu.VMEM((2, d_model * kv_heads // 8, head_dim), BF16),
            pltpu.VMEM((512, head_dim), F32),
            pltpu.VMEM((n_rows, hd), F32),
            pltpu.VMEM((n_rows, 2 * head_dim), F32),
            pltpu.VMEM((n_rows, hd), F32),
            pltpu.VMEM((n_rows, hd), BF16),
            pltpu.VMEM((n_rows, 2 * head_dim), BF16),
            pltpu.VMEM((n_rows, hd), BF16),
            pltpu.VMEM((micro_n, n_rows, hd), BF16),
            pltpu.VMEM((micro_n, n_rows, hd), BF16),
            pltpu.VMEM((n_rows, 2 * head_dim), BF16),
            pltpu.VMEM((heads, n_rows, n_rows), BF16),
            pltpu.VMEM((heads, n_rows, n_rows), BF16),
            pltpu.VMEM((micro_n, n_rows, 2 * head_dim), F32),
            pltpu.VMEM((micro_n, n_rows, 2 * head_dim), F32),
            pltpu.VMEM((micro_n, n_rows, 2 * head_dim), BF16),
            pltpu.VMEM((micro_n, par_rows, d_model), F32),
            pltpu.VMEM((n_rows, d_model // 4), F32),
            pltpu.VMEM((micro_n, par_rows, d_model), BF16),
            pltpu.VMEM((micro_n, par_rows, d_model), BF16),
            pltpu.VMEM((micro_n, 2, half, tok, d_model), BF16),
            pltpu.VMEM((micro_n, 2, half, tok, d_model), BF16),
            pltpu.VMEM((micro_n, tok, d_model), BF16),
            dma((micro_n, 2)), dma((2,)), dma((2,)), dma((6 * micro_n,)),
            dma((micro_n, 2, 2)), dma((micro_n, 2, 2, half, 2)),
            dma((micro_n, 2, 2)), dma((micro_n, 2, 2)), dma((2,)),
            dma((micro_n, 2)), dma((micro_n, 4)), dma((micro_n, 4)),
            dma((micro_n, 4)), dma((micro_n, 4, half, 2)),
        ]
        dx, dwq, dwk, dwv, dwo = pl.pallas_call(
            functools.partial(attn_kernel, n_dev, kv_heads),
            out_shape=(
                jax.ShapeDtypeStruct((micro_n, tok, d_model), BF16),
                pltpu.VMEM((d_model * heads, head_dim), F32),
                pltpu.VMEM((d_model // 2, head_dim), F32),
                pltpu.VMEM((d_model // 2, head_dim), F32),
                pltpu.VMEM((hd, d_model), F32),
            ),
            in_specs=[any_spec] * 6,
            out_specs=(any_spec,) + (pl.BlockSpec(memory_space=pltpu.VMEM),) * 4,
            scratch_shapes=scratch,
            compiler_params=pltpu.CompilerParams(collective_id=0, has_side_effects=True,
                                                 vmem_limit_bytes=46 * 1024 * 1024),
        )(x_loc, dy_loc, w_q.reshape(d_model * heads, head_dim), w_k.reshape(d_model * kv_heads, head_dim),
          w_v.reshape(d_model * kv_heads, head_dim), w_o.reshape(hd, d_model))

        return dx, dwq.reshape(d_model, heads, head_dim), dwk, dwv, dwo.reshape(heads, head_dim, d_model)

    return jax.shard_map(
        device_grads, mesh=mesh,
        in_specs=(P("data", "model", None), P("data", "model", None), P(None, "model", None),
                  P(None, None, None), P(None, None, None), P("model", None, None)),
        out_specs=(P("data", "model", None), P("data", "model", None), P(("data", "model"), None),
                   P(("data", "model"), None), P(("data", "model"), None, None)),
        check_vma=False)
```

```python
import functools

import jax
import jax.numpy as jnp
from jax import lax
from jax.experimental import pallas as pl
from jax.experimental.pallas import tpu as pltpu
from jax.sharding import PartitionSpec as P

BF16 = jnp.bfloat16
F32 = jnp.float32
MESH = pl.DeviceIdType.MESH

NT = (((1,), (1,)), ((), ()))
NN = (((1,), (0,)), ((), ()))
TN = (((0,), (0,)), ((), ()))


def dot(a, b, dims=NN):
    return lax.dot_general(a, b, dims, preferred_element_type=F32)


def attn_kernel(n_dev, kv_heads, x_in, dy_in, wq_in, wk_in, wv_in, wo_in,
                dx_own, dwq, dwk, dwv, dwo,
                xb, dyb, wq, wo, wkv, stage_q, stage_kv, unpacked,
                acc_q, acc_kv, acc_do, qb, kvb, dob, ob, dqb, dkvp, prob_b, ds_b,
                dkv_f, dkv_peer, dkv_tot,
                dx_f, dx_tmp, psend, precv, sbuf, rbuf,
                own_sem, w_sem, kvw_sem,
                ag_send, ag_recv, d2d_send, d2d_recv, wx_sem,
                dkv_sem, ps_send, ps_recv, rs_send, rs_recv):
    n_chip = n_dev // 2
    half = n_chip // 2
    micro_n, tok, d_model = x_in.shape
    head_dim = wk_in.shape[1]
    heads = wq.shape[1] // head_dim
    n_rows = n_dev * tok
    par_rows = n_rows // 2
    me = lax.axis_index("model")
    z, c = me // 2, me % 2
    right = lax.rem(me + 2, n_dev)
    left = lax.rem(me + n_dev - 2, n_dev)
    peer = z * 2 + (1 - c)
    scale = head_dim ** -0.5

    def to(dev):
        return {"model": dev}

    bufs = ((x_in, xb), (dy_in, dyb))
    my_row = pl.multiple_of(c * par_rows + z * tok, tok)
    own = []
    for m in range(micro_n):
        for t, (src, buf) in enumerate(bufs):
            cp = pltpu.make_async_copy(src.at[m], buf.at[m, pl.ds(my_row, tok)], own_sem.at[m, t])
            cp.start()
            own.append(cp)
    wq_cp = pltpu.make_async_copy(wq_in, stage_q, w_sem.at[0])
    wq_cp.start()
    wo_cp = pltpu.make_async_copy(wo_in, wo, w_sem.at[1])
    wo_cp.start()
    kv_rows = stage_kv.shape[1]
    n_kv = wk_in.shape[0] // kv_rows

    def kv_load(i):
        @pl.when(c == 0)
        def _():
            pltpu.make_async_copy(wk_in.at[pl.ds(i * kv_rows, kv_rows)], stage_kv.at[i % 2], kvw_sem.at[i % 2]).start()

        @pl.when(c == 1)
        def _():
            pltpu.make_async_copy(wv_in.at[pl.ds(i * kv_rows, kv_rows)], stage_kv.at[i % 2], kvw_sem.at[i % 2]).start()

    kv_load(0)
    kv_load(1)

    barrier = pltpu.get_barrier_semaphore()
    for dev in (left, right, peer):
        pl.semaphore_signal(barrier, inc=1, device_id=to(dev), device_id_type=MESH)
    pl.semaphore_wait(barrier, 3)

    n_col = 2
    col_w = d_model // n_col
    sub_w = col_w // 2

    def blk(m, t, chip, col, width, core=None):
        row = pl.multiple_of((c if core is None else core) * par_rows + chip * tok, tok)
        return bufs[t][1].at[m, pl.ds(row, tok), pl.ds(col, width)]

    def send(ref, dev, ssem, rsem):
        pltpu.make_async_remote_copy(src_ref=ref, dst_ref=ref, send_sem=ssem, recv_sem=rsem,
                                     device_id=to(dev), device_id_type=MESH).start()

    def ag_start(m):
        for t in range(2):
            own[m * 2 + t].wait()
        for t in range(2):
            for j in range(n_col):
                ref = blk(m, t, z, j * col_w, col_w)
                send(ref, right, ag_send.at[m, t, j], ag_recv.at[m, t, j, 0, 0])
                send(ref, left, ag_send.at[m, t, j], ag_recv.at[m, t, j, 0, 1])
                send(ref, peer, d2d_send.at[m, t, j], d2d_recv.at[m, t, j])

    def ag_event(m, t, j, d):
        last = d == half
        for side in range(2):
            chip = lax.rem(z + (n_chip - d if side == 0 else d), n_chip)
            col, width = (j * col_w, col_w) if not last else (j * col_w + side * sub_w, sub_w)
            ref = blk(m, t, chip, col, width)
            pltpu.make_async_copy(ref, ref, ag_recv.at[m, t, j, d - 1, side]).wait()
            if d < half - 1:
                fwd = ref
            elif d == half - 1:
                fwd = blk(m, t, chip, j * col_w + side * sub_w, sub_w)
            else:
                fwd = None
            if fwd is not None:
                send(fwd, right if side == 0 else left, ag_send.at[m, t, j], ag_recv.at[m, t, j, d, side])
            send(ref, peer, d2d_send.at[m, t, j], d2d_recv.at[m, t, j])

    def peer_blocks(m, t, j, core):
        row = pl.multiple_of(core * par_rows, par_rows)
        return bufs[t][1].at[m, pl.ds(row, par_rows), pl.ds(j * col_w, col_w)]

    def d2d_wait(m, t, j):
        ref = peer_blocks(m, t, j, 1 - c)
        pltpu.make_async_copy(ref, ref, d2d_recv.at[m, t, j]).wait()

    un_rows = unpacked.shape[0]

    def prep_wq():
        wq_cp.wait()
        per = un_rows // heads

        def body(i, _):
            unpacked[...] = stage_q[pl.ds(pl.multiple_of(i * un_rows, un_rows), un_rows), :].astype(F32)
            for h in range(heads):
                wq[pl.ds(pl.multiple_of(i * per, per), per), h * head_dim:(h + 1) * head_dim] = (
                    unpacked[pl.ds(h, per, stride=heads), :].astype(BF16))
            return 0

        lax.fori_loop(0, stage_q.shape[0] // un_rows, body, 0)

    kv_col = pl.multiple_of(c * head_dim, head_dim)

    def prep_kv(i):
        pltpu.make_async_copy(wk_in.at[pl.ds(i * kv_rows, kv_rows)], stage_kv.at[i % 2], kvw_sem.at[i % 2]).wait()
        per = un_rows // kv_heads
        base = i * (kv_rows // kv_heads)

        def body(k, _):
            unpacked[...] = stage_kv[i % 2, pl.ds(pl.multiple_of(k * un_rows, un_rows), un_rows), :].astype(F32)
            wkv[pl.ds(pl.multiple_of(base + k * per, per), per), pl.ds(kv_col, head_dim)] = (
                unpacked[pl.ds(z, per, stride=kv_heads), :].astype(BF16))
            return 0

        lax.fori_loop(0, kv_rows // un_rows, body, 0)
        if i + 2 < n_kv:
            kv_load(i + 2)

    def kv_swap():
        ref = wkv.at[:, pl.ds(kv_col, head_dim)]
        pltpu.make_async_remote_copy(src_ref=ref, dst_ref=ref, send_sem=wx_sem.at[0], recv_sem=wx_sem.at[1],
                                     device_id=to(peer), device_id_type=MESH).start()

    def kv_swap_wait():
        ref = wkv.at[:, pl.ds(kv_col, head_dim)]
        pltpu.make_async_copy(ref, ref, wx_sem.at[0]).wait()
        ref = wkv.at[:, pl.ds(pl.multiple_of((1 - c) * head_dim, head_dim), head_dim)]
        pltpu.make_async_copy(ref, ref, wx_sem.at[1]).wait()

    def proj_x(m, j):
        for k in range(2):
            cols = slice(j * col_w + k * sub_w, j * col_w + (k + 1) * sub_w)
            a = dot(xb[m, :, cols], wq[cols, :])
            b = dot(xb[m, :, cols], wkv[cols, :])
            if j == 0 and k == 0:
                acc_q[...] = a
                acc_kv[...] = b
            else:
                acc_q[...] += a
                acc_kv[...] += b

    def proj_dy(m, j):
        for k in range(2):
            cols = slice(j * col_w + k * sub_w, j * col_w + (k + 1) * sub_w)
            a = dot(dyb[m, :, cols], wo[:, cols], NT)
            if j == 0 and k == 0:
                acc_do[...] = a
            else:
                acc_do[...] += a

    def round_x():
        qb[...] = acc_q[...].astype(BF16)
        kvb[...] = acc_kv[...].astype(BF16)

    def round_dy():
        dob[...] = acc_do[...].astype(BF16)

    def position(axis):
        r = lax.broadcasted_iota(jnp.int32, (n_rows, 1) if axis == 0 else (1, n_rows), axis)
        inner = r % par_rows
        return (inner // tok) * (2 * tok) + (r // par_rows) * tok + inner % tok

    def head(m, h):
        cols = slice(h * head_dim, (h + 1) * head_dim)
        q, k, v = qb[:, cols], kvb[:, :head_dim], kvb[:, head_dim:]
        do = dob[:, cols]
        s = dot(q, k, NT) * scale
        s = jnp.where(position(0) >= position(1), s, -jnp.inf)
        e = jnp.exp(s - jnp.max(s, axis=-1, keepdims=True))
        p = e / jnp.sum(e, axis=-1, keepdims=True)
        pb = p.astype(BF16)
        o = dot(pb, v).astype(BF16)
        ob[m, :, cols] = o
        dp = dot(do, v, NT)
        delta = jnp.sum(do.astype(F32) * o.astype(F32), axis=-1, keepdims=True)
        ds = (p * (dp - delta)).astype(BF16)
        prob_b[h] = pb
        ds_b[h] = ds
        dqb[m, :, cols] = (dot(ds, k) * scale).astype(BF16)

    def head_kv(m, h):
        cols = slice(h * head_dim, (h + 1) * head_dim)
        dk = dot(ds_b[h], qb[:, cols], TN) * scale
        dv = dot(prob_b[h], dob[:, cols], TN)
        if h == 0:
            dkv_f[m, :, :head_dim] = dk
            dkv_f[m, :, head_dim:] = dv
        else:
            dkv_f[m, :, :head_dim] += dk
            dkv_f[m, :, head_dim:] += dv

    def kv_round(m):
        dkvp[...] = dkv_f[m].astype(BF16)
        pltpu.make_async_remote_copy(src_ref=dkv_f.at[m], dst_ref=dkv_peer.at[m], send_sem=dkv_sem.at[m, 0],
                                     recv_sem=dkv_sem.at[m, 1], device_id=to(peer), device_id_type=MESH).start()

    def kv_total(m):
        pltpu.make_async_copy(dkv_f.at[m], dkv_f.at[m], dkv_sem.at[m, 0]).wait()
        pltpu.make_async_copy(dkv_peer.at[m], dkv_peer.at[m], dkv_sem.at[m, 1]).wait()
        dkv_tot[m] = (dkv_f[m] + dkv_peer[m]).astype(BF16)

    dw_n = 4
    dw_w = d_model // dw_n

    def put(ref, idx, val, m):
        if m == 0:
            ref[idx] = val
        else:
            ref[idx] += val

    def dw_x(m, i):
        ck = lax.rem(c * (dw_n // 2) + i, dw_n)
        start = pl.multiple_of(ck * dw_w, dw_w)
        xt = xb[m, :, pl.ds(start, dw_w)].T
        g = dot(xt, dqb[m])
        for h in range(heads):
            put(dwq, (pl.ds(start * heads + h, dw_w, stride=heads), slice(None)),
                g[:, h * head_dim:(h + 1) * head_dim], m)
        if i < dw_n // 2:
            g = dot(xt, dkv_tot[m])
            rows = slice(i * dw_w, (i + 1) * dw_w)
            put(dwk, (rows, slice(None)), g[:, :head_dim], m)
            put(dwv, (rows, slice(None)), g[:, head_dim:], m)

    def dw_o(m, i):
        cols = slice(i * dw_w, (i + 1) * dw_w)
        put(dwo, (slice(None), cols), dot(ob[m], dyb[m, :, cols], TN), m)

    def dw_steps(m):
        return ([functools.partial(dw_o, m, i) for i in range(dw_n)]
                + [functools.partial(dw_x, m, i) for i in range(dw_n)])

    rs_n = 4
    rs_w = d_model // rs_n
    rs_h = rs_w // 2

    def dx_chunk(m, j):
        cols = slice(j * rs_w, (j + 1) * rs_w)
        dx_tmp[...] = dot(dqb[m], wq[cols, :], NT) + dot(dkvp[...], wkv[cols, :], NT)
        away = pl.ds(pl.multiple_of((1 - c) * par_rows, par_rows), par_rows)
        keep = pl.ds(pl.multiple_of(c * par_rows, par_rows), par_rows)
        psend[m, :, cols] = dx_tmp[away, :].astype(BF16)
        dx_f[m, :, cols] = dx_tmp[keep, :]
        pltpu.make_async_remote_copy(src_ref=psend.at[m, :, cols], dst_ref=precv.at[m, :, cols],
                                     send_sem=ps_send.at[m, j], recv_sem=ps_recv.at[m, j],
                                     device_id=to(peer), device_id_type=MESH).start()

    def own_part(m, chip, col, width):
        rows = pl.ds(pl.multiple_of(chip * tok, tok), tok)
        return dx_f[m, rows, col:col + width] + precv[m, rows, col:col + width].astype(F32)

    def rs_send_to(m, j, side, d, col, width):
        src = sbuf.at[m, side, d - 1, :, pl.ds(col, width)]
        dst = rbuf.at[m, side, d - 1, :, pl.ds(col, width)]
        pltpu.make_async_remote_copy(src_ref=src, dst_ref=dst, send_sem=rs_send.at[m, j],
                                     recv_sem=rs_recv.at[m, j, d - 1, side],
                                     device_id=to(right if side == 0 else left), device_id_type=MESH).start()

    def chip_at(side, d):
        return lax.rem(z + (d if side == 0 else n_chip - d), n_chip)

    def rs_start(m, j):
        ref = precv.at[m, :, pl.ds(j * rs_w, rs_w)]
        pltpu.make_async_copy(ref, ref, ps_recv.at[m, j]).wait()
        for side in range(2):
            col = j * rs_w + side * rs_h
            sbuf[m, side, half - 1, :, col:col + rs_h] = own_part(m, chip_at(side, half), col, rs_h).astype(BF16)
        for side in range(2):
            rs_send_to(m, j, side, half, j * rs_w + side * rs_h, rs_h)

    def rs_event(m, j, d):
        col = j * rs_w
        for side in range(2):
            rcol, rwidth = (col + side * rs_h, rs_h) if d == half else (col, rs_w)
            ref = rbuf.at[m, side, d - 1, :, pl.ds(rcol, rwidth)]
            pltpu.make_async_copy(ref, ref, rs_recv.at[m, j, d - 1, side]).wait()
        if d == 1:
            total = own_part(m, z, col, rs_w)
            for side in range(2):
                total = total + rbuf[m, side, 0, :, col:col + rs_w].astype(F32)
            dx_own[m, :, col:col + rs_w] = total.astype(BF16)
            return
        for side in range(2):
            chip = chip_at(side, d - 1)
            if d == half:
                a, b = col + side * rs_h, col + (1 - side) * rs_h
                sbuf[m, side, d - 2, :, a:a + rs_h] = (
                    own_part(m, chip, a, rs_h) + rbuf[m, side, d - 1, :, a:a + rs_h].astype(F32)).astype(BF16)
                sbuf[m, side, d - 2, :, b:b + rs_h] = own_part(m, chip, b, rs_h).astype(BF16)
            else:
                sbuf[m, side, d - 2, :, col:col + rs_w] = (
                    own_part(m, chip, col, rs_w)
                    + rbuf[m, side, d - 1, :, col:col + rs_w].astype(F32)).astype(BF16)
        for side in range(2):
            rs_send_to(m, j, side, d - 1, col, rs_w)

    tensor_cols = [(t, j) for t in range(2) for j in range(n_col)]

    ag_start(0)
    work = [prep_wq] + [functools.partial(prep_kv, i) for i in range(n_kv)] + [kv_swap]
    slots = [(d, t, j) for d in range(1, half) for t, j in tensor_cols]
    for s, (d, t, j) in enumerate(slots):
        ag_event(0, t, j, d)
        if work:
            work.pop(0)()
    for w in work:
        w()
    ag_start(1)
    wo_cp.wait()
    kv_swap_wait()

    def finish_gather(m, extra):
        for t, j in tensor_cols:
            ag_event(m, t, j, half)
            for f in extra.get((t, j), ()):
                f()
            if (t, j) == (0, 0):
                continue
            pt, pj = tensor_cols[tensor_cols.index((t, j)) - 1]
            finish_part(m, pt, pj)
        finish_part(m, *tensor_cols[-1])

    def finish_part(m, t, j):
        d2d_wait(m, t, j)
        (proj_x if t == 0 else proj_dy)(m, j)
        if j == n_col - 1:
            (round_x if t == 0 else round_dy)()

    def attn_steps(m):
        steps = []
        for h in range(heads):
            steps.append(functools.partial(head, m, h))
            steps.append(functools.partial(head_kv, m, h))
        steps.append(functools.partial(kv_round, m))
        return steps

    finish_gather(0, {})
    work = attn_steps(0) + [functools.partial(dx_chunk, 0, j) for j in range(rs_n)]
    later = [functools.partial(kv_total, 0)] + dw_steps(0)
    for d, t, j in slots:
        ag_event(1, t, j, d)
        (work or later).pop(0)()
    for j in range(rs_n):
        rs_start(0, j)
    finish_gather(1, {})
    work = attn_steps(1) + [functools.partial(dx_chunk, 1, j) for j in range(rs_n)]
    for d in range(half, 1, -1):
        for j in range(rs_n):
            rs_event(0, j, d)
            (work or later).pop(0)()
    for j in range(rs_n):
        rs_start(1, j)
    later += [functools.partial(kv_total, 1)] + dw_steps(1)
    for j in range(rs_n):
        rs_event(0, j, 1)
        later.pop(0)()
    for d in range(half, 0, -1):
        for j in range(rs_n):
            rs_event(1, j, d)
            if later:
                later.pop(0)()

    for m in range(micro_n):
        for t, j in tensor_cols:
            rows = n_chip - 1
            ref = bufs[t][1].at[m, pl.ds(0, rows * tok), pl.ds(j * col_w, col_w)]
            pltpu.make_async_copy(ref, ref, ag_send.at[m, t, j]).wait()
            ref = peer_blocks(m, t, j, c)
            pltpu.make_async_copy(ref, ref, d2d_send.at[m, t, j]).wait()
        for j in range(rs_n):
            ref = psend.at[m, :, pl.ds(j * rs_w, rs_w)]
            pltpu.make_async_copy(ref, ref, ps_send.at[m, j]).wait()
            ref = psend.at[m, pl.ds(0, (n_chip - 1) * tok), pl.ds(j * rs_w, rs_w)]
            pltpu.make_async_copy(ref, ref, rs_send.at[m, j]).wait()


def copy_kernel(n, *refs):
    srcs, dsts, sem = refs[:n], refs[n:2 * n], refs[2 * n]
    copies = [pltpu.make_async_copy(a, b, sem.at[i]) for i, (a, b) in enumerate(zip(srcs, dsts))]
    for cp in copies:
        cp.start()
    for cp in copies:
        cp.wait()


def solution(mesh):
    n_dev = mesh.shape["model"]

    def device_grads(x_loc, dy_loc, w_q, w_k, w_v, w_o):
        micro_n, tok, d_model = x_loc.shape
        heads, head_dim = w_q.shape[1], w_q.shape[2]
        kv_heads = w_k.shape[1]
        n_rows = tok * n_dev
        par_rows = n_rows // 2
        hd = heads * head_dim
        n_chip = n_dev // 2
        half = n_chip // 2
        any_spec = pl.BlockSpec(memory_space=pl.ANY)
        dma = pltpu.SemaphoreType.DMA
        scratch = [
            pltpu.VMEM((micro_n, n_rows, d_model), BF16),
            pltpu.VMEM((micro_n, n_rows, d_model), BF16),
            pltpu.VMEM((d_model, hd), BF16),
            pltpu.VMEM((hd, d_model), BF16),
            pltpu.VMEM((d_model, 2 * head_dim), BF16),
            pltpu.VMEM((d_model * heads, head_dim), BF16),
            pltpu.VMEM((2, d_model * kv_heads // 8, head_dim), BF16),
            pltpu.VMEM((512, head_dim), F32),
            pltpu.VMEM((n_rows, hd), F32),
            pltpu.VMEM((n_rows, 2 * head_dim), F32),
            pltpu.VMEM((n_rows, hd), F32),
            pltpu.VMEM((n_rows, hd), BF16),
            pltpu.VMEM((n_rows, 2 * head_dim), BF16),
            pltpu.VMEM((n_rows, hd), BF16),
            pltpu.VMEM((micro_n, n_rows, hd), BF16),
            pltpu.VMEM((micro_n, n_rows, hd), BF16),
            pltpu.VMEM((n_rows, 2 * head_dim), BF16),
            pltpu.VMEM((heads, n_rows, n_rows), BF16),
            pltpu.VMEM((heads, n_rows, n_rows), BF16),
            pltpu.VMEM((micro_n, n_rows, 2 * head_dim), F32),
            pltpu.VMEM((micro_n, n_rows, 2 * head_dim), F32),
            pltpu.VMEM((micro_n, n_rows, 2 * head_dim), BF16),
            pltpu.VMEM((micro_n, par_rows, d_model), F32),
            pltpu.VMEM((n_rows, d_model // 4), F32),
            pltpu.VMEM((micro_n, par_rows, d_model), BF16),
            pltpu.VMEM((micro_n, par_rows, d_model), BF16),
            pltpu.VMEM((micro_n, 2, half, tok, d_model), BF16),
            pltpu.VMEM((micro_n, 2, half, tok, d_model), BF16),
            dma((micro_n, 2)), dma((2,)), dma((2,)),
            dma((micro_n, 2, 2)), dma((micro_n, 2, 2, half, 2)),
            dma((micro_n, 2, 2)), dma((micro_n, 2, 2)), dma((2,)),
            dma((micro_n, 2)), dma((micro_n, 4)), dma((micro_n, 4)),
            dma((micro_n, 4)), dma((micro_n, 4, half, 2)),
        ]
        dx, dwq, dwk, dwv, dwo = pl.pallas_call(
            functools.partial(attn_kernel, n_dev, kv_heads),
            out_shape=(
                pltpu.VMEM((micro_n, tok, d_model), BF16),
                pltpu.VMEM((d_model * heads, head_dim), F32),
                pltpu.VMEM((d_model // 2, head_dim), F32),
                pltpu.VMEM((d_model // 2, head_dim), F32),
                pltpu.VMEM((hd, d_model), F32),
            ),
            in_specs=[any_spec] * 6,
            out_specs=(pl.BlockSpec(memory_space=pltpu.VMEM),) * 5,
            scratch_shapes=scratch,
            compiler_params=pltpu.CompilerParams(collective_id=0, has_side_effects=True,
                                                 vmem_limit_bytes=46 * 1024 * 1024),
        )(x_loc, dy_loc, w_q.reshape(d_model * heads, head_dim), w_k.reshape(d_model * kv_heads, head_dim),
          w_v.reshape(d_model * kv_heads, head_dim), w_o.reshape(hd, d_model))

        grads = (dx, dwq, dwk, dwv, dwo)
        dx, dwq, dwk, dwv, dwo = pl.pallas_call(
            functools.partial(copy_kernel, len(grads)),
            out_shape=tuple(jax.ShapeDtypeStruct(g.shape, g.dtype) for g in grads),
            in_specs=[pl.BlockSpec(memory_space=pltpu.VMEM)] * len(grads),
            out_specs=(any_spec,) * len(grads),
            scratch_shapes=[dma((len(grads),))],
            compiler_params=pltpu.CompilerParams(vmem_limit_bytes=1024 * 1024),
        )(*grads)
        return dx, dwq.reshape(d_model, heads, head_dim), dwk, dwv, dwo.reshape(heads, head_dim, d_model)

    return jax.shard_map(
        device_grads, mesh=mesh,
        in_specs=(P("data", "model", None), P("data", "model", None), P(None, "model", None),
                  P(None, None, None), P(None, None, None), P("model", None, None)),
        out_specs=(P("data", "model", None), P("data", "model", None), P(("data", "model"), None),
                   P(("data", "model"), None), P(("data", "model"), None, None)),
        check_vma=False)
```

```python
import functools

import jax
import jax.numpy as jnp
from jax import lax
from jax.experimental import pallas as pl
from jax.experimental.pallas import tpu as pltpu
from jax.sharding import PartitionSpec as P

BF16 = jnp.bfloat16
F32 = jnp.float32
MESH = pl.DeviceIdType.MESH

NT = (((1,), (1,)), ((), ()))
NN = (((1,), (0,)), ((), ()))
TN = (((0,), (0,)), ((), ()))


def dot(a, b, dims=NN):
    return lax.dot_general(a, b, dims, preferred_element_type=F32)


def attn_kernel(n_dev, kv_heads, x_in, dy_in, wq_in, wk_in, wv_in, wo_in,
                dx_own, dwq, dwk, dwv, dwo,
                xb, dyb, wq, wo, wkv, stage_q, stage_kv, unpacked,
                acc_q, acc_kv, acc_do, qb, kvb, dob, ob, dqb, dkvp, prob_b, ds_b,
                dkv_f, dkv_peer, dkv_tot,
                dx_f, dx_tmp, psend, precv, sbuf, rbuf,
                own_sem, w_sem, kvw_sem,
                ag_send, ag_recv, d2d_send, d2d_recv, wx_sem,
                dkv_sem, ps_send, ps_recv, rs_send, rs_recv):
    n_chip = n_dev // 2
    half = n_chip // 2
    micro_n, tok, d_model = x_in.shape
    head_dim = wk_in.shape[1]
    heads = wq.shape[1] // head_dim
    n_rows = n_dev * tok
    par_rows = n_rows // 2
    me = lax.axis_index("model")
    z, c = me // 2, me % 2
    right = lax.rem(me + 2, n_dev)
    left = lax.rem(me + n_dev - 2, n_dev)
    peer = z * 2 + (1 - c)
    scale = head_dim ** -0.5

    def to(dev):
        return {"model": dev}

    barrier = pltpu.get_barrier_semaphore()
    for dev in (left, right, peer):
        pl.semaphore_signal(barrier, inc=1, device_id=to(dev), device_id_type=MESH)

    bufs = ((x_in, xb), (dy_in, dyb))
    my_row = pl.multiple_of(c * par_rows + z * tok, tok)
    own = []
    for m in range(micro_n):
        for t, (src, buf) in enumerate(bufs):
            cp = pltpu.make_async_copy(src.at[m], buf.at[m, pl.ds(my_row, tok)], own_sem.at[m, t])
            cp.start()
            own.append(cp)
    wq_cp = pltpu.make_async_copy(wq_in, stage_q, w_sem.at[0])
    wq_cp.start()
    wo_cp = pltpu.make_async_copy(wo_in, wo, w_sem.at[1])
    wo_cp.start()
    kv_rows = stage_kv.shape[1]
    n_kv = wk_in.shape[0] // kv_rows

    def kv_load(i):
        @pl.when(c == 0)
        def _():
            pltpu.make_async_copy(wk_in.at[pl.ds(i * kv_rows, kv_rows)], stage_kv.at[i % 2], kvw_sem.at[i % 2]).start()

        @pl.when(c == 1)
        def _():
            pltpu.make_async_copy(wv_in.at[pl.ds(i * kv_rows, kv_rows)], stage_kv.at[i % 2], kvw_sem.at[i % 2]).start()

    kv_load(0)
    kv_load(1)

    pl.semaphore_wait(barrier, 3)

    n_col = 2
    col_w = d_model // n_col
    sub_w = col_w // 2

    def blk(m, t, chip, col, width, core=None):
        row = pl.multiple_of((c if core is None else core) * par_rows + chip * tok, tok)
        return bufs[t][1].at[m, pl.ds(row, tok), pl.ds(col, width)]

    def send(ref, dev, ssem, rsem):
        pltpu.make_async_remote_copy(src_ref=ref, dst_ref=ref, send_sem=ssem, recv_sem=rsem,
                                     device_id=to(dev), device_id_type=MESH).start()

    def ag_start(m):
        for t in range(2):
            own[m * 2 + t].wait()
        for t in range(2):
            for j in range(n_col):
                ref = blk(m, t, z, j * col_w, col_w)
                send(ref, right, ag_send.at[m, t, j], ag_recv.at[m, t, j, 0, 0])
                send(ref, left, ag_send.at[m, t, j], ag_recv.at[m, t, j, 0, 1])
                send(ref, peer, d2d_send.at[m, t, j], d2d_recv.at[m, t, j])

    def ag_event(m, t, j, d):
        last = d == half
        for side in range(2):
            chip = lax.rem(z + (n_chip - d if side == 0 else d), n_chip)
            col, width = (j * col_w, col_w) if not last else (j * col_w + side * sub_w, sub_w)
            ref = blk(m, t, chip, col, width)
            pltpu.make_async_copy(ref, ref, ag_recv.at[m, t, j, d - 1, side]).wait()
            if d < half - 1:
                fwd = ref
            elif d == half - 1:
                fwd = blk(m, t, chip, j * col_w + side * sub_w, sub_w)
            else:
                fwd = None
            if fwd is not None:
                send(fwd, right if side == 0 else left, ag_send.at[m, t, j], ag_recv.at[m, t, j, d, side])
            send(ref, peer, d2d_send.at[m, t, j], d2d_recv.at[m, t, j])

    def peer_blocks(m, t, j, core):
        row = pl.multiple_of(core * par_rows, par_rows)
        return bufs[t][1].at[m, pl.ds(row, par_rows), pl.ds(j * col_w, col_w)]

    def d2d_wait(m, t, j):
        ref = peer_blocks(m, t, j, 1 - c)
        pltpu.make_async_copy(ref, ref, d2d_recv.at[m, t, j]).wait()

    un_rows = unpacked.shape[0]

    def prep_wq():
        wq_cp.wait()
        per = un_rows // heads

        def body(i, _):
            unpacked[...] = stage_q[pl.ds(pl.multiple_of(i * un_rows, un_rows), un_rows), :].astype(F32)
            for h in range(heads):
                wq[pl.ds(pl.multiple_of(i * per, per), per), h * head_dim:(h + 1) * head_dim] = (
                    unpacked[pl.ds(h, per, stride=heads), :].astype(BF16))
            return 0

        lax.fori_loop(0, stage_q.shape[0] // un_rows, body, 0)

    kv_col = pl.multiple_of(c * head_dim, head_dim)

    def prep_kv(i):
        pltpu.make_async_copy(wk_in.at[pl.ds(i * kv_rows, kv_rows)], stage_kv.at[i % 2], kvw_sem.at[i % 2]).wait()
        per = un_rows // kv_heads
        base = i * (kv_rows // kv_heads)

        def body(k, _):
            unpacked[...] = stage_kv[i % 2, pl.ds(pl.multiple_of(k * un_rows, un_rows), un_rows), :].astype(F32)
            wkv[pl.ds(pl.multiple_of(base + k * per, per), per), pl.ds(kv_col, head_dim)] = (
                unpacked[pl.ds(z, per, stride=kv_heads), :].astype(BF16))
            return 0

        lax.fori_loop(0, kv_rows // un_rows, body, 0)
        if i + 2 < n_kv:
            kv_load(i + 2)

    def kv_swap():
        ref = wkv.at[:, pl.ds(kv_col, head_dim)]
        pltpu.make_async_remote_copy(src_ref=ref, dst_ref=ref, send_sem=wx_sem.at[0], recv_sem=wx_sem.at[1],
                                     device_id=to(peer), device_id_type=MESH).start()

    def kv_swap_wait():
        ref = wkv.at[:, pl.ds(kv_col, head_dim)]
        pltpu.make_async_copy(ref, ref, wx_sem.at[0]).wait()
        ref = wkv.at[:, pl.ds(pl.multiple_of((1 - c) * head_dim, head_dim), head_dim)]
        pltpu.make_async_copy(ref, ref, wx_sem.at[1]).wait()

    def proj_x(m, j):
        for k in range(2):
            cols = slice(j * col_w + k * sub_w, j * col_w + (k + 1) * sub_w)
            a = dot(xb[m, :, cols], wq[cols, :])
            b = dot(xb[m, :, cols], wkv[cols, :])
            if j == 0 and k == 0:
                acc_q[...] = a
                acc_kv[...] = b
            else:
                acc_q[...] += a
                acc_kv[...] += b

    def proj_dy(m, j):
        for k in range(2):
            cols = slice(j * col_w + k * sub_w, j * col_w + (k + 1) * sub_w)
            a = dot(dyb[m, :, cols], wo[:, cols], NT)
            if j == 0 and k == 0:
                acc_do[...] = a
            else:
                acc_do[...] += a

    def round_x():
        qb[...] = acc_q[...].astype(BF16)
        kvb[...] = acc_kv[...].astype(BF16)

    def round_dy():
        dob[...] = acc_do[...].astype(BF16)

    def position(axis):
        r = lax.broadcasted_iota(jnp.int32, (n_rows, 1) if axis == 0 else (1, n_rows), axis)
        inner = r % par_rows
        return (inner // tok) * (2 * tok) + (r // par_rows) * tok + inner % tok

    def head(m, h):
        cols = slice(h * head_dim, (h + 1) * head_dim)
        q, k, v = qb[:, cols], kvb[:, :head_dim], kvb[:, head_dim:]
        do = dob[:, cols]
        s = dot(q, k, NT) * scale
        s = jnp.where(position(0) >= position(1), s, -jnp.inf)
        e = jnp.exp(s - jnp.max(s, axis=-1, keepdims=True))
        p = e / jnp.sum(e, axis=-1, keepdims=True)
        pb = p.astype(BF16)
        o = dot(pb, v).astype(BF16)
        ob[m, :, cols] = o
        dp = dot(do, v, NT)
        delta = jnp.sum(do.astype(F32) * o.astype(F32), axis=-1, keepdims=True)
        ds = (p * (dp - delta)).astype(BF16)
        prob_b[h] = pb
        ds_b[h] = ds
        dqb[m, :, cols] = (dot(ds, k) * scale).astype(BF16)

    def head_kv(m, h):
        cols = slice(h * head_dim, (h + 1) * head_dim)
        dk = dot(ds_b[h], qb[:, cols], TN) * scale
        dv = dot(prob_b[h], dob[:, cols], TN)
        if h == 0:
            dkv_f[m, :, :head_dim] = dk
            dkv_f[m, :, head_dim:] = dv
        else:
            dkv_f[m, :, :head_dim] += dk
            dkv_f[m, :, head_dim:] += dv

    def kv_round(m):
        dkvp[...] = dkv_f[m].astype(BF16)
        pltpu.make_async_remote_copy(src_ref=dkv_f.at[m], dst_ref=dkv_peer.at[m], send_sem=dkv_sem.at[m, 0],
                                     recv_sem=dkv_sem.at[m, 1], device_id=to(peer), device_id_type=MESH).start()

    def kv_total(m):
        pltpu.make_async_copy(dkv_f.at[m], dkv_f.at[m], dkv_sem.at[m, 0]).wait()
        pltpu.make_async_copy(dkv_peer.at[m], dkv_peer.at[m], dkv_sem.at[m, 1]).wait()
        dkv_tot[m] = (dkv_f[m] + dkv_peer[m]).astype(BF16)

    dw_n = 4
    dw_w = d_model // dw_n

    def put(ref, idx, val, m):
        if m == 0:
            ref[idx] = val
        else:
            ref[idx] += val

    def dw_x(m, i):
        ck = lax.rem(c * (dw_n // 2) + i, dw_n)
        start = pl.multiple_of(ck * dw_w, dw_w)
        xt = xb[m, :, pl.ds(start, dw_w)].T
        g = dot(xt, dqb[m])
        for h in range(heads):
            put(dwq, (pl.ds(start * heads + h, dw_w, stride=heads), slice(None)),
                g[:, h * head_dim:(h + 1) * head_dim], m)
        if i < dw_n // 2:
            g = dot(xt, dkv_tot[m])
            rows = slice(i * dw_w, (i + 1) * dw_w)
            put(dwk, (rows, slice(None)), g[:, :head_dim], m)
            put(dwv, (rows, slice(None)), g[:, head_dim:], m)

    def dw_o(m, i):
        cols = slice(i * dw_w, (i + 1) * dw_w)
        put(dwo, (slice(None), cols), dot(ob[m], dyb[m, :, cols], TN), m)

    def dw_steps(m):
        return ([functools.partial(dw_o, m, i) for i in range(dw_n)]
                + [functools.partial(dw_x, m, i) for i in range(dw_n)])

    rs_n = 4
    rs_w = d_model // rs_n
    rs_h = rs_w // 2

    def dx_chunk(m, j):
        cols = slice(j * rs_w, (j + 1) * rs_w)
        dx_tmp[...] = dot(dqb[m], wq[cols, :], NT) + dot(dkvp[...], wkv[cols, :], NT)
        away = pl.ds(pl.multiple_of((1 - c) * par_rows, par_rows), par_rows)
        keep = pl.ds(pl.multiple_of(c * par_rows, par_rows), par_rows)
        psend[m, :, cols] = dx_tmp[away, :].astype(BF16)
        dx_f[m, :, cols] = dx_tmp[keep, :]
        pltpu.make_async_remote_copy(src_ref=psend.at[m, :, cols], dst_ref=precv.at[m, :, cols],
                                     send_sem=ps_send.at[m, j], recv_sem=ps_recv.at[m, j],
                                     device_id=to(peer), device_id_type=MESH).start()

    def own_part(m, chip, col, width):
        rows = pl.ds(pl.multiple_of(chip * tok, tok), tok)
        return dx_f[m, rows, col:col + width] + precv[m, rows, col:col + width].astype(F32)

    def rs_send_to(m, j, side, d, col, width):
        src = sbuf.at[m, side, d - 1, :, pl.ds(col, width)]
        dst = rbuf.at[m, side, d - 1, :, pl.ds(col, width)]
        pltpu.make_async_remote_copy(src_ref=src, dst_ref=dst, send_sem=rs_send.at[m, j],
                                     recv_sem=rs_recv.at[m, j, d - 1, side],
                                     device_id=to(right if side == 0 else left), device_id_type=MESH).start()

    def chip_at(side, d):
        return lax.rem(z + (d if side == 0 else n_chip - d), n_chip)

    def rs_start(m, j):
        ref = precv.at[m, :, pl.ds(j * rs_w, rs_w)]
        pltpu.make_async_copy(ref, ref, ps_recv.at[m, j]).wait()
        for side in range(2):
            col = j * rs_w + side * rs_h
            sbuf[m, side, half - 1, :, col:col + rs_h] = own_part(m, chip_at(side, half), col, rs_h).astype(BF16)
        for side in range(2):
            rs_send_to(m, j, side, half, j * rs_w + side * rs_h, rs_h)

    def rs_event(m, j, d):
        col = j * rs_w
        for side in range(2):
            rcol, rwidth = (col + side * rs_h, rs_h) if d == half else (col, rs_w)
            ref = rbuf.at[m, side, d - 1, :, pl.ds(rcol, rwidth)]
            pltpu.make_async_copy(ref, ref, rs_recv.at[m, j, d - 1, side]).wait()
        if d == 1:
            total = own_part(m, z, col, rs_w)
            for side in range(2):
                total = total + rbuf[m, side, 0, :, col:col + rs_w].astype(F32)
            dx_own[m, :, col:col + rs_w] = total.astype(BF16)
            return
        for side in range(2):
            chip = chip_at(side, d - 1)
            if d == half:
                a, b = col + side * rs_h, col + (1 - side) * rs_h
                sbuf[m, side, d - 2, :, a:a + rs_h] = (
                    own_part(m, chip, a, rs_h) + rbuf[m, side, d - 1, :, a:a + rs_h].astype(F32)).astype(BF16)
                sbuf[m, side, d - 2, :, b:b + rs_h] = own_part(m, chip, b, rs_h).astype(BF16)
            else:
                sbuf[m, side, d - 2, :, col:col + rs_w] = (
                    own_part(m, chip, col, rs_w)
                    + rbuf[m, side, d - 1, :, col:col + rs_w].astype(F32)).astype(BF16)
        for side in range(2):
            rs_send_to(m, j, side, d - 1, col, rs_w)

    tensor_cols = [(t, j) for t in range(2) for j in range(n_col)]

    ag_start(0)
    work = [prep_wq] + [functools.partial(prep_kv, i) for i in range(n_kv)] + [kv_swap]
    slots = [(d, t, j) for d in range(1, half) for t, j in tensor_cols]
    for s, (d, t, j) in enumerate(slots):
        ag_event(0, t, j, d)
        if work:
            work.pop(0)()
    for w in work:
        w()
    ag_start(1)
    wo_cp.wait()
    kv_swap_wait()

    def finish_gather(m, extra):
        for t, j in tensor_cols:
            ag_event(m, t, j, half)
            for f in extra.get((t, j), ()):
                f()
            if (t, j) == (0, 0):
                continue
            pt, pj = tensor_cols[tensor_cols.index((t, j)) - 1]
            finish_part(m, pt, pj)
        finish_part(m, *tensor_cols[-1])

    def finish_part(m, t, j):
        d2d_wait(m, t, j)
        (proj_x if t == 0 else proj_dy)(m, j)
        if j == n_col - 1:
            (round_x if t == 0 else round_dy)()

    def attn_steps(m):
        steps = []
        for h in range(heads):
            steps.append(functools.partial(head, m, h))
            steps.append(functools.partial(head_kv, m, h))
        steps.append(functools.partial(kv_round, m))
        return steps

    finish_gather(0, {})
    work = attn_steps(0) + [functools.partial(dx_chunk, 0, j) for j in range(rs_n)]
    later = [functools.partial(kv_total, 0)] + dw_steps(0)
    for i, (d, t, j) in enumerate(slots):
        ag_event(1, t, j, d)
        if i == len(slots) - 2:
            while work:
                work.pop(0)()
            for k in range(rs_n):
                rs_start(0, k)
        (work or later).pop(0)()
    finish_gather(1, {
        (0, 1): [functools.partial(rs_event, 0, 0, half)],
        (1, 0): [functools.partial(rs_event, 0, 1, half), functools.partial(rs_event, 0, 2, half)],
        (1, 1): [functools.partial(rs_event, 0, 3, half)],
    })
    attn = attn_steps(1)
    for k in range(heads):
        attn.pop(0)()
        rs_event(0, 2 * k, 3)
        attn.pop(0)()
        rs_event(0, 2 * k + 1, 3)
    for f in attn:
        f()
    dx_chunk(1, 0)
    dx_chunk(1, 1)
    rs_event(0, 0, 2)
    rs_start(1, 0)
    dx_chunk(1, 2)
    rs_event(0, 1, 2)
    rs_start(1, 1)
    dx_chunk(1, 3)
    rs_event(0, 2, 2)
    rs_start(1, 2)
    later.pop(0)()
    rs_event(0, 3, 2)
    later.pop(0)()
    rs_start(1, 3)
    later += [functools.partial(kv_total, 1)] + dw_steps(1)
    for j in range(rs_n):
        later.pop(0)()
        rs_event(1, j, half)
    for j in range(rs_n):
        rs_event(0, j, 1)
        later.pop(0)()
    for d in range(half - 1, 0, -1):
        for j in range(rs_n):
            rs_event(1, j, d)
            if later:
                later.pop(0)()
    for f in later:
        f()

    for m in range(micro_n):
        for t, j in tensor_cols:
            rows = n_chip - 1
            ref = bufs[t][1].at[m, pl.ds(0, rows * tok), pl.ds(j * col_w, col_w)]
            pltpu.make_async_copy(ref, ref, ag_send.at[m, t, j]).wait()
            ref = peer_blocks(m, t, j, c)
            pltpu.make_async_copy(ref, ref, d2d_send.at[m, t, j]).wait()
        for j in range(rs_n):
            ref = psend.at[m, :, pl.ds(j * rs_w, rs_w)]
            pltpu.make_async_copy(ref, ref, ps_send.at[m, j]).wait()
            ref = psend.at[m, pl.ds(0, (n_chip - 1) * tok), pl.ds(j * rs_w, rs_w)]
            pltpu.make_async_copy(ref, ref, rs_send.at[m, j]).wait()


def copy_kernel(n, *refs):
    srcs, dsts, sem = refs[:n], refs[n:2 * n], refs[2 * n]
    copies = [pltpu.make_async_copy(a, b, sem.at[i]) for i, (a, b) in enumerate(zip(srcs, dsts))]
    for cp in copies:
        cp.start()
    for cp in copies:
        cp.wait()


def solution(mesh):
    n_dev = mesh.shape["model"]

    def device_grads(x_loc, dy_loc, w_q, w_k, w_v, w_o):
        micro_n, tok, d_model = x_loc.shape
        heads, head_dim = w_q.shape[1], w_q.shape[2]
        kv_heads = w_k.shape[1]
        n_rows = tok * n_dev
        par_rows = n_rows // 2
        hd = heads * head_dim
        n_chip = n_dev // 2
        half = n_chip // 2
        any_spec = pl.BlockSpec(memory_space=pl.ANY)
        dma = pltpu.SemaphoreType.DMA
        scratch = [
            pltpu.VMEM((micro_n, n_rows, d_model), BF16),
            pltpu.VMEM((micro_n, n_rows, d_model), BF16),
            pltpu.VMEM((d_model, hd), BF16),
            pltpu.VMEM((hd, d_model), BF16),
            pltpu.VMEM((d_model, 2 * head_dim), BF16),
            pltpu.VMEM((d_model * heads, head_dim), BF16),
            pltpu.VMEM((2, d_model * kv_heads // 8, head_dim), BF16),
            pltpu.VMEM((512, head_dim), F32),
            pltpu.VMEM((n_rows, hd), F32),
            pltpu.VMEM((n_rows, 2 * head_dim), F32),
            pltpu.VMEM((n_rows, hd), F32),
            pltpu.VMEM((n_rows, hd), BF16),
            pltpu.VMEM((n_rows, 2 * head_dim), BF16),
            pltpu.VMEM((n_rows, hd), BF16),
            pltpu.VMEM((micro_n, n_rows, hd), BF16),
            pltpu.VMEM((micro_n, n_rows, hd), BF16),
            pltpu.VMEM((n_rows, 2 * head_dim), BF16),
            pltpu.VMEM((heads, n_rows, n_rows), BF16),
            pltpu.VMEM((heads, n_rows, n_rows), BF16),
            pltpu.VMEM((micro_n, n_rows, 2 * head_dim), F32),
            pltpu.VMEM((micro_n, n_rows, 2 * head_dim), F32),
            pltpu.VMEM((micro_n, n_rows, 2 * head_dim), BF16),
            pltpu.VMEM((micro_n, par_rows, d_model), F32),
            pltpu.VMEM((n_rows, d_model // 4), F32),
            pltpu.VMEM((micro_n, par_rows, d_model), BF16),
            pltpu.VMEM((micro_n, par_rows, d_model), BF16),
            pltpu.VMEM((micro_n, 2, half, tok, d_model), BF16),
            pltpu.VMEM((micro_n, 2, half, tok, d_model), BF16),
            dma((micro_n, 2)), dma((2,)), dma((2,)),
            dma((micro_n, 2, 2)), dma((micro_n, 2, 2, half, 2)),
            dma((micro_n, 2, 2)), dma((micro_n, 2, 2)), dma((2,)),
            dma((micro_n, 2)), dma((micro_n, 4)), dma((micro_n, 4)),
            dma((micro_n, 4)), dma((micro_n, 4, half, 2)),
        ]
        dx, dwq, dwk, dwv, dwo = pl.pallas_call(
            functools.partial(attn_kernel, n_dev, kv_heads),
            out_shape=(
                pltpu.VMEM((micro_n, tok, d_model), BF16),
                pltpu.VMEM((d_model * heads, head_dim), F32),
                pltpu.VMEM((d_model // 2, head_dim), F32),
                pltpu.VMEM((d_model // 2, head_dim), F32),
                pltpu.VMEM((hd, d_model), F32),
            ),
            in_specs=[any_spec] * 6,
            out_specs=(pl.BlockSpec(memory_space=pltpu.VMEM),) * 5,
            scratch_shapes=scratch,
            compiler_params=pltpu.CompilerParams(collective_id=0, has_side_effects=True,
                                                 vmem_limit_bytes=46 * 1024 * 1024),
        )(x_loc, dy_loc, w_q.reshape(d_model * heads, head_dim), w_k.reshape(d_model * kv_heads, head_dim),
          w_v.reshape(d_model * kv_heads, head_dim), w_o.reshape(hd, d_model))

        grads = (dx, dwq, dwk, dwv, dwo)
        dx, dwq, dwk, dwv, dwo = pl.pallas_call(
            functools.partial(copy_kernel, len(grads)),
            out_shape=tuple(jax.ShapeDtypeStruct(g.shape, g.dtype) for g in grads),
            in_specs=[pl.BlockSpec(memory_space=pltpu.VMEM)] * len(grads),
            out_specs=(any_spec,) * len(grads),
            scratch_shapes=[dma((len(grads),))],
            compiler_params=pltpu.CompilerParams(vmem_limit_bytes=1024 * 1024),
        )(*grads)
        return dx, dwq.reshape(d_model, heads, head_dim), dwk, dwv, dwo.reshape(heads, head_dim, d_model)

    return jax.shard_map(
        device_grads, mesh=mesh,
        in_specs=(P("data", "model", None), P("data", "model", None), P(None, "model", None),
                  P(None, None, None), P(None, None, None), P("model", None, None)),
        out_specs=(P("data", "model", None), P("data", "model", None), P(("data", "model"), None),
                   P(("data", "model"), None), P(("data", "model"), None, None)),
        check_vma=False)
```

```python
import functools

import jax
import jax.numpy as jnp
from jax import lax
from jax.experimental import pallas as pl
from jax.experimental.pallas import tpu as pltpu
from jax.sharding import PartitionSpec as P

BF16 = jnp.bfloat16
F32 = jnp.float32
MESH = pl.DeviceIdType.MESH

NT = (((1,), (1,)), ((), ()))
NN = (((1,), (0,)), ((), ()))
TN = (((0,), (0,)), ((), ()))


def dot(a, b, dims=NN):
    return lax.dot_general(a, b, dims, preferred_element_type=F32)


def attn_kernel(n_dev, kv_heads, x_in, dy_in, wq_in, wk_in, wv_in, wo_in,
                dx_own, dwq, dwk, dwv, dwo,
                xb, dyb, wq, wo, wkv, stage_q, stage_kv, unpacked,
                acc_q, acc_kv, acc_do, qb, kvb, dob, ob, dqb, dkvp, prob_b, ds_b,
                dkv_f, dkv_peer, dkv_tot,
                dx_f, dx_tmp, psend, precv, sbuf, rbuf,
                own_sem, w_sem, kvw_sem,
                ag_send, ag_recv, d2d_send, d2d_recv, wx_sem,
                dkv_sem, ps_send, ps_recv, rs_send, rs_recv):
    n_chip = n_dev // 2
    half = n_chip // 2
    micro_n, tok, d_model = x_in.shape
    head_dim = wk_in.shape[1]
    heads = wq.shape[1] // head_dim
    n_rows = n_dev * tok
    par_rows = n_rows // 2
    me = lax.axis_index("model")
    z, c = me // 2, me % 2
    right = lax.rem(me + 2, n_dev)
    left = lax.rem(me + n_dev - 2, n_dev)
    peer = z * 2 + (1 - c)
    scale = head_dim ** -0.5

    def to(dev):
        return {"model": dev}

    barrier = pltpu.get_barrier_semaphore()
    for dev in (left, right, peer):
        pl.semaphore_signal(barrier, inc=1, device_id=to(dev), device_id_type=MESH)

    bufs = ((x_in, xb), (dy_in, dyb))
    my_row = pl.multiple_of(c * par_rows + z * tok, tok)
    own = []
    for m in range(micro_n):
        for t, (src, buf) in enumerate(bufs):
            cp = pltpu.make_async_copy(src.at[m], buf.at[m, pl.ds(my_row, tok)], own_sem.at[m, t])
            cp.start()
            own.append(cp)
    wq_cp = pltpu.make_async_copy(wq_in, stage_q, w_sem.at[0])
    wq_cp.start()
    wo_cp = pltpu.make_async_copy(wo_in, wo, w_sem.at[1])
    wo_cp.start()
    kv_rows = stage_kv.shape[1]
    n_kv = wk_in.shape[0] // kv_rows

    def kv_load(i):
        @pl.when(c == 0)
        def _():
            pltpu.make_async_copy(wk_in.at[pl.ds(i * kv_rows, kv_rows)], stage_kv.at[i % 2], kvw_sem.at[i % 2]).start()

        @pl.when(c == 1)
        def _():
            pltpu.make_async_copy(wv_in.at[pl.ds(i * kv_rows, kv_rows)], stage_kv.at[i % 2], kvw_sem.at[i % 2]).start()

    kv_load(0)
    kv_load(1)

    pl.semaphore_wait(barrier, 3)

    n_col = 2
    col_w = d_model // n_col
    sub_w = col_w // 2

    def blk(m, t, chip, col, width, core=None):
        row = pl.multiple_of((c if core is None else core) * par_rows + chip * tok, tok)
        return bufs[t][1].at[m, pl.ds(row, tok), pl.ds(col, width)]

    def send(ref, dev, ssem, rsem):
        pltpu.make_async_remote_copy(src_ref=ref, dst_ref=ref, send_sem=ssem, recv_sem=rsem,
                                     device_id=to(dev), device_id_type=MESH).start()

    def ag_start(m):
        for t in range(2):
            own[m * 2 + t].wait()
        for t in range(2):
            for j in range(n_col):
                ref = blk(m, t, z, j * col_w, col_w)
                send(ref, right, ag_send.at[m, t, j], ag_recv.at[m, t, j, 0, 0])
                send(ref, left, ag_send.at[m, t, j], ag_recv.at[m, t, j, 0, 1])
                send(ref, peer, d2d_send.at[m, t, j], d2d_recv.at[m, t, j])

    def ag_event(m, t, j, d):
        last = d == half
        for side in range(2):
            chip = lax.rem(z + (n_chip - d if side == 0 else d), n_chip)
            col, width = (j * col_w, col_w) if not last else (j * col_w + side * sub_w, sub_w)
            ref = blk(m, t, chip, col, width)
            pltpu.make_async_copy(ref, ref, ag_recv.at[m, t, j, d - 1, side]).wait()
            if d < half - 1:
                fwd = ref
            elif d == half - 1:
                fwd = blk(m, t, chip, j * col_w + side * sub_w, sub_w)
            else:
                fwd = None
            if fwd is not None:
                send(fwd, right if side == 0 else left, ag_send.at[m, t, j], ag_recv.at[m, t, j, d, side])
            send(ref, peer, d2d_send.at[m, t, j], d2d_recv.at[m, t, j])

    def peer_blocks(m, t, j, core):
        row = pl.multiple_of(core * par_rows, par_rows)
        return bufs[t][1].at[m, pl.ds(row, par_rows), pl.ds(j * col_w, col_w)]

    def d2d_wait(m, t, j):
        ref = peer_blocks(m, t, j, 1 - c)
        pltpu.make_async_copy(ref, ref, d2d_recv.at[m, t, j]).wait()

    un_rows = unpacked.shape[0]

    def prep_wq():
        wq_cp.wait()
        per = un_rows // heads

        def body(i, _):
            unpacked[...] = stage_q[pl.ds(pl.multiple_of(i * un_rows, un_rows), un_rows), :].astype(F32)
            for h in range(heads):
                wq[pl.ds(pl.multiple_of(i * per, per), per), h * head_dim:(h + 1) * head_dim] = (
                    unpacked[pl.ds(h, per, stride=heads), :].astype(BF16))
            return 0

        lax.fori_loop(0, stage_q.shape[0] // un_rows, body, 0)

    kv_col = pl.multiple_of(c * head_dim, head_dim)

    def prep_kv(i):
        pltpu.make_async_copy(wk_in.at[pl.ds(i * kv_rows, kv_rows)], stage_kv.at[i % 2], kvw_sem.at[i % 2]).wait()
        per = un_rows // kv_heads
        base = i * (kv_rows // kv_heads)

        def body(k, _):
            unpacked[...] = stage_kv[i % 2, pl.ds(pl.multiple_of(k * un_rows, un_rows), un_rows), :].astype(F32)
            wkv[pl.ds(pl.multiple_of(base + k * per, per), per), pl.ds(kv_col, head_dim)] = (
                unpacked[pl.ds(z, per, stride=kv_heads), :].astype(BF16))
            return 0

        lax.fori_loop(0, kv_rows // un_rows, body, 0)
        if i + 2 < n_kv:
            kv_load(i + 2)

    def kv_swap():
        ref = wkv.at[:, pl.ds(kv_col, head_dim)]
        pltpu.make_async_remote_copy(src_ref=ref, dst_ref=ref, send_sem=wx_sem.at[0], recv_sem=wx_sem.at[1],
                                     device_id=to(peer), device_id_type=MESH).start()

    def kv_swap_wait():
        ref = wkv.at[:, pl.ds(kv_col, head_dim)]
        pltpu.make_async_copy(ref, ref, wx_sem.at[0]).wait()
        ref = wkv.at[:, pl.ds(pl.multiple_of((1 - c) * head_dim, head_dim), head_dim)]
        pltpu.make_async_copy(ref, ref, wx_sem.at[1]).wait()

    def proj_x(m, j):
        for k in range(2):
            cols = slice(j * col_w + k * sub_w, j * col_w + (k + 1) * sub_w)
            a = dot(xb[m, :, cols], wq[cols, :])
            b = dot(xb[m, :, cols], wkv[cols, :])
            if j == 0 and k == 0:
                acc_q[...] = a
                acc_kv[...] = b
            else:
                acc_q[...] += a
                acc_kv[...] += b

    def proj_dy(m, j):
        for k in range(2):
            cols = slice(j * col_w + k * sub_w, j * col_w + (k + 1) * sub_w)
            a = dot(dyb[m, :, cols], wo[:, cols], NT)
            if j == 0 and k == 0:
                acc_do[...] = a
            else:
                acc_do[...] += a

    def round_x():
        qb[...] = acc_q[...].astype(BF16)
        kvb[...] = acc_kv[...].astype(BF16)

    def round_dy():
        dob[...] = acc_do[...].astype(BF16)

    def position(axis):
        r = lax.broadcasted_iota(jnp.int32, (n_rows, 1) if axis == 0 else (1, n_rows), axis)
        inner = r % par_rows
        return (inner // tok) * (2 * tok) + (r // par_rows) * tok + inner % tok

    def head(m, h):
        cols = slice(h * head_dim, (h + 1) * head_dim)
        q, k, v = qb[:, cols], kvb[:, :head_dim], kvb[:, head_dim:]
        do = dob[:, cols]
        s = dot(q, k, NT) * scale
        s = jnp.where(position(0) >= position(1), s, -jnp.inf)
        e = jnp.exp(s - jnp.max(s, axis=-1, keepdims=True))
        p = e / jnp.sum(e, axis=-1, keepdims=True)
        pb = p.astype(BF16)
        o = dot(pb, v).astype(BF16)
        ob[m, :, cols] = o
        dp = dot(do, v, NT)
        delta = jnp.sum(do.astype(F32) * o.astype(F32), axis=-1, keepdims=True)
        ds = (p * (dp - delta)).astype(BF16)
        prob_b[h] = pb
        ds_b[h] = ds
        dqb[m, :, cols] = (dot(ds, k) * scale).astype(BF16)

    def head_kv(m, h):
        cols = slice(h * head_dim, (h + 1) * head_dim)
        dk = dot(ds_b[h], qb[:, cols], TN) * scale
        dv = dot(prob_b[h], dob[:, cols], TN)
        if h == 0:
            dkv_f[m, :, :head_dim] = dk
            dkv_f[m, :, head_dim:] = dv
        else:
            dkv_f[m, :, :head_dim] += dk
            dkv_f[m, :, head_dim:] += dv

    def kv_round(m):
        dkvp[...] = dkv_f[m].astype(BF16)
        pltpu.make_async_remote_copy(src_ref=dkv_f.at[m], dst_ref=dkv_peer.at[m], send_sem=dkv_sem.at[m, 0],
                                     recv_sem=dkv_sem.at[m, 1], device_id=to(peer), device_id_type=MESH).start()

    def kv_total(m):
        pltpu.make_async_copy(dkv_f.at[m], dkv_f.at[m], dkv_sem.at[m, 0]).wait()
        pltpu.make_async_copy(dkv_peer.at[m], dkv_peer.at[m], dkv_sem.at[m, 1]).wait()
        dkv_tot[m] = (dkv_f[m] + dkv_peer[m]).astype(BF16)

    dw_n = 4
    dw_w = d_model // dw_n

    def put(ref, idx, val, m):
        if m == 0:
            ref[idx] = val
        else:
            ref[idx] += val

    def dw_x(m, i):
        ck = lax.rem(c * (dw_n // 2) + i, dw_n)
        start = pl.multiple_of(ck * dw_w, dw_w)
        xt = xb[m, :, pl.ds(start, dw_w)].T
        g = dot(xt, dqb[m])
        for h in range(heads):
            put(dwq, (pl.ds(start * heads + h, dw_w, stride=heads), slice(None)),
                g[:, h * head_dim:(h + 1) * head_dim], m)
        if i < dw_n // 2:
            g = dot(xt, dkv_tot[m])
            rows = slice(i * dw_w, (i + 1) * dw_w)
            put(dwk, (rows, slice(None)), g[:, :head_dim], m)
            put(dwv, (rows, slice(None)), g[:, head_dim:], m)

    def dw_o(m, i):
        cols = slice(i * dw_w, (i + 1) * dw_w)
        put(dwo, (slice(None), cols), dot(ob[m], dyb[m, :, cols], TN), m)

    def dw_steps(m):
        return ([functools.partial(dw_o, m, i) for i in range(dw_n)]
                + [functools.partial(dw_x, m, i) for i in range(dw_n)])

    rs_n = 4
    rs_w = d_model // rs_n
    rs_h = rs_w // 2

    def dx_chunk(m, j):
        cols = slice(j * rs_w, (j + 1) * rs_w)
        dx_tmp[...] = dot(dqb[m], wq[cols, :], NT) + dot(dkvp[...], wkv[cols, :], NT)
        away = pl.ds(pl.multiple_of((1 - c) * par_rows, par_rows), par_rows)
        keep = pl.ds(pl.multiple_of(c * par_rows, par_rows), par_rows)
        psend[m, :, cols] = dx_tmp[away, :].astype(BF16)
        dx_f[m, :, cols] = dx_tmp[keep, :]
        pltpu.make_async_remote_copy(src_ref=psend.at[m, :, cols], dst_ref=precv.at[m, :, cols],
                                     send_sem=ps_send.at[m, j], recv_sem=ps_recv.at[m, j],
                                     device_id=to(peer), device_id_type=MESH).start()

    def own_part(m, chip, col, width):
        rows = pl.ds(pl.multiple_of(chip * tok, tok), tok)
        return dx_f[m, rows, col:col + width] + precv[m, rows, col:col + width].astype(F32)

    def rs_send_to(m, j, side, d, col, width):
        src = sbuf.at[m, side, d - 1, :, pl.ds(col, width)]
        dst = rbuf.at[m, side, d - 1, :, pl.ds(col, width)]
        pltpu.make_async_remote_copy(src_ref=src, dst_ref=dst, send_sem=rs_send.at[m, j],
                                     recv_sem=rs_recv.at[m, j, d - 1, side],
                                     device_id=to(right if side == 0 else left), device_id_type=MESH).start()

    def chip_at(side, d):
        return lax.rem(z + (d if side == 0 else n_chip - d), n_chip)

    def rs_start(m, j):
        ref = precv.at[m, :, pl.ds(j * rs_w, rs_w)]
        pltpu.make_async_copy(ref, ref, ps_recv.at[m, j]).wait()
        for side in range(2):
            col = j * rs_w + side * rs_h
            sbuf[m, side, half - 1, :, col:col + rs_h] = own_part(m, chip_at(side, half), col, rs_h).astype(BF16)
        for side in range(2):
            rs_send_to(m, j, side, half, j * rs_w + side * rs_h, rs_h)

    def rs_event(m, j, d):
        col = j * rs_w
        for side in range(2):
            rcol, rwidth = (col + side * rs_h, rs_h) if d == half else (col, rs_w)
            ref = rbuf.at[m, side, d - 1, :, pl.ds(rcol, rwidth)]
            pltpu.make_async_copy(ref, ref, rs_recv.at[m, j, d - 1, side]).wait()
        if d == 1:
            total = own_part(m, z, col, rs_w)
            for side in range(2):
                total = total + rbuf[m, side, 0, :, col:col + rs_w].astype(F32)
            dx_own[m, :, col:col + rs_w] = total.astype(BF16)
            return
        for side in range(2):
            chip = chip_at(side, d - 1)
            if d == half:
                a, b = col + side * rs_h, col + (1 - side) * rs_h
                sbuf[m, side, d - 2, :, a:a + rs_h] = (
                    own_part(m, chip, a, rs_h) + rbuf[m, side, d - 1, :, a:a + rs_h].astype(F32)).astype(BF16)
                sbuf[m, side, d - 2, :, b:b + rs_h] = own_part(m, chip, b, rs_h).astype(BF16)
            else:
                sbuf[m, side, d - 2, :, col:col + rs_w] = (
                    own_part(m, chip, col, rs_w)
                    + rbuf[m, side, d - 1, :, col:col + rs_w].astype(F32)).astype(BF16)
        for side in range(2):
            rs_send_to(m, j, side, d - 1, col, rs_w)

    tensor_cols = [(t, j) for t in range(2) for j in range(n_col)]

    ag_start(0)
    work = [prep_wq] + [functools.partial(prep_kv, i) for i in range(n_kv)] + [kv_swap]
    slots = [(d, t, j) for d in range(1, half) for t, j in tensor_cols]
    for s, (d, t, j) in enumerate(slots):
        ag_event(0, t, j, d)
        if work:
            work.pop(0)()
    for w in work:
        w()
    ag_start(1)
    wo_cp.wait()
    kv_swap_wait()

    def finish_gather(m, extra):
        for t, j in tensor_cols:
            ag_event(m, t, j, half)
            for f in extra.get((t, j), ()):
                f()
            if (t, j) == (0, 0):
                continue
            pt, pj = tensor_cols[tensor_cols.index((t, j)) - 1]
            finish_part(m, pt, pj)
        finish_part(m, *tensor_cols[-1])

    def finish_part(m, t, j):
        d2d_wait(m, t, j)
        (proj_x if t == 0 else proj_dy)(m, j)
        if j == n_col - 1:
            (round_x if t == 0 else round_dy)()

    def attn_steps(m):
        steps = []
        for h in range(heads):
            steps.append(functools.partial(head, m, h))
            steps.append(functools.partial(head_kv, m, h))
        steps.append(functools.partial(kv_round, m))
        return steps

    finish_gather(0, {})
    work = attn_steps(0) + [functools.partial(dx_chunk, 0, j) for j in range(rs_n)]
    later = [functools.partial(kv_total, 0)] + dw_steps(0)
    for i, (d, t, j) in enumerate(slots):
        ag_event(1, t, j, d)
        if i == len(slots) - 2:
            while work:
                work.pop(0)()
            for k in range(rs_n):
                rs_start(0, k)
        (work or later).pop(0)()
    ev = functools.partial(rs_event, 0)
    ag_event(1, 0, 0, half)
    ag_event(1, 0, 1, half)
    ag_event(1, 1, 0, half)
    ev(0, half)
    finish_part(1, 0, 0)
    ev(1, half)
    ev(2, half)
    finish_part(1, 0, 1)
    ev(3, half)
    ag_event(1, 1, 1, half)
    finish_part(1, 1, 0)
    ev(0, half - 1)
    finish_part(1, 1, 1)
    ev(1, half - 1)
    attn = attn_steps(1)
    attn.pop(0)()
    ev(2, half - 1)
    attn.pop(0)()
    attn.pop(0)()
    ev(3, half - 1)
    for f in attn:
        f()
    ev(0, half - 2)
    dx_chunk(1, 0)
    ev(1, half - 2)
    dx_chunk(1, 1)
    ev(2, half - 2)
    rs_start(1, 0)
    dx_chunk(1, 2)
    ev(3, half - 2)
    rs_start(1, 1)
    dx_chunk(1, 3)
    rs_start(1, 2)
    later.pop(0)()
    later.pop(0)()
    rs_start(1, 3)
    later += [functools.partial(kv_total, 1)] + dw_steps(1)
    for j in range(rs_n):
        later.pop(0)()
        rs_event(1, j, half)
    for j in range(rs_n):
        rs_event(0, j, 1)
        later.pop(0)()
    for d in range(half - 1, 1, -1):
        for j in range(rs_n):
            rs_event(1, j, d)
            if later:
                later.pop(0)()
    for f in later:
        f()
    for m in range(micro_n):
        for t, j in tensor_cols:
            ref = bufs[t][1].at[m, pl.ds(0, (n_chip - 1) * tok), pl.ds(j * col_w, col_w)]
            pltpu.make_async_copy(ref, ref, ag_send.at[m, t, j]).wait()
            ref = peer_blocks(m, t, j, c)
            pltpu.make_async_copy(ref, ref, d2d_send.at[m, t, j]).wait()
        for j in range(rs_n):
            ref = psend.at[m, :, pl.ds(j * rs_w, rs_w)]
            pltpu.make_async_copy(ref, ref, ps_send.at[m, j]).wait()

    def rs_drain(m):
        for j in range(rs_n):
            ref = psend.at[m, pl.ds(0, (n_chip - 1) * tok), pl.ds(j * rs_w, rs_w)]
            pltpu.make_async_copy(ref, ref, rs_send.at[m, j]).wait()

    rs_drain(0)
    for j in range(rs_n):
        rs_event(1, j, 1)
    rs_drain(1)


def copy_kernel(n, *refs):
    srcs, dsts, sem = refs[:n], refs[n:2 * n], refs[2 * n]
    pairs = []
    for a, b in zip(srcs, dsts):
        parts = max(1, a.shape[0] // 2560) if a.shape[-1] < 1024 else a.shape[0] // 64 or 1
        rows = a.shape[0] // parts
        pairs += [(a.at[pl.ds(i * rows, rows)], b.at[pl.ds(i * rows, rows)]) for i in range(parts)]
    copies = [pltpu.make_async_copy(a, b, sem.at[i]) for i, (a, b) in enumerate(pairs)]
    for cp in copies:
        cp.start()
    for cp in copies:
        cp.wait()


def solution(mesh):
    n_dev = mesh.shape["model"]

    def device_grads(x_loc, dy_loc, w_q, w_k, w_v, w_o):
        micro_n, tok, d_model = x_loc.shape
        heads, head_dim = w_q.shape[1], w_q.shape[2]
        kv_heads = w_k.shape[1]
        n_rows = tok * n_dev
        par_rows = n_rows // 2
        hd = heads * head_dim
        n_chip = n_dev // 2
        half = n_chip // 2
        any_spec = pl.BlockSpec(memory_space=pl.ANY)
        dma = pltpu.SemaphoreType.DMA
        scratch = [
            pltpu.VMEM((micro_n, n_rows, d_model), BF16),
            pltpu.VMEM((micro_n, n_rows, d_model), BF16),
            pltpu.VMEM((d_model, hd), BF16),
            pltpu.VMEM((hd, d_model), BF16),
            pltpu.VMEM((d_model, 2 * head_dim), BF16),
            pltpu.VMEM((d_model * heads, head_dim), BF16),
            pltpu.VMEM((2, d_model * kv_heads // 8, head_dim), BF16),
            pltpu.VMEM((512, head_dim), F32),
            pltpu.VMEM((n_rows, hd), F32),
            pltpu.VMEM((n_rows, 2 * head_dim), F32),
            pltpu.VMEM((n_rows, hd), F32),
            pltpu.VMEM((n_rows, hd), BF16),
            pltpu.VMEM((n_rows, 2 * head_dim), BF16),
            pltpu.VMEM((n_rows, hd), BF16),
            pltpu.VMEM((micro_n, n_rows, hd), BF16),
            pltpu.VMEM((micro_n, n_rows, hd), BF16),
            pltpu.VMEM((n_rows, 2 * head_dim), BF16),
            pltpu.VMEM((heads, n_rows, n_rows), BF16),
            pltpu.VMEM((heads, n_rows, n_rows), BF16),
            pltpu.VMEM((micro_n, n_rows, 2 * head_dim), F32),
            pltpu.VMEM((micro_n, n_rows, 2 * head_dim), F32),
            pltpu.VMEM((micro_n, n_rows, 2 * head_dim), BF16),
            pltpu.VMEM((micro_n, par_rows, d_model), F32),
            pltpu.VMEM((n_rows, d_model // 4), F32),
            pltpu.VMEM((micro_n, par_rows, d_model), BF16),
            pltpu.VMEM((micro_n, par_rows, d_model), BF16),
            pltpu.VMEM((micro_n, 2, half, tok, d_model), BF16),
            pltpu.VMEM((micro_n, 2, half, tok, d_model), BF16),
            dma((micro_n, 2)), dma((2,)), dma((2,)),
            dma((micro_n, 2, 2)), dma((micro_n, 2, 2, half, 2)),
            dma((micro_n, 2, 2)), dma((micro_n, 2, 2)), dma((2,)),
            dma((micro_n, 2)), dma((micro_n, 4)), dma((micro_n, 4)),
            dma((micro_n, 4)), dma((micro_n, 4, half, 2)),
        ]
        dx, dwq, dwk, dwv, dwo = pl.pallas_call(
            functools.partial(attn_kernel, n_dev, kv_heads),
            out_shape=(
                pltpu.VMEM((micro_n, tok, d_model), BF16),
                pltpu.VMEM((d_model * heads, head_dim), F32),
                pltpu.VMEM((d_model // 2, head_dim), F32),
                pltpu.VMEM((d_model // 2, head_dim), F32),
                pltpu.VMEM((hd, d_model), F32),
            ),
            in_specs=[any_spec] * 6,
            out_specs=(pl.BlockSpec(memory_space=pltpu.VMEM),) * 5,
            scratch_shapes=scratch,
            compiler_params=pltpu.CompilerParams(collective_id=0, has_side_effects=True,
                                                 vmem_limit_bytes=46 * 1024 * 1024),
        )(x_loc, dy_loc, w_q.reshape(d_model * heads, head_dim), w_k.reshape(d_model * kv_heads, head_dim),
          w_v.reshape(d_model * kv_heads, head_dim), w_o.reshape(hd, d_model))

        grads = (dx, dwq, dwk, dwv, dwo)
        dx, dwq, dwk, dwv, dwo = pl.pallas_call(
            functools.partial(copy_kernel, len(grads)),
            out_shape=tuple(jax.ShapeDtypeStruct(g.shape, g.dtype) for g in grads),
            in_specs=[pl.BlockSpec(memory_space=pltpu.VMEM)] * len(grads),
            out_specs=(any_spec,) * len(grads),
            scratch_shapes=[dma((16,))],
            compiler_params=pltpu.CompilerParams(vmem_limit_bytes=1024 * 1024),
        )(*grads)
        return dx, dwq.reshape(d_model, heads, head_dim), dwk, dwv, dwo.reshape(heads, head_dim, d_model)

    return jax.shard_map(
        device_grads, mesh=mesh,
        in_specs=(P("data", "model", None), P("data", "model", None), P(None, "model", None),
                  P(None, None, None), P(None, None, None), P("model", None, None)),
        out_specs=(P("data", "model", None), P("data", "model", None), P(("data", "model"), None),
                   P(("data", "model"), None), P(("data", "model"), None, None)),
        check_vma=False)
```

```python
import functools

import jax
import jax.numpy as jnp
from jax import lax
from jax.experimental import pallas as pl
from jax.experimental.pallas import tpu as pltpu
from jax.sharding import PartitionSpec as P

BF16 = jnp.bfloat16
F32 = jnp.float32
MESH = pl.DeviceIdType.MESH

NT = (((1,), (1,)), ((), ()))
NN = (((1,), (0,)), ((), ()))
TN = (((0,), (0,)), ((), ()))


def dot(a, b, dims=NN):
    return lax.dot_general(a, b, dims, preferred_element_type=F32)


def attn_kernel(n_dev, kv_heads, x_in, dy_in, wq_in, wk_in, wv_in, wo_in,
                dx_own, dwq, dwk, dwv, dwo,
                xb, dyb, wq, wo, wkv, stage_q, stage_kv, unpacked,
                acc_q, acc_kv, acc_do, qb, kvb, dob, ob, dqb, dkvp, prob_b, ds_b,
                dkv_f, dkv_peer, dkv_tot,
                dx_f, dx_tmp, psend, precv, sbuf, rbuf,
                own_sem, w_sem, kvw_sem,
                ag_send, ag_recv, d2d_send, d2d_recv, wx_sem,
                dkv_sem, ps_send, ps_recv, rs_send, rs_recv):
    n_chip = n_dev // 2
    half = n_chip // 2
    micro_n, tok, d_model = x_in.shape
    head_dim = wk_in.shape[1]
    heads = wq.shape[1] // head_dim
    n_rows = n_dev * tok
    par_rows = n_rows // 2
    me = lax.axis_index("model")
    z, c = me // 2, me % 2
    right = lax.rem(me + 2, n_dev)
    left = lax.rem(me + n_dev - 2, n_dev)
    peer = z * 2 + (1 - c)
    scale = head_dim ** -0.5

    def to(dev):
        return {"model": dev}

    barrier = pltpu.get_barrier_semaphore()
    for dev in (left, right, peer):
        pl.semaphore_signal(barrier, inc=1, device_id=to(dev), device_id_type=MESH)

    bufs = ((x_in, xb), (dy_in, dyb))
    my_row = pl.multiple_of(c * par_rows + z * tok, tok)
    own = []
    for m in range(micro_n):
        for t, (src, buf) in enumerate(bufs):
            cp = pltpu.make_async_copy(src.at[m], buf.at[m, pl.ds(my_row, tok)], own_sem.at[m, t])
            cp.start()
            own.append(cp)
    wq_cp = pltpu.make_async_copy(wq_in, stage_q, w_sem.at[0])
    wq_cp.start()
    wo_cp = pltpu.make_async_copy(wo_in, wo, w_sem.at[1])
    wo_cp.start()
    kv_rows = stage_kv.shape[1]
    n_kv = wk_in.shape[0] // kv_rows

    def kv_load(i):
        @pl.when(c == 0)
        def _():
            pltpu.make_async_copy(wk_in.at[pl.ds(i * kv_rows, kv_rows)], stage_kv.at[i % 2], kvw_sem.at[i % 2]).start()

        @pl.when(c == 1)
        def _():
            pltpu.make_async_copy(wv_in.at[pl.ds(i * kv_rows, kv_rows)], stage_kv.at[i % 2], kvw_sem.at[i % 2]).start()

    kv_load(0)
    kv_load(1)

    pl.semaphore_wait(barrier, 3)

    n_col = 2
    col_w = d_model // n_col
    sub_w = col_w // 2

    def blk(m, t, chip, col, width, core=None):
        row = pl.multiple_of((c if core is None else core) * par_rows + chip * tok, tok)
        return bufs[t][1].at[m, pl.ds(row, tok), pl.ds(col, width)]

    def send(ref, dev, ssem, rsem):
        pltpu.make_async_remote_copy(src_ref=ref, dst_ref=ref, send_sem=ssem, recv_sem=rsem,
                                     device_id=to(dev), device_id_type=MESH).start()

    def ag_start(m):
        for t in range(2):
            own[m * 2 + t].wait()
        for t in range(2):
            for j in range(n_col):
                ref = blk(m, t, z, j * col_w, col_w)
                send(ref, right, ag_send.at[m, t, j], ag_recv.at[m, t, j, 0, 0])
                send(ref, left, ag_send.at[m, t, j], ag_recv.at[m, t, j, 0, 1])
                send(ref, peer, d2d_send.at[m, t, j], d2d_recv.at[m, t, j])

    def ag_event(m, t, j, d):
        last = d == half
        for side in range(2):
            chip = lax.rem(z + (n_chip - d if side == 0 else d), n_chip)
            col, width = (j * col_w, col_w) if not last else (j * col_w + side * sub_w, sub_w)
            ref = blk(m, t, chip, col, width)
            pltpu.make_async_copy(ref, ref, ag_recv.at[m, t, j, d - 1, side]).wait()
            if d < half - 1:
                fwd = ref
            elif d == half - 1:
                fwd = blk(m, t, chip, j * col_w + side * sub_w, sub_w)
            else:
                fwd = None
            if fwd is not None:
                send(fwd, right if side == 0 else left, ag_send.at[m, t, j], ag_recv.at[m, t, j, d, side])
            send(ref, peer, d2d_send.at[m, t, j], d2d_recv.at[m, t, j])

    def peer_blocks(m, t, j, core):
        row = pl.multiple_of(core * par_rows, par_rows)
        return bufs[t][1].at[m, pl.ds(row, par_rows), pl.ds(j * col_w, col_w)]

    def d2d_wait(m, t, j):
        ref = peer_blocks(m, t, j, 1 - c)
        pltpu.make_async_copy(ref, ref, d2d_recv.at[m, t, j]).wait()

    un_rows = unpacked.shape[0]

    def prep_wq():
        wq_cp.wait()
        per = un_rows // heads

        def body(i, _):
            unpacked[...] = stage_q[pl.ds(pl.multiple_of(i * un_rows, un_rows), un_rows), :].astype(F32)
            for h in range(heads):
                wq[pl.ds(pl.multiple_of(i * per, per), per), h * head_dim:(h + 1) * head_dim] = (
                    unpacked[pl.ds(h, per, stride=heads), :].astype(BF16))
            return 0

        lax.fori_loop(0, stage_q.shape[0] // un_rows, body, 0)

    kv_col = pl.multiple_of(c * head_dim, head_dim)

    def prep_kv(i):
        pltpu.make_async_copy(wk_in.at[pl.ds(i * kv_rows, kv_rows)], stage_kv.at[i % 2], kvw_sem.at[i % 2]).wait()
        per = un_rows // kv_heads
        base = i * (kv_rows // kv_heads)

        def body(k, _):
            unpacked[...] = stage_kv[i % 2, pl.ds(pl.multiple_of(k * un_rows, un_rows), un_rows), :].astype(F32)
            wkv[pl.ds(pl.multiple_of(base + k * per, per), per), pl.ds(kv_col, head_dim)] = (
                unpacked[pl.ds(z, per, stride=kv_heads), :].astype(BF16))
            return 0

        lax.fori_loop(0, kv_rows // un_rows, body, 0)
        if i + 2 < n_kv:
            kv_load(i + 2)

    def kv_swap():
        ref = wkv.at[:, pl.ds(kv_col, head_dim)]
        pltpu.make_async_remote_copy(src_ref=ref, dst_ref=ref, send_sem=wx_sem.at[0], recv_sem=wx_sem.at[1],
                                     device_id=to(peer), device_id_type=MESH).start()

    def kv_swap_wait():
        ref = wkv.at[:, pl.ds(kv_col, head_dim)]
        pltpu.make_async_copy(ref, ref, wx_sem.at[0]).wait()
        ref = wkv.at[:, pl.ds(pl.multiple_of((1 - c) * head_dim, head_dim), head_dim)]
        pltpu.make_async_copy(ref, ref, wx_sem.at[1]).wait()

    def proj_x(m, j):
        for k in range(2):
            cols = slice(j * col_w + k * sub_w, j * col_w + (k + 1) * sub_w)
            a = dot(xb[m, :, cols], wq[cols, :])
            b = dot(xb[m, :, cols], wkv[cols, :])
            if j == 0 and k == 0:
                acc_q[...] = a
                acc_kv[...] = b
            else:
                acc_q[...] += a
                acc_kv[...] += b

    def proj_dy(m, j):
        for k in range(2):
            cols = slice(j * col_w + k * sub_w, j * col_w + (k + 1) * sub_w)
            a = dot(dyb[m, :, cols], wo[:, cols], NT)
            if j == 0 and k == 0:
                acc_do[...] = a
            else:
                acc_do[...] += a

    def round_x():
        qb[...] = acc_q[...].astype(BF16)
        kvb[...] = acc_kv[...].astype(BF16)

    def round_dy():
        dob[...] = acc_do[...].astype(BF16)

    def position(axis):
        r = lax.broadcasted_iota(jnp.int32, (n_rows, 1) if axis == 0 else (1, n_rows), axis)
        inner = r % par_rows
        return (inner // tok) * (2 * tok) + (r // par_rows) * tok + inner % tok

    def head(m, h):
        cols = slice(h * head_dim, (h + 1) * head_dim)
        q, k, v = qb[:, cols], kvb[:, :head_dim], kvb[:, head_dim:]
        do = dob[:, cols]
        s = dot(q, k, NT) * scale
        s = jnp.where(position(0) >= position(1), s, -jnp.inf)
        e = jnp.exp(s - jnp.max(s, axis=-1, keepdims=True))
        p = e / jnp.sum(e, axis=-1, keepdims=True)
        pb = p.astype(BF16)
        o = dot(pb, v).astype(BF16)
        ob[m, :, cols] = o
        dp = dot(do, v, NT)
        delta = jnp.sum(do.astype(F32) * o.astype(F32), axis=-1, keepdims=True)
        ds = (p * (dp - delta)).astype(BF16)
        prob_b[h] = pb
        ds_b[h] = ds
        dqb[m, :, cols] = (dot(ds, k) * scale).astype(BF16)

    def head_kv(m, h):
        cols = slice(h * head_dim, (h + 1) * head_dim)
        dk = dot(ds_b[h], qb[:, cols], TN) * scale
        dv = dot(prob_b[h], dob[:, cols], TN)
        if h == 0:
            dkv_f[m, :, :head_dim] = dk
            dkv_f[m, :, head_dim:] = dv
        else:
            dkv_f[m, :, :head_dim] += dk
            dkv_f[m, :, head_dim:] += dv

    def kv_round(m):
        dkvp[...] = dkv_f[m].astype(BF16)
        pltpu.make_async_remote_copy(src_ref=dkv_f.at[m], dst_ref=dkv_peer.at[m], send_sem=dkv_sem.at[m, 0],
                                     recv_sem=dkv_sem.at[m, 1], device_id=to(peer), device_id_type=MESH).start()

    def kv_total(m):
        pltpu.make_async_copy(dkv_f.at[m], dkv_f.at[m], dkv_sem.at[m, 0]).wait()
        pltpu.make_async_copy(dkv_peer.at[m], dkv_peer.at[m], dkv_sem.at[m, 1]).wait()
        dkv_tot[m] = (dkv_f[m] + dkv_peer[m]).astype(BF16)

    dw_n = 4
    dw_w = d_model // dw_n

    def put(ref, idx, val, m):
        if m == 0:
            ref[idx] = val
        else:
            ref[idx] += val

    def dw_x(m, i):
        ck = lax.rem(c * (dw_n // 2) + i, dw_n)
        start = pl.multiple_of(ck * dw_w, dw_w)
        xt = xb[m, :, pl.ds(start, dw_w)].T
        g = dot(xt, dqb[m])
        for h in range(heads):
            put(dwq, (pl.ds(start * heads + h, dw_w, stride=heads), slice(None)),
                g[:, h * head_dim:(h + 1) * head_dim], m)
        if i < dw_n // 2:
            g = dot(xt, dkv_tot[m])
            rows = slice(i * dw_w, (i + 1) * dw_w)
            put(dwk, (rows, slice(None)), g[:, :head_dim], m)
            put(dwv, (rows, slice(None)), g[:, head_dim:], m)

    def dw_o(m, i):
        cols = slice(i * dw_w, (i + 1) * dw_w)
        put(dwo, (slice(None), cols), dot(ob[m], dyb[m, :, cols], TN), m)

    def dw_steps(m):
        return ([functools.partial(dw_o, m, i) for i in range(dw_n)]
                + [functools.partial(dw_x, m, i) for i in range(dw_n)])

    rs_n = 4
    rs_w = d_model // rs_n
    rs_h = rs_w // 2

    def dx_chunk(m, j):
        cols = slice(j * rs_w, (j + 1) * rs_w)
        dx_tmp[...] = dot(dqb[m], wq[cols, :], NT) + dot(dkvp[...], wkv[cols, :], NT)
        away = pl.ds(pl.multiple_of((1 - c) * par_rows, par_rows), par_rows)
        keep = pl.ds(pl.multiple_of(c * par_rows, par_rows), par_rows)
        psend[m, :, cols] = dx_tmp[away, :].astype(BF16)
        dx_f[m, :, cols] = dx_tmp[keep, :]
        pltpu.make_async_remote_copy(src_ref=psend.at[m, :, cols], dst_ref=precv.at[m, :, cols],
                                     send_sem=ps_send.at[m, j], recv_sem=ps_recv.at[m, j],
                                     device_id=to(peer), device_id_type=MESH).start()

    def own_part(m, chip, col, width):
        rows = pl.ds(pl.multiple_of(chip * tok, tok), tok)
        return dx_f[m, rows, col:col + width] + precv[m, rows, col:col + width].astype(F32)

    def rs_send_to(m, j, side, d, col, width):
        src = sbuf.at[m, side, d - 1, :, pl.ds(col, width)]
        dst = rbuf.at[m, side, d - 1, :, pl.ds(col, width)]
        pltpu.make_async_remote_copy(src_ref=src, dst_ref=dst, send_sem=rs_send.at[m, j],
                                     recv_sem=rs_recv.at[m, j, d - 1, side],
                                     device_id=to(right if side == 0 else left), device_id_type=MESH).start()

    def chip_at(side, d):
        return lax.rem(z + (d if side == 0 else n_chip - d), n_chip)

    def rs_start(m, j):
        ref = precv.at[m, :, pl.ds(j * rs_w, rs_w)]
        pltpu.make_async_copy(ref, ref, ps_recv.at[m, j]).wait()
        for side in range(2):
            col = j * rs_w + side * rs_h
            sbuf[m, side, half - 1, :, col:col + rs_h] = own_part(m, chip_at(side, half), col, rs_h).astype(BF16)
        for side in range(2):
            rs_send_to(m, j, side, half, j * rs_w + side * rs_h, rs_h)

    def rs_event(m, j, d):
        col = j * rs_w
        for side in range(2):
            rcol, rwidth = (col + side * rs_h, rs_h) if d == half else (col, rs_w)
            ref = rbuf.at[m, side, d - 1, :, pl.ds(rcol, rwidth)]
            pltpu.make_async_copy(ref, ref, rs_recv.at[m, j, d - 1, side]).wait()
        if d == 1:
            total = own_part(m, z, col, rs_w)
            for side in range(2):
                total = total + rbuf[m, side, 0, :, col:col + rs_w].astype(F32)
            dx_own[m, :, col:col + rs_w] = total.astype(BF16)
            return
        for side in range(2):
            chip = chip_at(side, d - 1)
            if d == half:
                a, b = col + side * rs_h, col + (1 - side) * rs_h
                sbuf[m, side, d - 2, :, a:a + rs_h] = (
                    own_part(m, chip, a, rs_h) + rbuf[m, side, d - 1, :, a:a + rs_h].astype(F32)).astype(BF16)
                sbuf[m, side, d - 2, :, b:b + rs_h] = own_part(m, chip, b, rs_h).astype(BF16)
            else:
                sbuf[m, side, d - 2, :, col:col + rs_w] = (
                    own_part(m, chip, col, rs_w)
                    + rbuf[m, side, d - 1, :, col:col + rs_w].astype(F32)).astype(BF16)
        for side in range(2):
            rs_send_to(m, j, side, d - 1, col, rs_w)

    tensor_cols = [(t, j) for t in range(2) for j in range(n_col)]

    ag_start(0)
    work = [prep_wq] + [functools.partial(prep_kv, i) for i in range(n_kv)] + [kv_swap]
    slots = [(d, t, j) for d in range(1, half) for t, j in tensor_cols]
    for s, (d, t, j) in enumerate(slots):
        ag_event(0, t, j, d)
        if work:
            work.pop(0)()
    for w in work:
        w()
    ag_start(1)
    wo_cp.wait()
    kv_swap_wait()

    def finish_gather(m, extra):
        for t, j in tensor_cols:
            ag_event(m, t, j, half)
            for f in extra.get((t, j), ()):
                f()
            if (t, j) == (0, 0):
                continue
            pt, pj = tensor_cols[tensor_cols.index((t, j)) - 1]
            finish_part(m, pt, pj)
        finish_part(m, *tensor_cols[-1])

    def finish_part(m, t, j):
        d2d_wait(m, t, j)
        (proj_x if t == 0 else proj_dy)(m, j)
        if j == n_col - 1:
            (round_x if t == 0 else round_dy)()

    def attn_steps(m):
        steps = []
        for h in range(heads):
            steps.append(functools.partial(head, m, h))
            steps.append(functools.partial(head_kv, m, h))
        steps.append(functools.partial(kv_round, m))
        return steps

    finish_gather(0, {})
    work = attn_steps(0) + [functools.partial(dx_chunk, 0, j) for j in range(rs_n)]
    later = [functools.partial(kv_total, 0)] + dw_steps(0)
    for i, (d, t, j) in enumerate(slots):
        ag_event(1, t, j, d)
        if i == len(slots) - 2:
            while work:
                work.pop(0)()
            for k in range(rs_n):
                rs_start(0, k)
        (work or later).pop(0)()
    ev = functools.partial(rs_event, 0)
    ag_event(1, 0, 0, half)
    ag_event(1, 0, 1, half)
    finish_part(1, 0, 0)
    ag_event(1, 1, 0, half)
    ev(0, half)
    finish_part(1, 0, 1)
    ev(1, half)
    ev(2, half)
    finish_part(1, 1, 0)
    ag_event(1, 1, 1, half)
    ev(3, half)
    finish_part(1, 1, 1)
    attn = attn_steps(1)
    for k in range(2 * heads):
        ev(k, half - 1)
        attn.pop(0)()
    for f in attn:
        f()
    dx_chunk(1, 0)
    ev(0, half - 2)
    dx_chunk(1, 1)
    ev(1, half - 2)
    rs_start(1, 0)
    dx_chunk(1, 2)
    ev(2, half - 2)
    rs_start(1, 1)
    dx_chunk(1, 3)
    ev(3, half - 2)
    rs_start(1, 2)
    later.pop(0)()
    later.pop(0)()
    rs_start(1, 3)
    later += [functools.partial(kv_total, 1)] + dw_steps(1)
    for j in range(rs_n):
        later.pop(0)()
        rs_event(1, j, half)
    for j in range(rs_n):
        rs_event(0, j, 1)
        later.pop(0)()
    for d in range(half - 1, 1, -1):
        for j in range(rs_n):
            rs_event(1, j, d)
            if later:
                later.pop(0)()
    for f in later:
        f()
    for m in range(micro_n):
        for t, j in tensor_cols:
            ref = bufs[t][1].at[m, pl.ds(0, (n_chip - 1) * tok), pl.ds(j * col_w, col_w)]
            pltpu.make_async_copy(ref, ref, ag_send.at[m, t, j]).wait()
            ref = peer_blocks(m, t, j, c)
            pltpu.make_async_copy(ref, ref, d2d_send.at[m, t, j]).wait()
        for j in range(rs_n):
            ref = psend.at[m, :, pl.ds(j * rs_w, rs_w)]
            pltpu.make_async_copy(ref, ref, ps_send.at[m, j]).wait()

    def rs_drain(m):
        for j in range(rs_n):
            ref = psend.at[m, pl.ds(0, (n_chip - 1) * tok), pl.ds(j * rs_w, rs_w)]
            pltpu.make_async_copy(ref, ref, rs_send.at[m, j]).wait()

    rs_drain(0)
    for j in range(rs_n):
        rs_event(1, j, 1)
    rs_drain(1)


def copy_kernel(n, *refs):
    srcs, dsts, sem = refs[:n], refs[n:2 * n], refs[2 * n]
    pairs = []
    for a, b in zip(srcs, dsts):
        parts = max(1, a.shape[0] // 2560) if a.shape[-1] < 1024 else a.shape[0] // 64 or 1
        rows = a.shape[0] // parts
        pairs += [(a.at[pl.ds(i * rows, rows)], b.at[pl.ds(i * rows, rows)]) for i in range(parts)]
    copies = [pltpu.make_async_copy(a, b, sem.at[i]) for i, (a, b) in enumerate(pairs)]
    for cp in copies:
        cp.start()
    for cp in copies:
        cp.wait()


def solution(mesh):
    n_dev = mesh.shape["model"]

    def device_grads(x_loc, dy_loc, w_q, w_k, w_v, w_o):
        micro_n, tok, d_model = x_loc.shape
        heads, head_dim = w_q.shape[1], w_q.shape[2]
        kv_heads = w_k.shape[1]
        n_rows = tok * n_dev
        par_rows = n_rows // 2
        hd = heads * head_dim
        n_chip = n_dev // 2
        half = n_chip // 2
        any_spec = pl.BlockSpec(memory_space=pl.ANY)
        dma = pltpu.SemaphoreType.DMA
        scratch = [
            pltpu.VMEM((micro_n, n_rows, d_model), BF16),
            pltpu.VMEM((micro_n, n_rows, d_model), BF16),
            pltpu.VMEM((d_model, hd), BF16),
            pltpu.VMEM((hd, d_model), BF16),
            pltpu.VMEM((d_model, 2 * head_dim), BF16),
            pltpu.VMEM((d_model * heads, head_dim), BF16),
            pltpu.VMEM((2, d_model * kv_heads // 8, head_dim), BF16),
            pltpu.VMEM((512, head_dim), F32),
            pltpu.VMEM((n_rows, hd), F32),
            pltpu.VMEM((n_rows, 2 * head_dim), F32),
            pltpu.VMEM((n_rows, hd), F32),
            pltpu.VMEM((n_rows, hd), BF16),
            pltpu.VMEM((n_rows, 2 * head_dim), BF16),
            pltpu.VMEM((n_rows, hd), BF16),
            pltpu.VMEM((micro_n, n_rows, hd), BF16),
            pltpu.VMEM((micro_n, n_rows, hd), BF16),
            pltpu.VMEM((n_rows, 2 * head_dim), BF16),
            pltpu.VMEM((heads, n_rows, n_rows), BF16),
            pltpu.VMEM((heads, n_rows, n_rows), BF16),
            pltpu.VMEM((micro_n, n_rows, 2 * head_dim), F32),
            pltpu.VMEM((micro_n, n_rows, 2 * head_dim), F32),
            pltpu.VMEM((micro_n, n_rows, 2 * head_dim), BF16),
            pltpu.VMEM((micro_n, par_rows, d_model), F32),
            pltpu.VMEM((n_rows, d_model // 4), F32),
            pltpu.VMEM((micro_n, par_rows, d_model), BF16),
            pltpu.VMEM((micro_n, par_rows, d_model), BF16),
            pltpu.VMEM((micro_n, 2, half, tok, d_model), BF16),
            pltpu.VMEM((micro_n, 2, half, tok, d_model), BF16),
            dma((micro_n, 2)), dma((2,)), dma((2,)),
            dma((micro_n, 2, 2)), dma((micro_n, 2, 2, half, 2)),
            dma((micro_n, 2, 2)), dma((micro_n, 2, 2)), dma((2,)),
            dma((micro_n, 2)), dma((micro_n, 4)), dma((micro_n, 4)),
            dma((micro_n, 4)), dma((micro_n, 4, half, 2)),
        ]
        dx, dwq, dwk, dwv, dwo = pl.pallas_call(
            functools.partial(attn_kernel, n_dev, kv_heads),
            out_shape=(
                pltpu.VMEM((micro_n, tok, d_model), BF16),
                pltpu.VMEM((d_model * heads, head_dim), F32),
                pltpu.VMEM((d_model // 2, head_dim), F32),
                pltpu.VMEM((d_model // 2, head_dim), F32),
                pltpu.VMEM((hd, d_model), F32),
            ),
            in_specs=[any_spec] * 6,
            out_specs=(pl.BlockSpec(memory_space=pltpu.VMEM),) * 5,
            scratch_shapes=scratch,
            compiler_params=pltpu.CompilerParams(collective_id=0, has_side_effects=True,
                                                 vmem_limit_bytes=46 * 1024 * 1024),
        )(x_loc, dy_loc, w_q.reshape(d_model * heads, head_dim), w_k.reshape(d_model * kv_heads, head_dim),
          w_v.reshape(d_model * kv_heads, head_dim), w_o.reshape(hd, d_model))

        grads = (dx, dwq, dwk, dwv, dwo)
        dx, dwq, dwk, dwv, dwo = pl.pallas_call(
            functools.partial(copy_kernel, len(grads)),
            out_shape=tuple(jax.ShapeDtypeStruct(g.shape, g.dtype) for g in grads),
            in_specs=[pl.BlockSpec(memory_space=pltpu.VMEM)] * len(grads),
            out_specs=(any_spec,) * len(grads),
            scratch_shapes=[dma((16,))],
            compiler_params=pltpu.CompilerParams(vmem_limit_bytes=1024 * 1024),
        )(*grads)
        return dx, dwq.reshape(d_model, heads, head_dim), dwk, dwv, dwo.reshape(heads, head_dim, d_model)

    return jax.shard_map(
        device_grads, mesh=mesh,
        in_specs=(P("data", "model", None), P("data", "model", None), P(None, "model", None),
                  P(None, None, None), P(None, None, None), P("model", None, None)),
        out_specs=(P("data", "model", None), P("data", "model", None), P(("data", "model"), None),
                   P(("data", "model"), None), P(("data", "model"), None, None)),
        check_vma=False)
```

```python
import functools

import jax
import jax.numpy as jnp
from jax import lax
from jax.experimental import pallas as pl
from jax.experimental.pallas import tpu as pltpu
from jax.sharding import PartitionSpec as P

BF16 = jnp.bfloat16
F32 = jnp.float32
MESH = pl.DeviceIdType.MESH

NT = (((1,), (1,)), ((), ()))
NN = (((1,), (0,)), ((), ()))
TN = (((0,), (0,)), ((), ()))


def dot(a, b, dims=NN):
    return lax.dot_general(a, b, dims, preferred_element_type=F32)


def attn_kernel(n_dev, kv_heads, x_in, dy_in, wq_in, wk_in, wv_in, wo_in,
                dx_own, dwq, dwk, dwv, dwo,
                xb, dyb, wq, wo, wkv, stage_q, stage_kv, unpacked,
                acc_q, acc_kv, acc_do, qb, kvb, dob, ob, dqb, dkvp, prob_b, ds_b,
                dkv_f, dkv_peer, dkv_tot,
                dx_f, dx_tmp, psend, precv, sbuf, rbuf,
                own_sem, w_sem, kvw_sem,
                ag_send, ag_recv, d2d_send, d2d_recv, wx_sem,
                dkv_sem, ps_send, ps_recv, rs_send, rs_recv):
    n_chip = n_dev // 2
    half = n_chip // 2
    micro_n, tok, d_model = x_in.shape
    head_dim = wk_in.shape[1]
    heads = wq.shape[1] // head_dim
    n_rows = n_dev * tok
    par_rows = n_rows // 2
    me = lax.axis_index("model")
    z, c = me // 2, me % 2
    right = lax.rem(me + 2, n_dev)
    left = lax.rem(me + n_dev - 2, n_dev)
    peer = z * 2 + (1 - c)
    scale = head_dim ** -0.5

    def to(dev):
        return {"model": dev}

    barrier = pltpu.get_barrier_semaphore()
    for dev in (left, right, peer):
        pl.semaphore_signal(barrier, inc=1, device_id=to(dev), device_id_type=MESH)

    bufs = ((x_in, xb), (dy_in, dyb))
    my_row = pl.multiple_of(c * par_rows + z * tok, tok)
    own = []
    for m in range(micro_n):
        for t, (src, buf) in enumerate(bufs):
            cp = pltpu.make_async_copy(src.at[m], buf.at[m, pl.ds(my_row, tok)], own_sem.at[m, t])
            cp.start()
            own.append(cp)
    wq_cp = pltpu.make_async_copy(wq_in, stage_q, w_sem.at[0])
    wq_cp.start()
    wo_cp = pltpu.make_async_copy(wo_in, wo, w_sem.at[1])
    wo_cp.start()
    kv_rows = stage_kv.shape[1]
    n_kv = wk_in.shape[0] // kv_rows

    def kv_load(i):
        @pl.when(c == 0)
        def _():
            pltpu.make_async_copy(wk_in.at[pl.ds(i * kv_rows, kv_rows)], stage_kv.at[i % 2], kvw_sem.at[i % 2]).start()

        @pl.when(c == 1)
        def _():
            pltpu.make_async_copy(wv_in.at[pl.ds(i * kv_rows, kv_rows)], stage_kv.at[i % 2], kvw_sem.at[i % 2]).start()

    kv_load(0)
    kv_load(1)

    pl.semaphore_wait(barrier, 3)

    n_col = 2
    col_w = d_model // n_col
    sub_w = col_w // 2

    def blk(m, t, chip, col, width, core=None):
        row = pl.multiple_of((c if core is None else core) * par_rows + chip * tok, tok)
        return bufs[t][1].at[m, pl.ds(row, tok), pl.ds(col, width)]

    def send(ref, dev, ssem, rsem):
        pltpu.make_async_remote_copy(src_ref=ref, dst_ref=ref, send_sem=ssem, recv_sem=rsem,
                                     device_id=to(dev), device_id_type=MESH).start()

    def ag_start(m):
        for t in range(2):
            own[m * 2 + t].wait()
        for t in range(2):
            for j in range(n_col):
                ref = blk(m, t, z, j * col_w, col_w)
                send(ref, right, ag_send.at[m, t, j], ag_recv.at[m, t, j, 0, 0])
                send(ref, left, ag_send.at[m, t, j], ag_recv.at[m, t, j, 0, 1])
                send(ref, peer, d2d_send.at[m, t, j], d2d_recv.at[m, t, j])

    def ag_event(m, t, j, d):
        last = d == half
        for side in range(2):
            chip = lax.rem(z + (n_chip - d if side == 0 else d), n_chip)
            col, width = (j * col_w, col_w) if not last else (j * col_w + side * sub_w, sub_w)
            ref = blk(m, t, chip, col, width)
            pltpu.make_async_copy(ref, ref, ag_recv.at[m, t, j, d - 1, side]).wait()
            if d < half - 1:
                fwd = ref
            elif d == half - 1:
                fwd = blk(m, t, chip, j * col_w + side * sub_w, sub_w)
            else:
                fwd = None
            if fwd is not None:
                send(fwd, right if side == 0 else left, ag_send.at[m, t, j], ag_recv.at[m, t, j, d, side])
            send(ref, peer, d2d_send.at[m, t, j], d2d_recv.at[m, t, j])

    def peer_blocks(m, t, j, core):
        row = pl.multiple_of(core * par_rows, par_rows)
        return bufs[t][1].at[m, pl.ds(row, par_rows), pl.ds(j * col_w, col_w)]

    def d2d_wait(m, t, j):
        ref = peer_blocks(m, t, j, 1 - c)
        pltpu.make_async_copy(ref, ref, d2d_recv.at[m, t, j]).wait()

    un_rows = unpacked.shape[0]

    def prep_wq():
        wq_cp.wait()
        per = un_rows // heads

        def body(i, _):
            unpacked[...] = stage_q[pl.ds(pl.multiple_of(i * un_rows, un_rows), un_rows), :].astype(F32)
            for h in range(heads):
                wq[pl.ds(pl.multiple_of(i * per, per), per), h * head_dim:(h + 1) * head_dim] = (
                    unpacked[pl.ds(h, per, stride=heads), :].astype(BF16))
            return 0

        lax.fori_loop(0, stage_q.shape[0] // un_rows, body, 0)

    kv_col = pl.multiple_of(c * head_dim, head_dim)

    def prep_kv(i):
        pltpu.make_async_copy(wk_in.at[pl.ds(i * kv_rows, kv_rows)], stage_kv.at[i % 2], kvw_sem.at[i % 2]).wait()
        per = un_rows // kv_heads
        base = i * (kv_rows // kv_heads)

        def body(k, _):
            unpacked[...] = stage_kv[i % 2, pl.ds(pl.multiple_of(k * un_rows, un_rows), un_rows), :].astype(F32)
            wkv[pl.ds(pl.multiple_of(base + k * per, per), per), pl.ds(kv_col, head_dim)] = (
                unpacked[pl.ds(z, per, stride=kv_heads), :].astype(BF16))
            return 0

        lax.fori_loop(0, kv_rows // un_rows, body, 0)
        if i + 2 < n_kv:
            kv_load(i + 2)

    def kv_swap():
        ref = wkv.at[:, pl.ds(kv_col, head_dim)]
        pltpu.make_async_remote_copy(src_ref=ref, dst_ref=ref, send_sem=wx_sem.at[0], recv_sem=wx_sem.at[1],
                                     device_id=to(peer), device_id_type=MESH).start()

    def kv_swap_wait():
        ref = wkv.at[:, pl.ds(kv_col, head_dim)]
        pltpu.make_async_copy(ref, ref, wx_sem.at[0]).wait()
        ref = wkv.at[:, pl.ds(pl.multiple_of((1 - c) * head_dim, head_dim), head_dim)]
        pltpu.make_async_copy(ref, ref, wx_sem.at[1]).wait()

    def proj_x(m, j):
        for k in range(2):
            cols = slice(j * col_w + k * sub_w, j * col_w + (k + 1) * sub_w)
            a = dot(xb[m, :, cols], wq[cols, :])
            b = dot(xb[m, :, cols], wkv[cols, :])
            if j == 0 and k == 0:
                acc_q[...] = a
                acc_kv[...] = b
            else:
                acc_q[...] += a
                acc_kv[...] += b

    def proj_dy(m, j):
        for k in range(2):
            cols = slice(j * col_w + k * sub_w, j * col_w + (k + 1) * sub_w)
            a = dot(dyb[m, :, cols], wo[:, cols], NT)
            if j == 0 and k == 0:
                acc_do[...] = a
            else:
                acc_do[...] += a

    def round_x():
        qb[...] = acc_q[...].astype(BF16)
        kvb[...] = acc_kv[...].astype(BF16)

    def round_dy():
        dob[...] = acc_do[...].astype(BF16)

    def position(axis):
        r = lax.broadcasted_iota(jnp.int32, (n_rows, 1) if axis == 0 else (1, n_rows), axis)
        inner = r % par_rows
        return (inner // tok) * (2 * tok) + (r // par_rows) * tok + inner % tok

    def head(m, h):
        cols = slice(h * head_dim, (h + 1) * head_dim)
        q, k, v = qb[:, cols], kvb[:, :head_dim], kvb[:, head_dim:]
        do = dob[:, cols]
        s = dot(q, k, NT) * scale
        s = jnp.where(position(0) >= position(1), s, -jnp.inf)
        e = jnp.exp(s - jnp.max(s, axis=-1, keepdims=True))
        p = e / jnp.sum(e, axis=-1, keepdims=True)
        pb = p.astype(BF16)
        o = dot(pb, v).astype(BF16)
        ob[m, :, cols] = o
        dp = dot(do, v, NT)
        delta = jnp.sum(do.astype(F32) * o.astype(F32), axis=-1, keepdims=True)
        ds = (p * (dp - delta)).astype(BF16)
        prob_b[h] = pb
        ds_b[h] = ds
        dqb[m, :, cols] = (dot(ds, k) * scale).astype(BF16)

    def head_kv(m, h):
        cols = slice(h * head_dim, (h + 1) * head_dim)
        dk = dot(ds_b[h], qb[:, cols], TN) * scale
        dv = dot(prob_b[h], dob[:, cols], TN)
        if h == 0:
            dkv_f[m, :, :head_dim] = dk
            dkv_f[m, :, head_dim:] = dv
        else:
            dkv_f[m, :, :head_dim] += dk
            dkv_f[m, :, head_dim:] += dv

    def kv_round(m):
        dkvp[...] = dkv_f[m].astype(BF16)
        pltpu.make_async_remote_copy(src_ref=dkv_f.at[m], dst_ref=dkv_peer.at[m], send_sem=dkv_sem.at[m, 0],
                                     recv_sem=dkv_sem.at[m, 1], device_id=to(peer), device_id_type=MESH).start()

    def kv_total(m):
        pltpu.make_async_copy(dkv_f.at[m], dkv_f.at[m], dkv_sem.at[m, 0]).wait()
        pltpu.make_async_copy(dkv_peer.at[m], dkv_peer.at[m], dkv_sem.at[m, 1]).wait()
        dkv_tot[m] = (dkv_f[m] + dkv_peer[m]).astype(BF16)

    dw_n = 4
    dw_w = d_model // dw_n

    def put(ref, idx, val, m):
        if m == 0:
            ref[idx] = val
        else:
            ref[idx] += val

    def dw_x(m, i):
        ck = lax.rem(c * (dw_n // 2) + i, dw_n)
        start = pl.multiple_of(ck * dw_w, dw_w)
        xt = xb[m, :, pl.ds(start, dw_w)].T
        g = dot(xt, dqb[m])
        for h in range(heads):
            put(dwq, (pl.ds(start * heads + h, dw_w, stride=heads), slice(None)),
                g[:, h * head_dim:(h + 1) * head_dim], m)
        if i < dw_n // 2:
            g = dot(xt, dkv_tot[m])
            rows = slice(i * dw_w, (i + 1) * dw_w)
            put(dwk, (rows, slice(None)), g[:, :head_dim], m)
            put(dwv, (rows, slice(None)), g[:, head_dim:], m)

    def dw_o(m, i):
        cols = slice(i * dw_w, (i + 1) * dw_w)
        put(dwo, (slice(None), cols), dot(ob[m], dyb[m, :, cols], TN), m)

    def dw_steps(m):
        return ([functools.partial(dw_o, m, i) for i in range(dw_n)]
                + [functools.partial(dw_x, m, i) for i in range(dw_n)])

    rs_n = 4
    rs_w = d_model // rs_n
    rs_h = rs_w // 2

    def dx_chunk(m, j):
        cols = slice(j * rs_w, (j + 1) * rs_w)
        dx_tmp[...] = dot(dqb[m], wq[cols, :], NT) + dot(dkvp[...], wkv[cols, :], NT)
        away = pl.ds(pl.multiple_of((1 - c) * par_rows, par_rows), par_rows)
        keep = pl.ds(pl.multiple_of(c * par_rows, par_rows), par_rows)
        psend[m, :, cols] = dx_tmp[away, :].astype(BF16)
        dx_f[m, :, cols] = dx_tmp[keep, :]
        pltpu.make_async_remote_copy(src_ref=psend.at[m, :, cols], dst_ref=precv.at[m, :, cols],
                                     send_sem=ps_send.at[m, j], recv_sem=ps_recv.at[m, j],
                                     device_id=to(peer), device_id_type=MESH).start()

    def own_part(m, chip, col, width):
        rows = pl.ds(pl.multiple_of(chip * tok, tok), tok)
        return dx_f[m, rows, col:col + width] + precv[m, rows, col:col + width].astype(F32)

    def rs_send_to(m, j, side, d, col, width):
        src = sbuf.at[m, side, d - 1, :, pl.ds(col, width)]
        dst = rbuf.at[m, side, d - 1, :, pl.ds(col, width)]
        pltpu.make_async_remote_copy(src_ref=src, dst_ref=dst, send_sem=rs_send.at[m, j],
                                     recv_sem=rs_recv.at[m, j, d - 1, side],
                                     device_id=to(right if side == 0 else left), device_id_type=MESH).start()

    def chip_at(side, d):
        return lax.rem(z + (d if side == 0 else n_chip - d), n_chip)

    def rs_start(m, j):
        ref = precv.at[m, :, pl.ds(j * rs_w, rs_w)]
        pltpu.make_async_copy(ref, ref, ps_recv.at[m, j]).wait()
        for side in range(2):
            col = j * rs_w + side * rs_h
            sbuf[m, side, half - 1, :, col:col + rs_h] = own_part(m, chip_at(side, half), col, rs_h).astype(BF16)
        for side in range(2):
            rs_send_to(m, j, side, half, j * rs_w + side * rs_h, rs_h)

    def rs_event(m, j, d):
        col = j * rs_w
        for side in range(2):
            rcol, rwidth = (col + side * rs_h, rs_h) if d == half else (col, rs_w)
            ref = rbuf.at[m, side, d - 1, :, pl.ds(rcol, rwidth)]
            pltpu.make_async_copy(ref, ref, rs_recv.at[m, j, d - 1, side]).wait()
        if d == 1:
            total = own_part(m, z, col, rs_w)
            for side in range(2):
                total = total + rbuf[m, side, 0, :, col:col + rs_w].astype(F32)
            dx_own[m, :, col:col + rs_w] = total.astype(BF16)
            return
        for side in range(2):
            chip = chip_at(side, d - 1)
            if d == half:
                a, b = col + side * rs_h, col + (1 - side) * rs_h
                sbuf[m, side, d - 2, :, a:a + rs_h] = (
                    own_part(m, chip, a, rs_h) + rbuf[m, side, d - 1, :, a:a + rs_h].astype(F32)).astype(BF16)
                sbuf[m, side, d - 2, :, b:b + rs_h] = own_part(m, chip, b, rs_h).astype(BF16)
            else:
                sbuf[m, side, d - 2, :, col:col + rs_w] = (
                    own_part(m, chip, col, rs_w)
                    + rbuf[m, side, d - 1, :, col:col + rs_w].astype(F32)).astype(BF16)
        for side in range(2):
            rs_send_to(m, j, side, d - 1, col, rs_w)

    tensor_cols = [(t, j) for t in range(2) for j in range(n_col)]

    ag_start(0)
    work = [prep_wq] + [functools.partial(prep_kv, i) for i in range(n_kv)] + [kv_swap]
    slots = [(d, t, j) for d in range(1, half) for t, j in tensor_cols]
    for s, (d, t, j) in enumerate(slots):
        ag_event(0, t, j, d)
        if work:
            work.pop(0)()
    for w in work:
        w()
    ag_start(1)
    wo_cp.wait()
    kv_swap_wait()

    def finish_gather(m, extra):
        for t, j in tensor_cols:
            ag_event(m, t, j, half)
            for f in extra.get((t, j), ()):
                f()
            if (t, j) == (0, 0):
                continue
            pt, pj = tensor_cols[tensor_cols.index((t, j)) - 1]
            finish_part(m, pt, pj)
        finish_part(m, *tensor_cols[-1])

    def finish_part(m, t, j):
        d2d_wait(m, t, j)
        (proj_x if t == 0 else proj_dy)(m, j)
        if j == n_col - 1:
            (round_x if t == 0 else round_dy)()

    def attn_steps(m):
        steps = []
        for h in range(heads):
            steps.append(functools.partial(head, m, h))
            steps.append(functools.partial(head_kv, m, h))
        steps.append(functools.partial(kv_round, m))
        return steps

    finish_gather(0, {})
    work = attn_steps(0) + [functools.partial(dx_chunk, 0, j) for j in range(rs_n)]
    later = [functools.partial(kv_total, 0)] + dw_steps(0)
    for i, (d, t, j) in enumerate(slots):
        ag_event(1, t, j, d)
        if i == len(slots) - 2:
            while work:
                work.pop(0)()
            for k in range(rs_n):
                rs_start(0, k)
        (work or later).pop(0)()
    ev = functools.partial(rs_event, 0)
    ag_event(1, 0, 0, half)
    ag_event(1, 0, 1, half)
    ev(0, half)
    finish_part(1, 0, 0)
    ag_event(1, 1, 0, half)
    ev(1, half)
    ev(2, half)
    finish_part(1, 0, 1)
    ag_event(1, 1, 1, half)
    ev(3, half)
    finish_part(1, 1, 0)
    finish_part(1, 1, 1)
    attn = attn_steps(1)
    for k in range(2 * heads):
        attn.pop(0)()
        ev(k, half - 1)
    for f in attn:
        f()
    dx_chunk(1, 0)
    dx_chunk(1, 1)
    ev(0, half - 2)
    rs_start(1, 0)
    dx_chunk(1, 2)
    ev(1, half - 2)
    rs_start(1, 1)
    dx_chunk(1, 3)
    ev(2, half - 2)
    rs_start(1, 2)
    later.pop(0)()
    ev(3, half - 2)
    later.pop(0)()
    rs_start(1, 3)
    later += [functools.partial(kv_total, 1)] + dw_steps(1)
    for j in range(rs_n):
        if j < rs_n - 1:
            later.pop(0)()
        rs_event(1, j, half)
    for j in range(rs_n):
        rs_event(1, j, half - 1)
        later.pop(0)()
    for j in range(rs_n):
        rs_event(0, j, 1)
        if later:
            later.pop(0)()
        rs_event(1, j, half - 2)
        if later:
            later.pop(0)()
    for f in later:
        f()
    for m in range(micro_n):
        for t, j in tensor_cols:
            ref = bufs[t][1].at[m, pl.ds(0, (n_chip - 1) * tok), pl.ds(j * col_w, col_w)]
            pltpu.make_async_copy(ref, ref, ag_send.at[m, t, j]).wait()
            ref = peer_blocks(m, t, j, c)
            pltpu.make_async_copy(ref, ref, d2d_send.at[m, t, j]).wait()
        for j in range(rs_n):
            ref = psend.at[m, :, pl.ds(j * rs_w, rs_w)]
            pltpu.make_async_copy(ref, ref, ps_send.at[m, j]).wait()

    def rs_drain(m):
        for j in range(rs_n):
            ref = psend.at[m, pl.ds(0, (n_chip - 1) * tok), pl.ds(j * rs_w, rs_w)]
            pltpu.make_async_copy(ref, ref, rs_send.at[m, j]).wait()

    rs_drain(0)
    for j in range(rs_n):
        rs_event(1, j, 1)
    rs_drain(1)


def copy_kernel(n, *refs):
    srcs, dsts, sem = refs[:n], refs[n:2 * n], refs[2 * n]
    pairs = []
    for a, b in zip(srcs, dsts):
        parts = max(1, a.shape[0] // 2560) if a.shape[-1] < 1024 else a.shape[0] // 64 or 1
        rows = a.shape[0] // parts
        pairs += [(a.at[pl.ds(i * rows, rows)], b.at[pl.ds(i * rows, rows)]) for i in range(parts)]
    copies = [pltpu.make_async_copy(a, b, sem.at[i]) for i, (a, b) in enumerate(pairs)]
    for cp in copies:
        cp.start()
    for cp in copies:
        cp.wait()


def solution(mesh):
    n_dev = mesh.shape["model"]

    def device_grads(x_loc, dy_loc, w_q, w_k, w_v, w_o):
        micro_n, tok, d_model = x_loc.shape
        heads, head_dim = w_q.shape[1], w_q.shape[2]
        kv_heads = w_k.shape[1]
        n_rows = tok * n_dev
        par_rows = n_rows // 2
        hd = heads * head_dim
        n_chip = n_dev // 2
        half = n_chip // 2
        any_spec = pl.BlockSpec(memory_space=pl.ANY)
        dma = pltpu.SemaphoreType.DMA
        scratch = [
            pltpu.VMEM((micro_n, n_rows, d_model), BF16),
            pltpu.VMEM((micro_n, n_rows, d_model), BF16),
            pltpu.VMEM((d_model, hd), BF16),
            pltpu.VMEM((hd, d_model), BF16),
            pltpu.VMEM((d_model, 2 * head_dim), BF16),
            pltpu.VMEM((d_model * heads, head_dim), BF16),
            pltpu.VMEM((2, d_model * kv_heads // 8, head_dim), BF16),
            pltpu.VMEM((512, head_dim), F32),
            pltpu.VMEM((n_rows, hd), F32),
            pltpu.VMEM((n_rows, 2 * head_dim), F32),
            pltpu.VMEM((n_rows, hd), F32),
            pltpu.VMEM((n_rows, hd), BF16),
            pltpu.VMEM((n_rows, 2 * head_dim), BF16),
            pltpu.VMEM((n_rows, hd), BF16),
            pltpu.VMEM((micro_n, n_rows, hd), BF16),
            pltpu.VMEM((micro_n, n_rows, hd), BF16),
            pltpu.VMEM((n_rows, 2 * head_dim), BF16),
            pltpu.VMEM((heads, n_rows, n_rows), BF16),
            pltpu.VMEM((heads, n_rows, n_rows), BF16),
            pltpu.VMEM((micro_n, n_rows, 2 * head_dim), F32),
            pltpu.VMEM((micro_n, n_rows, 2 * head_dim), F32),
            pltpu.VMEM((micro_n, n_rows, 2 * head_dim), BF16),
            pltpu.VMEM((micro_n, par_rows, d_model), F32),
            pltpu.VMEM((n_rows, d_model // 4), F32),
            pltpu.VMEM((micro_n, par_rows, d_model), BF16),
            pltpu.VMEM((micro_n, par_rows, d_model), BF16),
            pltpu.VMEM((micro_n, 2, half, tok, d_model), BF16),
            pltpu.VMEM((micro_n, 2, half, tok, d_model), BF16),
            dma((micro_n, 2)), dma((2,)), dma((2,)),
            dma((micro_n, 2, 2)), dma((micro_n, 2, 2, half, 2)),
            dma((micro_n, 2, 2)), dma((micro_n, 2, 2)), dma((2,)),
            dma((micro_n, 2)), dma((micro_n, 4)), dma((micro_n, 4)),
            dma((micro_n, 4)), dma((micro_n, 4, half, 2)),
        ]
        dx, dwq, dwk, dwv, dwo = pl.pallas_call(
            functools.partial(attn_kernel, n_dev, kv_heads),
            out_shape=(
                pltpu.VMEM((micro_n, tok, d_model), BF16),
                pltpu.VMEM((d_model * heads, head_dim), F32),
                pltpu.VMEM((d_model // 2, head_dim), F32),
                pltpu.VMEM((d_model // 2, head_dim), F32),
                pltpu.VMEM((hd, d_model), F32),
            ),
            in_specs=[any_spec] * 6,
            out_specs=(pl.BlockSpec(memory_space=pltpu.VMEM),) * 5,
            scratch_shapes=scratch,
            compiler_params=pltpu.CompilerParams(collective_id=0, has_side_effects=True,
                                                 vmem_limit_bytes=46 * 1024 * 1024),
        )(x_loc, dy_loc, w_q.reshape(d_model * heads, head_dim), w_k.reshape(d_model * kv_heads, head_dim),
          w_v.reshape(d_model * kv_heads, head_dim), w_o.reshape(hd, d_model))

        grads = (dx, dwq, dwk, dwv, dwo)
        dx, dwq, dwk, dwv, dwo = pl.pallas_call(
            functools.partial(copy_kernel, len(grads)),
            out_shape=tuple(jax.ShapeDtypeStruct(g.shape, g.dtype) for g in grads),
            in_specs=[pl.BlockSpec(memory_space=pltpu.VMEM)] * len(grads),
            out_specs=(any_spec,) * len(grads),
            scratch_shapes=[dma((16,))],
            compiler_params=pltpu.CompilerParams(vmem_limit_bytes=1024 * 1024),
        )(*grads)
        return dx, dwq.reshape(d_model, heads, head_dim), dwk, dwv, dwo.reshape(heads, head_dim, d_model)

    return jax.shard_map(
        device_grads, mesh=mesh,
        in_specs=(P("data", "model", None), P("data", "model", None), P(None, "model", None),
                  P(None, None, None), P(None, None, None), P("model", None, None)),
        out_specs=(P("data", "model", None), P("data", "model", None), P(("data", "model"), None),
                   P(("data", "model"), None), P(("data", "model"), None, None)),
        check_vma=False)
```

```python
import functools

import jax
import jax.numpy as jnp
from jax import lax
from jax.experimental import pallas as pl
from jax.experimental.pallas import tpu as pltpu
from jax.sharding import PartitionSpec as P

BF16 = jnp.bfloat16
F32 = jnp.float32
MESH = pl.DeviceIdType.MESH

NT = (((1,), (1,)), ((), ()))
NN = (((1,), (0,)), ((), ()))
TN = (((0,), (0,)), ((), ()))


def dot(a, b, dims=NN):
    return lax.dot_general(a, b, dims, preferred_element_type=F32)


def attn_kernel(n_dev, kv_heads, x_in, dy_in, wq_in, wk_in, wv_in, wo_in,
                dx_own, dwq, dwk, dwv, dwo,
                xb, dyb, wall, wo, stage_q, stage_kv, unpacked,
                acc_x, acc_do, qb, kvb, dob, ob, dqb, dkvp, prob_b, ds_b,
                dkv_f, dkv_peer, dkv_tot,
                dx_f, psend, precv, sbuf, rbuf,
                own_sem, w_sem, kvw_sem,
                ag_send, ag_recv, d2d_send, d2d_recv, wx_sem,
                dkv_sem, ps_send, ps_recv, rs_send, rs_recv):
    n_chip = n_dev // 2
    half = n_chip // 2
    micro_n, tok, d_model = x_in.shape
    head_dim = wk_in.shape[1]
    hd = wo.shape[0]
    heads = hd // head_dim
    n_rows = n_dev * tok
    par_rows = n_rows // 2
    me = lax.axis_index("model")
    z, c = me // 2, me % 2
    right = lax.rem(me + 2, n_dev)
    left = lax.rem(me + n_dev - 2, n_dev)
    peer = z * 2 + (1 - c)
    scale = head_dim ** -0.5

    def to(dev):
        return {"model": dev}

    barrier = pltpu.get_barrier_semaphore()
    for dev in (left, right, peer):
        pl.semaphore_signal(barrier, inc=1, device_id=to(dev), device_id_type=MESH)

    bufs = ((x_in, xb), (dy_in, dyb))
    my_row = pl.multiple_of(c * par_rows + z * tok, tok)
    own = []
    for m in range(micro_n):
        for t, (src, buf) in enumerate(bufs):
            cp = pltpu.make_async_copy(src.at[m], buf.at[m, pl.ds(my_row, tok)], own_sem.at[m, t])
            cp.start()
            own.append(cp)
    wq_cp = pltpu.make_async_copy(wq_in, stage_q, w_sem.at[0])
    wq_cp.start()
    wo_cp = pltpu.make_async_copy(wo_in, wo, w_sem.at[1])
    wo_cp.start()
    kv_rows = stage_kv.shape[1]
    n_kv = wk_in.shape[0] // kv_rows

    def kv_load(i):
        @pl.when(c == 0)
        def _():
            pltpu.make_async_copy(wk_in.at[pl.ds(i * kv_rows, kv_rows)], stage_kv.at[i % 2], kvw_sem.at[i % 2]).start()

        @pl.when(c == 1)
        def _():
            pltpu.make_async_copy(wv_in.at[pl.ds(i * kv_rows, kv_rows)], stage_kv.at[i % 2], kvw_sem.at[i % 2]).start()

    kv_load(0)
    kv_load(1)

    pl.semaphore_wait(barrier, 3)

    n_col = 2
    col_w = d_model // n_col
    sub_w = col_w // 2

    def blk(m, t, chip, col, width, core=None):
        row = pl.multiple_of((c if core is None else core) * par_rows + chip * tok, tok)
        return bufs[t][1].at[m, pl.ds(row, tok), pl.ds(col, width)]

    def send(ref, dev, ssem, rsem):
        pltpu.make_async_remote_copy(src_ref=ref, dst_ref=ref, send_sem=ssem, recv_sem=rsem,
                                     device_id=to(dev), device_id_type=MESH).start()

    def ag_start(m):
        for t in range(2):
            own[m * 2 + t].wait()
        for t in range(2):
            for j in range(n_col):
                ref = blk(m, t, z, j * col_w, col_w)
                send(ref, right, ag_send.at[m, t, j], ag_recv.at[m, t, j, 0, 0])
                send(ref, left, ag_send.at[m, t, j], ag_recv.at[m, t, j, 0, 1])
                send(ref, peer, d2d_send.at[m, t, j], d2d_recv.at[m, t, j])

    def ag_event(m, t, j, d):
        last = d == half
        for side in range(2):
            chip = lax.rem(z + (n_chip - d if side == 0 else d), n_chip)
            col, width = (j * col_w, col_w) if not last else (j * col_w + side * sub_w, sub_w)
            ref = blk(m, t, chip, col, width)
            pltpu.make_async_copy(ref, ref, ag_recv.at[m, t, j, d - 1, side]).wait()
            if d < half - 1:
                fwd = ref
            elif d == half - 1:
                fwd = blk(m, t, chip, j * col_w + side * sub_w, sub_w)
            else:
                fwd = None
            if fwd is not None:
                send(fwd, right if side == 0 else left, ag_send.at[m, t, j], ag_recv.at[m, t, j, d, side])
            send(ref, peer, d2d_send.at[m, t, j], d2d_recv.at[m, t, j])

    def peer_blocks(m, t, j, core):
        row = pl.multiple_of(core * par_rows, par_rows)
        return bufs[t][1].at[m, pl.ds(row, par_rows), pl.ds(j * col_w, col_w)]

    def d2d_wait(m, t, j):
        ref = peer_blocks(m, t, j, 1 - c)
        pltpu.make_async_copy(ref, ref, d2d_recv.at[m, t, j]).wait()

    un_rows = unpacked.shape[0]

    def prep_wq():
        wq_cp.wait()
        per = un_rows // heads

        def body(i, _):
            unpacked[...] = stage_q[pl.ds(pl.multiple_of(i * un_rows, un_rows), un_rows), :].astype(F32)
            for h in range(heads):
                wall[pl.ds(pl.multiple_of(i * per, per), per), h * head_dim:(h + 1) * head_dim] = (
                    unpacked[pl.ds(h, per, stride=heads), :].astype(BF16))
            return 0

        lax.fori_loop(0, stage_q.shape[0] // un_rows, body, 0)

    kv_col = pl.multiple_of(hd + c * head_dim, head_dim)

    def prep_kv(i):
        pltpu.make_async_copy(wk_in.at[pl.ds(i * kv_rows, kv_rows)], stage_kv.at[i % 2], kvw_sem.at[i % 2]).wait()
        per = un_rows // kv_heads
        base = i * (kv_rows // kv_heads)

        def body(k, _):
            unpacked[...] = stage_kv[i % 2, pl.ds(pl.multiple_of(k * un_rows, un_rows), un_rows), :].astype(F32)
            wall[pl.ds(pl.multiple_of(base + k * per, per), per), pl.ds(kv_col, head_dim)] = (
                unpacked[pl.ds(z, per, stride=kv_heads), :].astype(BF16))
            return 0

        lax.fori_loop(0, kv_rows // un_rows, body, 0)
        if i + 2 < n_kv:
            kv_load(i + 2)

    def kv_swap():
        ref = wall.at[:, pl.ds(kv_col, head_dim)]
        pltpu.make_async_remote_copy(src_ref=ref, dst_ref=ref, send_sem=wx_sem.at[0], recv_sem=wx_sem.at[1],
                                     device_id=to(peer), device_id_type=MESH).start()

    def kv_swap_wait():
        ref = wall.at[:, pl.ds(kv_col, head_dim)]
        pltpu.make_async_copy(ref, ref, wx_sem.at[0]).wait()
        ref = wall.at[:, pl.ds(pl.multiple_of(hd + (1 - c) * head_dim, head_dim), head_dim)]
        pltpu.make_async_copy(ref, ref, wx_sem.at[1]).wait()

    def proj_x(m, j):
        for k in range(2):
            cols = slice(j * col_w + k * sub_w, j * col_w + (k + 1) * sub_w)
            a = dot(xb[m, :, cols], wall[cols, :])
            if j == 0 and k == 0:
                acc_x[...] = a
            else:
                acc_x[...] += a

    def proj_dy(m, j):
        for k in range(2):
            cols = slice(j * col_w + k * sub_w, j * col_w + (k + 1) * sub_w)
            a = dot(dyb[m, :, cols], wo[:, cols], NT)
            if j == 0 and k == 0:
                acc_do[...] = a
            else:
                acc_do[...] += a

    def round_x():
        qb[...] = acc_x[:, :hd].astype(BF16)
        kvb[...] = acc_x[:, hd:].astype(BF16)

    def round_dy():
        dob[...] = acc_do[...].astype(BF16)

    def position(axis):
        r = lax.broadcasted_iota(jnp.int32, (n_rows, 1) if axis == 0 else (1, n_rows), axis)
        inner = r % par_rows
        return (inner // tok) * (2 * tok) + (r // par_rows) * tok + inner % tok

    def head(m, h):
        cols = slice(h * head_dim, (h + 1) * head_dim)
        q, k, v = qb[:, cols], kvb[:, :head_dim], kvb[:, head_dim:]
        do = dob[:, cols]
        s = dot(q, k, NT) * scale
        s = jnp.where(position(0) >= position(1), s, -jnp.inf)
        e = jnp.exp(s - jnp.max(s, axis=-1, keepdims=True))
        p = e / jnp.sum(e, axis=-1, keepdims=True)
        pb = p.astype(BF16)
        o = dot(pb, v).astype(BF16)
        ob[m, :, cols] = o
        dp = dot(do, v, NT)
        delta = jnp.sum(do.astype(F32) * o.astype(F32), axis=-1, keepdims=True)
        ds = (p * (dp - delta)).astype(BF16)
        prob_b[h] = pb
        ds_b[h] = ds
        dqb[m, :, cols] = (dot(ds, k) * scale).astype(BF16)

    def head_kv(m, h):
        cols = slice(h * head_dim, (h + 1) * head_dim)
        dk = dot(ds_b[h], qb[:, cols], TN) * scale
        dv = dot(prob_b[h], dob[:, cols], TN)
        if h == 0:
            dkv_f[m, :, :head_dim] = dk
            dkv_f[m, :, head_dim:] = dv
        else:
            dkv_f[m, :, :head_dim] += dk
            dkv_f[m, :, head_dim:] += dv

    def kv_round(m):
        dkvp[...] = dkv_f[m].astype(BF16)
        pltpu.make_async_remote_copy(src_ref=dkv_f.at[m], dst_ref=dkv_peer.at[m], send_sem=dkv_sem.at[m, 0],
                                     recv_sem=dkv_sem.at[m, 1], device_id=to(peer), device_id_type=MESH).start()

    def kv_total(m):
        pltpu.make_async_copy(dkv_f.at[m], dkv_f.at[m], dkv_sem.at[m, 0]).wait()
        pltpu.make_async_copy(dkv_peer.at[m], dkv_peer.at[m], dkv_sem.at[m, 1]).wait()
        dkv_tot[m] = (dkv_f[m] + dkv_peer[m]).astype(BF16)

    dw_n = 4
    dw_w = d_model // dw_n

    def put(ref, idx, val, m):
        if m == 0:
            ref[idx] = val
        else:
            ref[idx] += val

    def dw_x(m, i):
        ck = lax.rem(c * (dw_n // 2) + i, dw_n)
        start = pl.multiple_of(ck * dw_w, dw_w)
        xt = xb[m, :, pl.ds(start, dw_w)].T
        g = dot(xt, dqb[m])
        for h in range(heads):
            put(dwq, (pl.ds(start * heads + h, dw_w, stride=heads), slice(None)),
                g[:, h * head_dim:(h + 1) * head_dim], m)
        if i < dw_n // 2:
            g = dot(xt, dkv_tot[m])
            rows = slice(i * dw_w, (i + 1) * dw_w)
            put(dwk, (rows, slice(None)), g[:, :head_dim], m)
            put(dwv, (rows, slice(None)), g[:, head_dim:], m)

    def dw_o(m, i):
        cols = slice(i * dw_w, (i + 1) * dw_w)
        put(dwo, (slice(None), cols), dot(ob[m], dyb[m, :, cols], TN), m)

    def dw_steps(m):
        return ([functools.partial(dw_o, m, i) for i in range(dw_n)]
                + [functools.partial(dw_x, m, i) for i in range(dw_n)])

    rs_n = 4
    rs_w = d_model // rs_n
    rs_h = rs_w // 2

    def dx_chunk(m, j):
        cols = slice(j * rs_w, (j + 1) * rs_w)
        away = pl.ds(pl.multiple_of((1 - c) * par_rows, par_rows), par_rows)
        keep = pl.ds(pl.multiple_of(c * par_rows, par_rows), par_rows)
        lhs = jnp.concatenate([jnp.concatenate([dqb[m, rows, :], dkvp[rows, :]], axis=1) for rows in (away, keep)], axis=0)
        part = dot(lhs, wall[cols, :], NT)
        psend[m, :, cols] = part[:par_rows].astype(BF16)
        dx_f[m, :, cols] = part[par_rows:]
        pltpu.make_async_remote_copy(src_ref=psend.at[m, :, cols], dst_ref=precv.at[m, :, cols],
                                     send_sem=ps_send.at[m, j], recv_sem=ps_recv.at[m, j],
                                     device_id=to(peer), device_id_type=MESH).start()

    def own_part(m, chip, col, width):
        rows = pl.ds(pl.multiple_of(chip * tok, tok), tok)
        return dx_f[m, rows, col:col + width] + precv[m, rows, col:col + width].astype(F32)

    def rs_send_to(m, j, side, d, col, width):
        src = sbuf.at[m, side, d - 1, :, pl.ds(col, width)]
        dst = rbuf.at[m, side, d - 1, :, pl.ds(col, width)]
        pltpu.make_async_remote_copy(src_ref=src, dst_ref=dst, send_sem=rs_send.at[m, j],
                                     recv_sem=rs_recv.at[m, j, d - 1, side],
                                     device_id=to(right if side == 0 else left), device_id_type=MESH).start()

    def chip_at(side, d):
        return lax.rem(z + (d if side == 0 else n_chip - d), n_chip)

    def rs_start(m, j):
        ref = precv.at[m, :, pl.ds(j * rs_w, rs_w)]
        pltpu.make_async_copy(ref, ref, ps_recv.at[m, j]).wait()
        for side in range(2):
            col = j * rs_w + side * rs_h
            sbuf[m, side, half - 1, :, col:col + rs_h] = own_part(m, chip_at(side, half), col, rs_h).astype(BF16)
        for side in range(2):
            rs_send_to(m, j, side, half, j * rs_w + side * rs_h, rs_h)

    def rs_event(m, j, d):
        col = j * rs_w
        for side in range(2):
            rcol, rwidth = (col + side * rs_h, rs_h) if d == half else (col, rs_w)
            ref = rbuf.at[m, side, d - 1, :, pl.ds(rcol, rwidth)]
            pltpu.make_async_copy(ref, ref, rs_recv.at[m, j, d - 1, side]).wait()
        if d == 1:
            total = own_part(m, z, col, rs_w)
            for side in range(2):
                total = total + rbuf[m, side, 0, :, col:col + rs_w].astype(F32)
            dx_own[m, :, col:col + rs_w] = total.astype(BF16)
            return
        for side in range(2):
            chip = chip_at(side, d - 1)
            if d == half:
                a, b = col + side * rs_h, col + (1 - side) * rs_h
                sbuf[m, side, d - 2, :, a:a + rs_h] = (
                    own_part(m, chip, a, rs_h) + rbuf[m, side, d - 1, :, a:a + rs_h].astype(F32)).astype(BF16)
                sbuf[m, side, d - 2, :, b:b + rs_h] = own_part(m, chip, b, rs_h).astype(BF16)
            else:
                sbuf[m, side, d - 2, :, col:col + rs_w] = (
                    own_part(m, chip, col, rs_w)
                    + rbuf[m, side, d - 1, :, col:col + rs_w].astype(F32)).astype(BF16)
        for side in range(2):
            rs_send_to(m, j, side, d - 1, col, rs_w)

    tensor_cols = [(t, j) for t in range(2) for j in range(n_col)]

    ag_start(0)
    work = [prep_wq] + [functools.partial(prep_kv, i) for i in range(n_kv)] + [kv_swap]
    slots = [(d, t, j) for d in range(1, half) for t, j in tensor_cols]
    for s, (d, t, j) in enumerate(slots):
        ag_event(0, t, j, d)
        if work:
            work.pop(0)()
    for w in work:
        w()
    ag_start(1)
    wo_cp.wait()
    kv_swap_wait()

    def finish_gather(m, extra):
        for t, j in tensor_cols:
            ag_event(m, t, j, half)
            for f in extra.get((t, j), ()):
                f()
            if (t, j) == (0, 0):
                continue
            pt, pj = tensor_cols[tensor_cols.index((t, j)) - 1]
            finish_part(m, pt, pj)
        finish_part(m, *tensor_cols[-1])

    def finish_part(m, t, j):
        d2d_wait(m, t, j)
        (proj_x if t == 0 else proj_dy)(m, j)
        if j == n_col - 1:
            (round_x if t == 0 else round_dy)()

    def attn_steps(m):
        steps = []
        for h in range(heads):
            steps.append(functools.partial(head, m, h))
            steps.append(functools.partial(head_kv, m, h))
        steps.append(functools.partial(kv_round, m))
        return steps

    finish_gather(0, {})
    work = attn_steps(0) + [functools.partial(dx_chunk, 0, j) for j in range(rs_n)]
    later = [functools.partial(kv_total, 0)] + dw_steps(0)
    for i, (d, t, j) in enumerate(slots):
        ag_event(1, t, j, d)
        if i == len(slots) - 2:
            while work:
                work.pop(0)()
            for k in range(rs_n):
                rs_start(0, k)
        (work or later).pop(0)()
    ev = functools.partial(rs_event, 0)
    ag_event(1, 0, 0, half)
    ag_event(1, 0, 1, half)
    ev(0, half)
    finish_part(1, 0, 0)
    ag_event(1, 1, 0, half)
    ev(1, half)
    ev(2, half)
    finish_part(1, 0, 1)
    ag_event(1, 1, 1, half)
    ev(3, half)
    finish_part(1, 1, 0)
    finish_part(1, 1, 1)
    attn = attn_steps(1)
    for k in range(2 * heads):
        attn.pop(0)()
        ev(k, half - 1)
    for f in attn:
        f()
    dx_chunk(1, 0)
    dx_chunk(1, 1)
    ev(0, half - 2)
    rs_start(1, 0)
    dx_chunk(1, 2)
    ev(1, half - 2)
    rs_start(1, 1)
    dx_chunk(1, 3)
    ev(2, half - 2)
    rs_start(1, 2)
    later.pop(0)()
    ev(3, half - 2)
    later.pop(0)()
    rs_start(1, 3)
    later += [functools.partial(kv_total, 1)] + dw_steps(1)
    for j in range(rs_n):
        if j < rs_n - 1:
            later.pop(0)()
        rs_event(1, j, half)
    for j in range(rs_n):
        rs_event(1, j, half - 1)
        later.pop(0)()
    for j in range(rs_n):
        rs_event(0, j, 1)
        if later:
            later.pop(0)()
        rs_event(1, j, half - 2)
        if later:
            later.pop(0)()
    for f in later:
        f()
    for m in range(micro_n):
        for t, j in tensor_cols:
            ref = bufs[t][1].at[m, pl.ds(0, (n_chip - 1) * tok), pl.ds(j * col_w, col_w)]
            pltpu.make_async_copy(ref, ref, ag_send.at[m, t, j]).wait()
            ref = peer_blocks(m, t, j, c)
            pltpu.make_async_copy(ref, ref, d2d_send.at[m, t, j]).wait()
        for j in range(rs_n):
            ref = psend.at[m, :, pl.ds(j * rs_w, rs_w)]
            pltpu.make_async_copy(ref, ref, ps_send.at[m, j]).wait()

    def rs_drain(m):
        for j in range(rs_n):
            ref = psend.at[m, pl.ds(0, (n_chip - 1) * tok), pl.ds(j * rs_w, rs_w)]
            pltpu.make_async_copy(ref, ref, rs_send.at[m, j]).wait()

    rs_drain(0)
    for j in range(rs_n):
        rs_event(1, j, 1)
    rs_drain(1)


def copy_kernel(n, *refs):
    srcs, dsts, sem = refs[:n], refs[n:2 * n], refs[2 * n]
    pairs = []
    for a, b in zip(srcs, dsts):
        parts = max(1, a.shape[0] // 2560) if a.shape[-1] < 1024 else a.shape[0] // 64 or 1
        rows = a.shape[0] // parts
        pairs += [(a.at[pl.ds(i * rows, rows)], b.at[pl.ds(i * rows, rows)]) for i in range(parts)]
    copies = [pltpu.make_async_copy(a, b, sem.at[i]) for i, (a, b) in enumerate(pairs)]
    for cp in copies:
        cp.start()
    for cp in copies:
        cp.wait()


def solution(mesh):
    n_dev = mesh.shape["model"]

    def device_grads(x_loc, dy_loc, w_q, w_k, w_v, w_o):
        micro_n, tok, d_model = x_loc.shape
        heads, head_dim = w_q.shape[1], w_q.shape[2]
        kv_heads = w_k.shape[1]
        n_rows = tok * n_dev
        par_rows = n_rows // 2
        hd = heads * head_dim
        n_chip = n_dev // 2
        half = n_chip // 2
        any_spec = pl.BlockSpec(memory_space=pl.ANY)
        dma = pltpu.SemaphoreType.DMA
        scratch = [
            pltpu.VMEM((micro_n, n_rows, d_model), BF16),
            pltpu.VMEM((micro_n, n_rows, d_model), BF16),
            pltpu.VMEM((d_model, hd + 2 * head_dim), BF16),
            pltpu.VMEM((hd, d_model), BF16),
            pltpu.VMEM((d_model * heads, head_dim), BF16),
            pltpu.VMEM((2, d_model * kv_heads // 8, head_dim), BF16),
            pltpu.VMEM((512, head_dim), F32),
            pltpu.VMEM((n_rows, hd + 2 * head_dim), F32),
            pltpu.VMEM((n_rows, hd), F32),
            pltpu.VMEM((n_rows, hd), BF16),
            pltpu.VMEM((n_rows, 2 * head_dim), BF16),
            pltpu.VMEM((n_rows, hd), BF16),
            pltpu.VMEM((micro_n, n_rows, hd), BF16),
            pltpu.VMEM((micro_n, n_rows, hd), BF16),
            pltpu.VMEM((n_rows, 2 * head_dim), BF16),
            pltpu.VMEM((heads, n_rows, n_rows), BF16),
            pltpu.VMEM((heads, n_rows, n_rows), BF16),
            pltpu.VMEM((micro_n, n_rows, 2 * head_dim), F32),
            pltpu.VMEM((micro_n, n_rows, 2 * head_dim), F32),
            pltpu.VMEM((micro_n, n_rows, 2 * head_dim), BF16),
            pltpu.VMEM((micro_n, par_rows, d_model), F32),
            pltpu.VMEM((micro_n, par_rows, d_model), BF16),
            pltpu.VMEM((micro_n, par_rows, d_model), BF16),
            pltpu.VMEM((micro_n, 2, half, tok, d_model), BF16),
            pltpu.VMEM((micro_n, 2, half, tok, d_model), BF16),
            dma((micro_n, 2)), dma((2,)), dma((2,)),
            dma((micro_n, 2, 2)), dma((micro_n, 2, 2, half, 2)),
            dma((micro_n, 2, 2)), dma((micro_n, 2, 2)), dma((2,)),
            dma((micro_n, 2)), dma((micro_n, 4)), dma((micro_n, 4)),
            dma((micro_n, 4)), dma((micro_n, 4, half, 2)),
        ]
        dx, dwq, dwk, dwv, dwo = pl.pallas_call(
            functools.partial(attn_kernel, n_dev, kv_heads),
            out_shape=(
                pltpu.VMEM((micro_n, tok, d_model), BF16),
                pltpu.VMEM((d_model * heads, head_dim), F32),
                pltpu.VMEM((d_model // 2, head_dim), F32),
                pltpu.VMEM((d_model // 2, head_dim), F32),
                pltpu.VMEM((hd, d_model), F32),
            ),
            in_specs=[any_spec] * 6,
            out_specs=(pl.BlockSpec(memory_space=pltpu.VMEM),) * 5,
            scratch_shapes=scratch,
            compiler_params=pltpu.CompilerParams(collective_id=0, has_side_effects=True,
                                                 vmem_limit_bytes=46 * 1024 * 1024),
        )(x_loc, dy_loc, w_q.reshape(d_model * heads, head_dim), w_k.reshape(d_model * kv_heads, head_dim),
          w_v.reshape(d_model * kv_heads, head_dim), w_o.reshape(hd, d_model))

        grads = (dx, dwq, dwk, dwv, dwo)
        dx, dwq, dwk, dwv, dwo = pl.pallas_call(
            functools.partial(copy_kernel, len(grads)),
            out_shape=tuple(jax.ShapeDtypeStruct(g.shape, g.dtype) for g in grads),
            in_specs=[pl.BlockSpec(memory_space=pltpu.VMEM)] * len(grads),
            out_specs=(any_spec,) * len(grads),
            scratch_shapes=[dma((16,))],
            compiler_params=pltpu.CompilerParams(vmem_limit_bytes=1024 * 1024),
        )(*grads)
        return dx, dwq.reshape(d_model, heads, head_dim), dwk, dwv, dwo.reshape(heads, head_dim, d_model)

    return jax.shard_map(
        device_grads, mesh=mesh,
        in_specs=(P("data", "model", None), P("data", "model", None), P(None, "model", None),
                  P(None, None, None), P(None, None, None), P("model", None, None)),
        out_specs=(P("data", "model", None), P("data", "model", None), P(("data", "model"), None),
                   P(("data", "model"), None), P(("data", "model"), None, None)),
        check_vma=False)
```

```python
import functools

import jax
import jax.numpy as jnp
from jax import lax
from jax.experimental import pallas as pl
from jax.experimental.pallas import tpu as pltpu
from jax.sharding import PartitionSpec as P

BF16 = jnp.bfloat16
F32 = jnp.float32
MESH = pl.DeviceIdType.MESH

NT = (((1,), (1,)), ((), ()))
NN = (((1,), (0,)), ((), ()))
TN = (((0,), (0,)), ((), ()))


def dot(a, b, dims=NN):
    return lax.dot_general(a, b, dims, preferred_element_type=F32)


def attn_kernel(n_dev, kv_heads, x_in, dy_in, wq_in, wk_in, wv_in, wo_in,
                dx_own, dwq, dwk, dwv, dwo,
                xb, dyb, wall, wo, stage_q, stage_kv, unpacked,
                acc_x, acc_do, qb, kvb, dob, ob, dqb, dkvp, prob_b, ds_b,
                dkv_f, dkv_peer, dkv_tot,
                dx_f, psend, precv, sbuf, rbuf,
                own_sem, w_sem, kvw_sem,
                ag_send, ag_recv, d2d_send, d2d_recv, wx_sem,
                dkv_sem, ps_send, ps_recv, rs_send, rs_recv):
    n_chip = n_dev // 2
    half = n_chip // 2
    micro_n, tok, d_model = x_in.shape
    head_dim = wk_in.shape[1]
    hd = wo.shape[0]
    heads = hd // head_dim
    n_rows = n_dev * tok
    par_rows = n_rows // 2
    me = lax.axis_index("model")
    z, c = me // 2, me % 2
    right = lax.rem(me + 2, n_dev)
    left = lax.rem(me + n_dev - 2, n_dev)
    peer = z * 2 + (1 - c)
    scale = head_dim ** -0.5

    def to(dev):
        return {"model": dev}

    barrier = pltpu.get_barrier_semaphore()
    for dev in (left, right, peer):
        pl.semaphore_signal(barrier, inc=1, device_id=to(dev), device_id_type=MESH)

    bufs = ((x_in, xb), (dy_in, dyb))
    my_row = pl.multiple_of(c * par_rows + z * tok, tok)
    own = []
    for m in range(micro_n):
        for t, (src, buf) in enumerate(bufs):
            cp = pltpu.make_async_copy(src.at[m], buf.at[m, pl.ds(my_row, tok)], own_sem.at[m, t])
            cp.start()
            own.append(cp)
    wq_cp = pltpu.make_async_copy(wq_in, stage_q, w_sem.at[0])
    wq_cp.start()
    wo_cp = pltpu.make_async_copy(wo_in, wo, w_sem.at[1])
    wo_cp.start()
    kv_rows = stage_kv.shape[1]
    n_kv = wk_in.shape[0] // kv_rows

    def kv_load(i):
        @pl.when(c == 0)
        def _():
            pltpu.make_async_copy(wk_in.at[pl.ds(i * kv_rows, kv_rows)], stage_kv.at[i % 2], kvw_sem.at[i % 2]).start()

        @pl.when(c == 1)
        def _():
            pltpu.make_async_copy(wv_in.at[pl.ds(i * kv_rows, kv_rows)], stage_kv.at[i % 2], kvw_sem.at[i % 2]).start()

    kv_load(0)
    kv_load(1)

    pl.semaphore_wait(barrier, 3)

    n_col = 2
    col_w = d_model // n_col
    sub_w = col_w // 2

    def blk(m, t, chip, col, width, core=None):
        row = pl.multiple_of((c if core is None else core) * par_rows + chip * tok, tok)
        return bufs[t][1].at[m, pl.ds(row, tok), pl.ds(col, width)]

    def send(ref, dev, ssem, rsem):
        pltpu.make_async_remote_copy(src_ref=ref, dst_ref=ref, send_sem=ssem, recv_sem=rsem,
                                     device_id=to(dev), device_id_type=MESH).start()

    def ag_start(m):
        for t in range(2):
            own[m * 2 + t].wait()
        for t in range(2):
            for j in range(n_col):
                ref = blk(m, t, z, j * col_w, col_w)
                send(ref, right, ag_send.at[m, t, j], ag_recv.at[m, t, j, 0, 0])
                send(ref, left, ag_send.at[m, t, j], ag_recv.at[m, t, j, 0, 1])
                send(ref, peer, d2d_send.at[m, t, j], d2d_recv.at[m, t, j])

    def ag_event(m, t, j, d):
        last = d == half
        for side in range(2):
            chip = lax.rem(z + (n_chip - d if side == 0 else d), n_chip)
            col, width = (j * col_w, col_w) if not last else (j * col_w + side * sub_w, sub_w)
            ref = blk(m, t, chip, col, width)
            pltpu.make_async_copy(ref, ref, ag_recv.at[m, t, j, d - 1, side]).wait()
            if d < half - 1:
                fwd = ref
            elif d == half - 1:
                fwd = blk(m, t, chip, j * col_w + side * sub_w, sub_w)
            else:
                fwd = None
            if fwd is not None:
                send(fwd, right if side == 0 else left, ag_send.at[m, t, j], ag_recv.at[m, t, j, d, side])
            send(ref, peer, d2d_send.at[m, t, j], d2d_recv.at[m, t, j])

    def peer_blocks(m, t, j, core):
        row = pl.multiple_of(core * par_rows, par_rows)
        return bufs[t][1].at[m, pl.ds(row, par_rows), pl.ds(j * col_w, col_w)]

    def d2d_wait(m, t, j):
        ref = peer_blocks(m, t, j, 1 - c)
        pltpu.make_async_copy(ref, ref, d2d_recv.at[m, t, j]).wait()

    un_rows = unpacked.shape[0]

    def prep_wq():
        wq_cp.wait()
        per = un_rows // heads

        def body(i, _):
            unpacked[...] = stage_q[pl.ds(pl.multiple_of(i * un_rows, un_rows), un_rows), :].astype(F32)
            for h in range(heads):
                wall[pl.ds(pl.multiple_of(i * per, per), per), h * head_dim:(h + 1) * head_dim] = (
                    unpacked[pl.ds(h, per, stride=heads), :].astype(BF16))
            return 0

        lax.fori_loop(0, stage_q.shape[0] // un_rows, body, 0)

    kv_col = pl.multiple_of(hd + c * head_dim, head_dim)

    def prep_kv(i):
        pltpu.make_async_copy(wk_in.at[pl.ds(i * kv_rows, kv_rows)], stage_kv.at[i % 2], kvw_sem.at[i % 2]).wait()
        per = un_rows // kv_heads
        base = i * (kv_rows // kv_heads)

        def body(k, _):
            unpacked[...] = stage_kv[i % 2, pl.ds(pl.multiple_of(k * un_rows, un_rows), un_rows), :].astype(F32)
            wall[pl.ds(pl.multiple_of(base + k * per, per), per), pl.ds(kv_col, head_dim)] = (
                unpacked[pl.ds(z, per, stride=kv_heads), :].astype(BF16))
            return 0

        lax.fori_loop(0, kv_rows // un_rows, body, 0)
        if i + 2 < n_kv:
            kv_load(i + 2)

    def kv_swap():
        ref = wall.at[:, pl.ds(kv_col, head_dim)]
        pltpu.make_async_remote_copy(src_ref=ref, dst_ref=ref, send_sem=wx_sem.at[0], recv_sem=wx_sem.at[1],
                                     device_id=to(peer), device_id_type=MESH).start()

    def kv_swap_wait():
        ref = wall.at[:, pl.ds(kv_col, head_dim)]
        pltpu.make_async_copy(ref, ref, wx_sem.at[0]).wait()
        ref = wall.at[:, pl.ds(pl.multiple_of(hd + (1 - c) * head_dim, head_dim), head_dim)]
        pltpu.make_async_copy(ref, ref, wx_sem.at[1]).wait()

    def proj_x(m, j):
        for k in range(2):
            cols = slice(j * col_w + k * sub_w, j * col_w + (k + 1) * sub_w)
            a = dot(xb[m, :, cols], wall[cols, :])
            if j == 0 and k == 0:
                acc_x[...] = a
            else:
                acc_x[...] += a

    def proj_dy(m, j):
        for k in range(2):
            cols = slice(j * col_w + k * sub_w, j * col_w + (k + 1) * sub_w)
            a = dot(dyb[m, :, cols], wo[:, cols], NT)
            if j == 0 and k == 0:
                acc_do[...] = a
            else:
                acc_do[...] += a

    def round_x():
        qb[...] = acc_x[:, :hd].astype(BF16)
        kvb[...] = acc_x[:, hd:].astype(BF16)

    def round_dy():
        dob[...] = acc_do[...].astype(BF16)

    def position(axis):
        r = lax.broadcasted_iota(jnp.int32, (n_rows, 1) if axis == 0 else (1, n_rows), axis)
        inner = r % par_rows
        return (inner // tok) * (2 * tok) + (r // par_rows) * tok + inner % tok

    def head(m, h):
        cols = slice(h * head_dim, (h + 1) * head_dim)
        q, k, v = qb[:, cols], kvb[:, :head_dim], kvb[:, head_dim:]
        do = dob[:, cols]
        s = dot(q, k, NT) * scale
        s = jnp.where(position(0) >= position(1), s, -jnp.inf)
        e = jnp.exp(s - jnp.max(s, axis=-1, keepdims=True))
        p = e / jnp.sum(e, axis=-1, keepdims=True)
        pb = p.astype(BF16)
        o = dot(pb, v).astype(BF16)
        ob[m, :, cols] = o
        dp = dot(do, v, NT)
        delta = jnp.sum(do.astype(F32) * o.astype(F32), axis=-1, keepdims=True)
        ds = (p * (dp - delta)).astype(BF16)
        prob_b[h] = pb
        ds_b[h] = ds
        dqb[m, :, cols] = (dot(ds, k) * scale).astype(BF16)

    def head_kv(m, h):
        cols = slice(h * head_dim, (h + 1) * head_dim)
        dk = dot(ds_b[h], qb[:, cols], TN) * scale
        dv = dot(prob_b[h], dob[:, cols], TN)
        if h == 0:
            dkv_f[m, :, :head_dim] = dk
            dkv_f[m, :, head_dim:] = dv
        else:
            dkv_f[m, :, :head_dim] += dk
            dkv_f[m, :, head_dim:] += dv

    def kv_round(m):
        dkvp[...] = dkv_f[m].astype(BF16)
        pltpu.make_async_remote_copy(src_ref=dkv_f.at[m], dst_ref=dkv_peer.at[m], send_sem=dkv_sem.at[m, 0],
                                     recv_sem=dkv_sem.at[m, 1], device_id=to(peer), device_id_type=MESH).start()

    def kv_total(m):
        pltpu.make_async_copy(dkv_f.at[m], dkv_f.at[m], dkv_sem.at[m, 0]).wait()
        pltpu.make_async_copy(dkv_peer.at[m], dkv_peer.at[m], dkv_sem.at[m, 1]).wait()
        dkv_tot[m] = (dkv_f[m] + dkv_peer[m]).astype(BF16)

    dw_n = 4
    dw_w = d_model // dw_n

    def put(ref, idx, val, m):
        if m == 0:
            ref[idx] = val
        else:
            ref[idx] += val

    def dw_x(m, i):
        ck = lax.rem(c * (dw_n // 2) + i, dw_n)
        start = pl.multiple_of(ck * dw_w, dw_w)
        xt = xb[m, :, pl.ds(start, dw_w)].T
        g = dot(xt, dqb[m])
        for h in range(heads):
            put(dwq, (pl.ds(start * heads + h, dw_w, stride=heads), slice(None)),
                g[:, h * head_dim:(h + 1) * head_dim], m)
        if i < dw_n // 2:
            g = dot(xt, dkv_tot[m])
            rows = slice(i * dw_w, (i + 1) * dw_w)
            put(dwk, (rows, slice(None)), g[:, :head_dim], m)
            put(dwv, (rows, slice(None)), g[:, head_dim:], m)

    def dw_o(m, i):
        cols = slice(i * dw_w, (i + 1) * dw_w)
        put(dwo, (slice(None), cols), dot(ob[m], dyb[m, :, cols], TN), m)

    def dw_steps(m):
        return ([functools.partial(dw_o, m, i) for i in range(dw_n)]
                + [functools.partial(dw_x, m, i) for i in range(dw_n)])

    rs_n = 4
    rs_w = d_model // rs_n
    rs_h = rs_w // 2

    def dx_chunk(m, j):
        cols = slice(j * rs_w, (j + 1) * rs_w)
        away = pl.ds(pl.multiple_of((1 - c) * par_rows, par_rows), par_rows)
        keep = pl.ds(pl.multiple_of(c * par_rows, par_rows), par_rows)
        lhs = jnp.concatenate([jnp.concatenate([dqb[m, rows, :], dkvp[rows, :]], axis=1) for rows in (away, keep)], axis=0)
        part = dot(lhs, wall[cols, :], NT)
        psend[m, :, cols] = part[:par_rows].astype(BF16)
        dx_f[m, :, cols] = part[par_rows:]
        pltpu.make_async_remote_copy(src_ref=psend.at[m, :, cols], dst_ref=precv.at[m, :, cols],
                                     send_sem=ps_send.at[m, j], recv_sem=ps_recv.at[m, j],
                                     device_id=to(peer), device_id_type=MESH).start()

    def own_part(m, chip, col, width):
        rows = pl.ds(pl.multiple_of(chip * tok, tok), tok)
        return dx_f[m, rows, col:col + width] + precv[m, rows, col:col + width].astype(F32)

    def rs_send_to(m, j, side, d, col, width):
        src = sbuf.at[m, side, d - 1, :, pl.ds(col, width)]
        dst = rbuf.at[m, side, d - 1, :, pl.ds(col, width)]
        pltpu.make_async_remote_copy(src_ref=src, dst_ref=dst, send_sem=rs_send.at[m, j],
                                     recv_sem=rs_recv.at[m, j, d - 1, side],
                                     device_id=to(right if side == 0 else left), device_id_type=MESH).start()

    def chip_at(side, d):
        return lax.rem(z + (d if side == 0 else n_chip - d), n_chip)

    def rs_start(m, j):
        ref = precv.at[m, :, pl.ds(j * rs_w, rs_w)]
        pltpu.make_async_copy(ref, ref, ps_recv.at[m, j]).wait()
        for side in range(2):
            col = j * rs_w + side * rs_h
            sbuf[m, side, half - 1, :, col:col + rs_h] = own_part(m, chip_at(side, half), col, rs_h).astype(BF16)
        for side in range(2):
            rs_send_to(m, j, side, half, j * rs_w + side * rs_h, rs_h)

    def rs_event(m, j, d):
        col = j * rs_w
        for side in range(2):
            rcol, rwidth = (col + side * rs_h, rs_h) if d == half else (col, rs_w)
            ref = rbuf.at[m, side, d - 1, :, pl.ds(rcol, rwidth)]
            pltpu.make_async_copy(ref, ref, rs_recv.at[m, j, d - 1, side]).wait()
        if d == 1:
            total = own_part(m, z, col, rs_w)
            for side in range(2):
                total = total + rbuf[m, side, 0, :, col:col + rs_w].astype(F32)
            dx_own[m, :, col:col + rs_w] = total.astype(BF16)
            return
        for side in range(2):
            chip = chip_at(side, d - 1)
            if d == half:
                a, b = col + side * rs_h, col + (1 - side) * rs_h
                sbuf[m, side, d - 2, :, a:a + rs_h] = (
                    own_part(m, chip, a, rs_h) + rbuf[m, side, d - 1, :, a:a + rs_h].astype(F32)).astype(BF16)
                sbuf[m, side, d - 2, :, b:b + rs_h] = own_part(m, chip, b, rs_h).astype(BF16)
            else:
                sbuf[m, side, d - 2, :, col:col + rs_w] = (
                    own_part(m, chip, col, rs_w)
                    + rbuf[m, side, d - 1, :, col:col + rs_w].astype(F32)).astype(BF16)
        for side in range(2):
            rs_send_to(m, j, side, d - 1, col, rs_w)

    tensor_cols = [(t, j) for t in range(2) for j in range(n_col)]

    ag_start(0)
    work = [prep_wq] + [functools.partial(prep_kv, i) for i in range(n_kv)] + [kv_swap]
    slots = [(d, t, j) for d in range(1, half) for t, j in tensor_cols]
    for s, (d, t, j) in enumerate(slots):
        ag_event(0, t, j, d)
        if work:
            work.pop(0)()
    for w in work:
        w()
    ag_start(1)
    wo_cp.wait()
    kv_swap_wait()

    def finish_gather(m, extra):
        for t, j in tensor_cols:
            ag_event(m, t, j, half)
            for f in extra.get((t, j), ()):
                f()
            if (t, j) == (0, 0):
                continue
            pt, pj = tensor_cols[tensor_cols.index((t, j)) - 1]
            finish_part(m, pt, pj)
        finish_part(m, *tensor_cols[-1])

    def finish_part(m, t, j):
        d2d_wait(m, t, j)
        (proj_x if t == 0 else proj_dy)(m, j)
        if j == n_col - 1:
            (round_x if t == 0 else round_dy)()

    def attn_steps(m):
        steps = []
        for h in range(heads):
            steps.append(functools.partial(head, m, h))
            steps.append(functools.partial(head_kv, m, h))
        steps.append(functools.partial(kv_round, m))
        return steps

    finish_gather(0, {})
    work = attn_steps(0) + [functools.partial(dx_chunk, 0, j) for j in range(rs_n)]
    later = [functools.partial(kv_total, 0)] + dw_steps(0)
    for i, (d, t, j) in enumerate(slots):
        ag_event(1, t, j, d)
        if i == len(slots) - 2:
            while work:
                work.pop(0)()
            for k in range(rs_n):
                rs_start(0, k)
        (work or later).pop(0)()
    ev = functools.partial(rs_event, 0)
    ag_event(1, 0, 0, half)
    ag_event(1, 0, 1, half)
    finish_part(1, 0, 0)
    ev(0, half)
    ag_event(1, 1, 0, half)
    ev(1, half)
    ev(2, half)
    finish_part(1, 0, 1)
    ag_event(1, 1, 1, half)
    ev(3, half)
    finish_part(1, 1, 0)
    finish_part(1, 1, 1)
    attn = attn_steps(1)
    for k in range(2 * heads):
        attn.pop(0)()
        ev(k, half - 1)
    for f in attn:
        f()
    dx_chunk(1, 0)
    dx_chunk(1, 1)
    ev(0, half - 2)
    rs_start(1, 0)
    dx_chunk(1, 2)
    ev(1, half - 2)
    rs_start(1, 1)
    dx_chunk(1, 3)
    ev(2, half - 2)
    rs_start(1, 2)
    later.pop(0)()
    ev(3, half - 2)
    later.pop(0)()
    rs_start(1, 3)
    later += [functools.partial(kv_total, 1)] + dw_steps(1)
    for j in range(rs_n):
        if j < rs_n - 1:
            later.pop(0)()
        rs_event(1, j, half)
    for j in range(rs_n):
        rs_event(1, j, half - 1)
        later.pop(0)()
    for j in range(rs_n):
        rs_event(0, j, 1)
        if later:
            later.pop(0)()
        rs_event(1, j, half - 2)
        if later:
            later.pop(0)()
    for f in later:
        f()
    for m in range(micro_n):
        for t, j in tensor_cols:
            ref = bufs[t][1].at[m, pl.ds(0, (n_chip - 1) * tok), pl.ds(j * col_w, col_w)]
            pltpu.make_async_copy(ref, ref, ag_send.at[m, t, j]).wait()
            ref = peer_blocks(m, t, j, c)
            pltpu.make_async_copy(ref, ref, d2d_send.at[m, t, j]).wait()
        for j in range(rs_n):
            ref = psend.at[m, :, pl.ds(j * rs_w, rs_w)]
            pltpu.make_async_copy(ref, ref, ps_send.at[m, j]).wait()

    def rs_drain(m):
        for j in range(rs_n):
            ref = psend.at[m, pl.ds(0, (n_chip - 1) * tok), pl.ds(j * rs_w, rs_w)]
            pltpu.make_async_copy(ref, ref, rs_send.at[m, j]).wait()

    rs_drain(0)
    for j in range(rs_n):
        rs_event(1, j, 1)
    rs_drain(1)


def copy_kernel(n, *refs):
    srcs, dsts, sem = refs[:n], refs[n:2 * n], refs[2 * n]
    pairs = []
    for a, b in zip(srcs, dsts):
        parts = max(1, a.shape[0] // 2560) if a.shape[-1] < 1024 else a.shape[0] // 64 or 1
        rows = a.shape[0] // parts
        pairs += [(a.at[pl.ds(i * rows, rows)], b.at[pl.ds(i * rows, rows)]) for i in range(parts)]
    copies = [pltpu.make_async_copy(a, b, sem.at[i]) for i, (a, b) in enumerate(pairs)]
    for cp in copies:
        cp.start()
    for cp in copies:
        cp.wait()


def solution(mesh):
    n_dev = mesh.shape["model"]

    def device_grads(x_loc, dy_loc, w_q, w_k, w_v, w_o):
        micro_n, tok, d_model = x_loc.shape
        heads, head_dim = w_q.shape[1], w_q.shape[2]
        kv_heads = w_k.shape[1]
        n_rows = tok * n_dev
        par_rows = n_rows // 2
        hd = heads * head_dim
        n_chip = n_dev // 2
        half = n_chip // 2
        any_spec = pl.BlockSpec(memory_space=pl.ANY)
        dma = pltpu.SemaphoreType.DMA
        scratch = [
            pltpu.VMEM((micro_n, n_rows, d_model), BF16),
            pltpu.VMEM((micro_n, n_rows, d_model), BF16),
            pltpu.VMEM((d_model, hd + 2 * head_dim), BF16),
            pltpu.VMEM((hd, d_model), BF16),
            pltpu.VMEM((d_model * heads, head_dim), BF16),
            pltpu.VMEM((2, d_model * kv_heads // 8, head_dim), BF16),
            pltpu.VMEM((512, head_dim), F32),
            pltpu.VMEM((n_rows, hd + 2 * head_dim), F32),
            pltpu.VMEM((n_rows, hd), F32),
            pltpu.VMEM((n_rows, hd), BF16),
            pltpu.VMEM((n_rows, 2 * head_dim), BF16),
            pltpu.VMEM((n_rows, hd), BF16),
            pltpu.VMEM((micro_n, n_rows, hd), BF16),
            pltpu.VMEM((micro_n, n_rows, hd), BF16),
            pltpu.VMEM((n_rows, 2 * head_dim), BF16),
            pltpu.VMEM((heads, n_rows, n_rows), BF16),
            pltpu.VMEM((heads, n_rows, n_rows), BF16),
            pltpu.VMEM((micro_n, n_rows, 2 * head_dim), F32),
            pltpu.VMEM((micro_n, n_rows, 2 * head_dim), F32),
            pltpu.VMEM((micro_n, n_rows, 2 * head_dim), BF16),
            pltpu.VMEM((micro_n, par_rows, d_model), F32),
            pltpu.VMEM((micro_n, par_rows, d_model), BF16),
            pltpu.VMEM((micro_n, par_rows, d_model), BF16),
            pltpu.VMEM((micro_n, 2, half, tok, d_model), BF16),
            pltpu.VMEM((micro_n, 2, half, tok, d_model), BF16),
            dma((micro_n, 2)), dma((2,)), dma((2,)),
            dma((micro_n, 2, 2)), dma((micro_n, 2, 2, half, 2)),
            dma((micro_n, 2, 2)), dma((micro_n, 2, 2)), dma((2,)),
            dma((micro_n, 2)), dma((micro_n, 4)), dma((micro_n, 4)),
            dma((micro_n, 4)), dma((micro_n, 4, half, 2)),
        ]
        dx, dwq, dwk, dwv, dwo = pl.pallas_call(
            functools.partial(attn_kernel, n_dev, kv_heads),
            out_shape=(
                pltpu.VMEM((micro_n, tok, d_model), BF16),
                pltpu.VMEM((d_model * heads, head_dim), F32),
                pltpu.VMEM((d_model // 2, head_dim), F32),
                pltpu.VMEM((d_model // 2, head_dim), F32),
                pltpu.VMEM((hd, d_model), F32),
            ),
            in_specs=[any_spec] * 6,
            out_specs=(pl.BlockSpec(memory_space=pltpu.VMEM),) * 5,
            scratch_shapes=scratch,
            compiler_params=pltpu.CompilerParams(collective_id=0, has_side_effects=True,
                                                 vmem_limit_bytes=46 * 1024 * 1024),
        )(x_loc, dy_loc, w_q.reshape(d_model * heads, head_dim), w_k.reshape(d_model * kv_heads, head_dim),
          w_v.reshape(d_model * kv_heads, head_dim), w_o.reshape(hd, d_model))

        grads = (dx, dwq, dwk, dwv, dwo)
        dx, dwq, dwk, dwv, dwo = pl.pallas_call(
            functools.partial(copy_kernel, len(grads)),
            out_shape=tuple(jax.ShapeDtypeStruct(g.shape, g.dtype) for g in grads),
            in_specs=[pl.BlockSpec(memory_space=pltpu.VMEM)] * len(grads),
            out_specs=(any_spec,) * len(grads),
            scratch_shapes=[dma((16,))],
            compiler_params=pltpu.CompilerParams(vmem_limit_bytes=1024 * 1024),
        )(*grads)
        return dx, dwq.reshape(d_model, heads, head_dim), dwk, dwv, dwo.reshape(heads, head_dim, d_model)

    return jax.shard_map(
        device_grads, mesh=mesh,
        in_specs=(P("data", "model", None), P("data", "model", None), P(None, "model", None),
                  P(None, None, None), P(None, None, None), P("model", None, None)),
        out_specs=(P("data", "model", None), P("data", "model", None), P(("data", "model"), None),
                   P(("data", "model"), None), P(("data", "model"), None, None)),
        check_vma=False)
```
